8 devices in a mesh: graph: 8 (over z, y, x, core).
Axes of the slice: x: 2, y: 2, z: 1, core: 2. Of those that a mesh axis runs over, the one named last changes fastest.
Arguments:
- node_feats: bfloat16 [16384, 200], P('graph')
- w_one: float32 [200, 512], replicated
- w_two: float32 [512, 107], replicated
- send_idx: int32 [16, 1024], P('graph')
- edge_src: int32 [65536], P('graph')
- edge_dst: int32 [65536], P('graph')
- edge_w: float32 [65536], P('graph')
- labels: int32 [16384], P('graph')
- label_mask: int32 [16384], P('graph')
Outputs:
- output 1: float32 [], replicated
- output 2: float32 [200, 512], replicated
- output 3: float32 [512, 107], replicated
All inputs are finite; a program needn't handle non-finite values.
Results may differ from the reference program's by a relative error of at most 0.001.
Values are sent between devices in bfloat16 or wider.
A program may use at most 1 GiB of HBM per device.

```python
import jax
import jax.numpy as jnp
from jax import lax

GRAPH = 8
N_LOC = 2048
HALO = 1024
EDGES = 8192
F_IN = 200
F_HID = 512
CLASSES = 107


def draw_structure(key):
    sub_keys = jax.random.split(key, 9)
    halo_pct = jax.random.randint(sub_keys[0], (GRAPH, 1), 5, 21, jnp.int32)
    pick_draw = jax.random.randint(sub_keys[1], (GRAPH, EDGES), 0, 100, jnp.int32)
    own_src = jax.random.randint(sub_keys[2], (GRAPH, EDGES), 0, N_LOC, jnp.int32)
    halo_src = jax.random.randint(sub_keys[3], (GRAPH, EDGES), N_LOC, N_LOC + 2 * HALO, jnp.int32)
    edge_src = jnp.where(pick_draw < halo_pct, halo_src, own_src)
    edge_dst = jax.random.randint(sub_keys[4], (GRAPH, EDGES), 0, N_LOC, jnp.int32)
    live_count = jax.random.randint(sub_keys[5], (GRAPH, 1), EDGES // 4, EDGES + 1, jnp.int32)
    is_live = jnp.arange(EDGES)[None, :] < live_count
    send_idx = jax.random.randint(sub_keys[6], (GRAPH * 2, HALO), 0, N_LOC, jnp.int32)
    labels = jax.random.randint(sub_keys[7], (GRAPH * N_LOC,), 0, CLASSES, jnp.int32)
    label_mask = jax.random.randint(sub_keys[8], (GRAPH * N_LOC,), 0, 2, jnp.int32)
    return edge_src, edge_dst, is_live, send_idx, labels, label_mask


def normalise(raw_weight, edge_dst):
    weight_sum = jax.vmap(lambda w_g, dst_g: jax.ops.segment_sum(w_g, dst_g, num_segments=N_LOC))(raw_weight, edge_dst)
    node_sum = jnp.take_along_axis(weight_sum, edge_dst, axis=1)
    return raw_weight / jnp.maximum(node_sum, 1e-6)


def setup_inputs(seed: int = 0) -> dict:
    key_list = jax.random.split(jax.random.key(seed), 5)
    edge_src, edge_dst, is_live, send_idx, labels, label_mask = draw_structure(key_list[0])
    deg_gain = EDGES / N_LOC
    node_feats = jax.random.normal(key_list[1], (GRAPH * N_LOC, F_IN), jnp.float32)
    w_one = jax.random.normal(key_list[2], (F_IN, F_HID), jnp.float32) * (deg_gain / F_IN) ** 0.5
    w_two = jax.random.normal(key_list[3], (F_HID, CLASSES), jnp.float32) * (deg_gain / F_HID) ** 0.5
    raw_weight = jax.random.uniform(key_list[4], (GRAPH, EDGES), jnp.float32, 0.5, 1.5) * is_live
    edge_w = normalise(raw_weight, edge_dst)
    return {"node_feats": node_feats.astype(jnp.bfloat16), "w_one": w_one, "w_two": w_two, "send_idx": send_idx, "edge_src": edge_src.reshape(-1), "edge_dst": edge_dst.reshape(-1), "edge_w": edge_w.reshape(-1), "labels": labels, "label_mask": label_mask}


def halo_extend(node_table, send_rows):
    pick_rows = jax.vmap(lambda table_g, idx_g: table_g[idx_g])
    from_prev = pick_rows(jnp.roll(node_table, 1, axis=0), jnp.roll(send_rows[:, 1], 1, axis=0))
    from_next = pick_rows(jnp.roll(node_table, -1, axis=0), jnp.roll(send_rows[:, 0], -1, axis=0))
    return jnp.concatenate([node_table, from_prev, from_next], axis=1)


def aggregate(ext_table, src_dev, dst_dev, w_dev):
    def one_device(args_g):
        ext_g, src_g, dst_g, w_g = args_g
        return jax.ops.segment_sum(w_g[:, None] * ext_g[src_g].astype(jnp.float32), dst_g, num_segments=N_LOC)
    return lax.map(one_device, (ext_table, src_dev, dst_dev, w_dev))


def scatter_back(grad_rows, send_rows, src_dev, dst_dev, w_dev):
    def one_device(args_g):
        grad_g, src_g, dst_g, w_g = args_g
        return jax.ops.segment_sum(w_g[:, None] * grad_g[dst_g], src_g, num_segments=N_LOC + 2 * HALO)
    ext_grad = lax.map(one_device, (grad_rows, src_dev, dst_dev, w_dev))
    back_prev = jnp.roll(ext_grad[:, N_LOC:N_LOC + HALO], -1, axis=0)
    back_next = jnp.roll(ext_grad[:, N_LOC + HALO:], 1, axis=0)
    row_ids = jnp.concatenate([send_rows[:, 1], send_rows[:, 0]], axis=1)
    ret_vals = jnp.concatenate([back_prev, back_next], axis=1)
    returned = jax.vmap(lambda vals_g, ids_g: jax.ops.segment_sum(vals_g, ids_g, num_segments=N_LOC))(ret_vals, row_ids)
    return ext_grad[:, :N_LOC] + returned


def reference(node_feats, w_one, w_two, send_idx, edge_src, edge_dst, edge_w, labels, label_mask):
    send_rows = send_idx.reshape(GRAPH, 2, HALO)
    src_dev = edge_src.reshape(GRAPH, EDGES)
    dst_dev = edge_dst.reshape(GRAPH, EDGES)
    w_dev = edge_w.reshape(GRAPH, EDGES)
    w_one_b = w_one.astype(jnp.bfloat16)
    w_two_b = w_two.astype(jnp.bfloat16)
    tab_one = jnp.dot(node_feats, w_one_b, preferred_element_type=jnp.float32).astype(jnp.bfloat16)
    pre_one = aggregate(halo_extend(tab_one.reshape(GRAPH, N_LOC, F_HID), send_rows), src_dev, dst_dev, w_dev).reshape(GRAPH * N_LOC, F_HID)
    hidden = jnp.maximum(pre_one, 0.0).astype(jnp.bfloat16)
    tab_two = jnp.dot(hidden, w_two_b, preferred_element_type=jnp.float32).astype(jnp.bfloat16)
    logits = aggregate(halo_extend(tab_two.reshape(GRAPH, N_LOC, CLASSES), send_rows), src_dev, dst_dev, w_dev).reshape(GRAPH * N_LOC, CLASSES)
    mask_f = label_mask.astype(jnp.float32)
    label_count = jnp.maximum(jnp.sum(mask_f), 1.0)
    log_norm = jax.nn.logsumexp(logits, axis=1)
    one_hot = (labels[:, None] == jnp.arange(CLASSES)[None, :]).astype(jnp.float32)
    picked = jnp.sum(logits * one_hot, axis=1)
    mean_loss = jnp.sum(mask_f * (log_norm - picked)) / label_count
    d_logits = (jnp.exp(logits - log_norm[:, None]) - one_hot) * (mask_f / label_count)[:, None]
    d_tab_two = scatter_back(d_logits.reshape(GRAPH, N_LOC, CLASSES), send_rows, src_dev, dst_dev, w_dev).reshape(GRAPH * N_LOC, CLASSES).astype(jnp.bfloat16)
    grad_two = jnp.dot(hidden.T, d_tab_two, preferred_element_type=jnp.float32)
    d_hidden = jnp.dot(d_tab_two, w_two_b.T, preferred_element_type=jnp.float32)
    d_pre = jnp.where(pre_one > 0.0, d_hidden, 0.0)
    d_tab_one = scatter_back(d_pre.reshape(GRAPH, N_LOC, F_HID), send_rows, src_dev, dst_dev, w_dev).reshape(GRAPH * N_LOC, F_HID).astype(jnp.bfloat16)
    grad_one = jnp.dot(node_feats.T, d_tab_one, preferred_element_type=jnp.float32)
    return mean_loss, grad_one, grad_two
```

```python
import functools

import jax
import jax.numpy as jnp
from jax import lax
from jax.experimental import pallas as pl
from jax.experimental.pallas import tpu as pltpu
from jax.sharding import PartitionSpec as P

GRAPH_AXIS = "graph"
CONTRACT_ROWS = (((0,), (0,)), ((), ()))
MESH = pl.DeviceIdType.MESH
F32 = jnp.float32
BF16 = jnp.bfloat16
LANES = 128
CHUNK = 256
SLOT = 384
VMEM_LIMIT = 64000000

SMEM_SPEC = pl.BlockSpec(memory_space=pltpu.SMEM)
VMEM_SPEC = pl.BlockSpec(memory_space=pltpu.VMEM)


def params(**kw):
    return pltpu.CompilerParams(vmem_limit_bytes=VMEM_LIMIT, **kw)


def zero_rows(refs):
    rows = refs[0].shape[0]

    def body(i, _):
        for ref in refs:
            ref[pl.ds(i * 64, 64), :] = jnp.zeros((64, LANES), F32)
        return 0

    lax.fori_loop(0, rows // 64, body, 0)


def sum_rows(out, refs):
    rows = refs[0].shape[0]

    def body(i, _):
        total = refs[0][pl.ds(i * 64, 64), :]
        for ref in refs[1:]:
            total = total + ref[pl.ds(i * 64, 64), :]
        out[pl.ds(i * 64, 64), :] = total
        return 0

    lax.fori_loop(0, rows // 64, body, 0)


def edge_pass(from_ref, to_ref, w_ref, cnt_ref, table, accs, width, unroll, back):
    n_acc = len(accs)
    shift = unroll.bit_length() - 1

    def row(r, _):
        blocks = lax.shift_right_logical(cnt_ref[r] + (unroll - 1), shift)

        def body(j, _):
            off = r * SLOT + (SLOT - unroll - j * unroll if back else j * unroll)
            vals = [table[pl.ds(pl.multiple_of(from_ref[off + u], width), width), :] * w_ref[off + u] for u in range(unroll)]
            for g in range(unroll // n_acc):
                rows = [pl.multiple_of(to_ref[off + g * n_acc + k], width) for k in range(n_acc)]
                old = [accs[k][pl.ds(rows[k], width), :] for k in range(n_acc)]
                for k in range(n_acc):
                    accs[k][pl.ds(rows[k], width), :] = old[k] + vals[g * n_acc + k]
            return 0

        lax.fori_loop(0, blocks, body, 0)
        return 0

    lax.fori_loop(0, cnt_ref.shape[0], row, 0)


def scatter_pass(ids_ref, table, accs, width, unroll):
    n_acc = len(accs)

    def body(j, _):
        off = j * unroll
        for g in range(unroll // n_acc):
            rows = [pl.multiple_of(ids_ref[off + g * n_acc + k], width) for k in range(n_acc)]
            vals = [table[pl.ds(pl.multiple_of((off + g * n_acc + k) * width, width), width), :] for k in range(n_acc)]
            old = [accs[k][pl.ds(rows[k], width), :] for k in range(n_acc)]
            for k in range(n_acc):
                accs[k][pl.ds(rows[k], width), :] = old[k] + vals[k]
        return 0

    lax.fori_loop(0, ids_ref.shape[0] // unroll, body, 0)


def gather_pass(ids_ref, table, out, width, unroll=8):
    def body(j, _):
        for u in range(unroll):
            i = j * unroll + u
            out[pl.ds(pl.multiple_of(i * width, width), width), :] = table[pl.ds(pl.multiple_of(ids_ref[i], width), width), :]
        return 0

    lax.fori_loop(0, ids_ref.shape[0] // unroll, body, 0)


def spread(table, start, block):
    tiles = block.shape[1] // LANES
    for c in range(tiles):
        table[pl.ds(start * tiles + c, block.shape[0], tiles), :] = block[:, c * LANES:(c + 1) * LANES]


def unspread(table, start, rows, tiles):
    return jnp.concatenate([table[pl.ds(start * tiles + c, rows, tiles), :] for c in range(tiles)], axis=1)


def halo_rows_kernel(ids2, x, to_next, to_prev, table, picked):
    rows = x.shape[0]

    def put(i, _):
        spread(table, i * 256, x[pl.ds(i * 256, 256), :].astype(F32))
        return 0

    lax.fori_loop(0, rows // 256, put, 0)
    gather_pass(ids2, table, picked, 2)
    half = to_next.shape[0]

    def take(i, _):
        to_next[pl.ds(i * 256, 256), :] = unspread(picked, i * 256, 256, 2).astype(BF16)
        to_prev[pl.ds(i * 256, 256), :] = unspread(picked, half + i * 256, 256, 2).astype(BF16)
        return 0

    lax.fori_loop(0, half // 256, take, 0)


def one_own_kernel(s4, d4, w, cnt, x, w1, y, table, *accs):
    zero_rows(accs)

    def put(i, _):
        t = jnp.dot(x[pl.ds(i * 256, 256), :], w1[...], preferred_element_type=F32)
        spread(table, i * 256, t.astype(BF16).astype(F32))
        return 0

    lax.fori_loop(0, x.shape[0] // 256, put, 0)
    edge_pass(s4, d4, w, cnt, table, accs, 4, 16, False)
    sum_rows(y, accs)


def one_halo_kernel(s4, d4, w, cnt, ids, y_own, x_prev, x_next, w1, w2, hid, t2, to_next, to_prev, table, picked, *accs):
    zero_rows(accs)
    half = x_prev.shape[0]

    def put(i, _):
        t = jnp.dot(x_prev[pl.ds(i * 256, 256), :], w1[...], preferred_element_type=F32)
        spread(table, i * 256, t.astype(BF16).astype(F32))
        t = jnp.dot(x_next[pl.ds(i * 256, 256), :], w1[...], preferred_element_type=F32)
        spread(table, half + i * 256, t.astype(BF16).astype(F32))
        return 0

    lax.fori_loop(0, half // 256, put, 0)
    edge_pass(s4, d4, w, cnt, table, accs, 4, 8, True)
    sum_rows(accs[0], (y_own,) + accs)

    def act(i, _):
        h = jnp.maximum(unspread(accs[0], i * 256, 256, 4), 0.0).astype(BF16)
        hid[pl.ds(i * 256, 256), :] = h
        t = jnp.dot(h, w2[...], preferred_element_type=F32)
        t2[pl.ds(i * 256, 256), :] = t.astype(BF16).astype(F32)
        return 0

    lax.fori_loop(0, hid.shape[0] // 256, act, 0)
    gather_pass(ids, t2, picked, 1)

    def take(i, _):
        to_next[pl.ds(i * 256, 256), :] = picked[pl.ds(i * 256, 256), :].astype(BF16)
        to_prev[pl.ds(i * 256, 256), :] = picked[pl.ds(half + i * 256, 256), :].astype(BF16)
        return 0

    lax.fori_loop(0, half // 256, take, 0)


def narrow_own_kernel(frm, to, w, cnt, table, out, *accs):
    zero_rows(accs)
    edge_pass(frm, to, w, cnt, table, accs, 1, 16, False)
    sum_rows(out, accs)


def wide_own_kernel(frm, to, w, cnt, table, out, *accs):
    zero_rows(accs)
    edge_pass(frm, to, w, cnt, table, accs, 4, 16, False)
    sum_rows(out, accs)


def logits_kernel(classes, s, d, w, cnt, z_own, t_prev, t_next, labels, count, dz, back_prev, back_next, loss, table, *accs):
    zero_rows(accs)
    half = t_prev.shape[0]

    def put(i, _):
        table[pl.ds(i * 256, 256), :] = t_prev[pl.ds(i * 256, 256), :].astype(F32)
        table[pl.ds(half + i * 256, 256), :] = t_next[pl.ds(i * 256, 256), :].astype(F32)
        return 0

    lax.fori_loop(0, half // 256, put, 0)
    edge_pass(s, d, w, cnt, table, accs, 1, 8, True)
    scale = 1.0 / count[0:1, :]
    denom = count[0:1, :]
    loss[...] = jnp.zeros_like(loss)

    def soft(i, _):
        at = pl.ds(i * 64, 64)
        z = z_own[at, :]
        for acc in accs:
            z = z + acc[at, :]
        lane = lax.broadcasted_iota(jnp.int32, z.shape, 1)
        lab = labels[at, :]
        hot = lab == lane
        keep = lab >= 0
        zm = jnp.where(lane < classes, z, -jnp.inf)
        top = jnp.max(zm, axis=1, keepdims=True)
        ex = jnp.exp(zm - top)
        log_norm = jnp.log(jnp.sum(ex, axis=1, keepdims=True)) + top
        hot_f = jnp.where(hot, 1.0, 0.0)
        term = jnp.where(hot, log_norm - z, 0.0)
        part = term[0:8]
        for b in range(1, 8):
            part = part + term[b * 8:b * 8 + 8]
        loss[...] += part
        mask_f = jnp.where(keep, 1.0, 0.0)
        dz[at, :] = jnp.where(lane < classes, (jnp.exp(zm - log_norm) - hot_f) * (mask_f / denom), 0.0)
        return 0

    lax.fori_loop(0, dz.shape[0] // 64, soft, 0)
    zero_rows(accs)
    edge_pass(d, s, w, cnt, dz, accs, 1, 8, True)

    def fin(i, _):
        at = pl.ds(i * 64, 64)
        bt = pl.ds(half + i * 64, 64)
        a, b = accs[0][at, :], accs[0][bt, :]
        for acc in accs[1:]:
            a, b = a + acc[at, :], b + acc[bt, :]
        back_prev[at, :] = a
        back_next[at, :] = b
        return 0

    lax.fori_loop(0, half // 64, fin, 0)


def hidden_grad_kernel(s4, d4, w, cnt, ids, own, ret_next, ret_prev, hid, w2t, dt2, dy, back_prev, back_next, *accs):
    n_loc, half = own.shape[0], ret_next.shape[0]
    narrow = tuple(acc.at[pl.ds(0, n_loc)] for acc in accs)
    zero_rows(narrow)
    scatter_pass(ids.at[pl.ds(0, half)], ret_next, narrow, 1, 8)
    scatter_pass(ids.at[pl.ds(half, half)], ret_prev, narrow, 1, 8)

    def fold(i, _):
        at = pl.ds(i * 256, 256)
        total = own[at, :]
        for acc in narrow:
            total = total + acc[at, :]
        dt = total.astype(BF16)
        dt2[at, :] = dt
        dh = jnp.dot(dt, w2t[...], preferred_element_type=F32)
        spread(dy, i * 256, jnp.where(hid[at, :].astype(F32) > 0.0, dh, 0.0))
        return 0

    lax.fori_loop(0, n_loc // 256, fold, 0)
    zero_rows(accs)
    edge_pass(d4, s4, w, cnt, dy, accs, 4, 8, True)
    quad = 4 * half

    def fin(i, _):
        at = pl.ds(i * 64, 64)
        bt = pl.ds(quad + i * 64, 64)
        a, b = accs[0][at, :], accs[0][bt, :]
        for acc in accs[1:]:
            a, b = a + acc[at, :], b + acc[bt, :]
        back_prev[at, :] = a
        back_next[at, :] = b
        return 0

    lax.fori_loop(0, quad // 64, fin, 0)


def table_grad_kernel(ids4, own, ret_next, ret_prev, dt1, *accs):
    half = ids4.shape[0] // 2
    zero_rows(accs)
    scatter_pass(ids4.at[pl.ds(0, half)], ret_next, accs, 4, 8)
    scatter_pass(ids4.at[pl.ds(half, half)], ret_prev, accs, 4, 8)

    def fold(i, _):
        total = unspread(own, i * 128, 128, 4)
        for acc in accs:
            total = total + unspread(acc, i * 128, 128, 4)
        dt1[pl.ds(i * 128, 128), :] = total.astype(BF16)
        return 0

    lax.fori_loop(0, dt1.shape[0] // 128, fold, 0)


def enter(me, num_dev):
    barrier = pltpu.get_barrier_semaphore()
    for step in range(1, num_dev):
        pl.semaphore_signal(barrier, inc=1, device_id=(lax.rem(me + step, num_dev),), device_id_type=MESH)
    pl.semaphore_wait(barrier, num_dev - 1)


def push(src, dst, send_sem, recv_sem, dev):
    copy = pltpu.make_async_remote_copy(src_ref=src, dst_ref=dst, send_sem=send_sem, recv_sem=recv_sem, device_id=(dev,), device_id_type=MESH)
    copy.start()
    return copy


def count_kernel(num_dev, part, out, slots, send_sem, recv_sem):
    me = lax.axis_index(GRAPH_AXIS)
    enter(me, num_dev)
    copies = []
    for step in range(1, num_dev):
        copies.append(push(part, slots.at[step - 1], send_sem.at[step - 1], recv_sem.at[step - 1], lax.rem(me + step, num_dev)))
    for copy in copies:
        copy.wait()
    total = part[...]
    for step in range(num_dev - 1):
        total = total + slots[step]
    out[...] = total


def reduce_kernel(num_dev, g1, g2, loss, o1, o2, lo, r1, r2, s1, s2, q1, q2, lslots, sem_s, sem_r, lsem_s, lsem_r):
    me = lax.axis_index(GRAPH_AXIS)
    core = lax.rem(me, 2)
    chip = me // 2
    mate = me + 1 - 2 * core
    h1, h2 = g1.shape[0] // 2, g2.shape[0] // 2
    e1, e2 = h1 // 4, h2 // 4
    enter(me, num_dev)
    other = 1 - core
    pair = [
        push(g1.at[pl.ds(pl.multiple_of(other * h1, h1), h1)], r1, sem_s.at[0], sem_r.at[0], mate),
        push(g2.at[pl.ds(pl.multiple_of(other * h2, h2), h2)], r2, sem_s.at[1], sem_r.at[1], mate),
    ]
    scalar = []
    for step in range(1, num_dev):
        scalar.append(push(loss, lslots.at[step - 1], lsem_s.at[step - 1], lsem_r.at[step - 1], lax.rem(me + step, num_dev)))
    for copy in pair:
        copy.wait()
    s1[...] = g1[pl.ds(pl.multiple_of(core * h1, h1), h1), :] + r1[...]
    s2[...] = g2[pl.ds(pl.multiple_of(core * h2, h2), h2), :] + r2[...]
    spreads = []
    for step in range(1, 4):
        far = lax.rem(chip + step, 4)
        dev = far * 2 + core
        k = 2 * step
        spreads.append(push(s1.at[pl.ds(pl.multiple_of(far * e1, e1), e1)], q1.at[step - 1], sem_s.at[k], sem_r.at[k], dev))
        spreads.append(push(s2.at[pl.ds(pl.multiple_of(far * e2, e2), e2)], q2.at[step - 1], sem_s.at[k + 1], sem_r.at[k + 1], dev))
    for copy in spreads:
        copy.wait()
    mine1 = pl.ds(pl.multiple_of(core * h1 + chip * e1, e1), e1)
    mine2 = pl.ds(pl.multiple_of(core * h2 + chip * e2, e2), e2)
    t1 = s1[pl.ds(pl.multiple_of(chip * e1, e1), e1), :]
    t2 = s2[pl.ds(pl.multiple_of(chip * e2, e2), e2), :]
    for step in range(3):
        t1 = t1 + q1[step]
        t2 = t2 + q2[step]
    o1[mine1, :] = t1
    o2[mine2, :] = t2
    gathers = []
    for step in range(1, 4):
        dev = lax.rem(chip + step, 4) * 2 + core
        k = 6 + 2 * step
        gathers.append((push(o1.at[mine1], o1.at[mine1], sem_s.at[k], sem_r.at[k], dev), push(o2.at[mine2], o2.at[mine2], sem_s.at[k + 1], sem_r.at[k + 1], dev)))
    tails = [push(o1.at[mine1], o1.at[mine1], sem_s.at[14], sem_r.at[14], mate), push(o2.at[mine2], o2.at[mine2], sem_s.at[15], sem_r.at[15], mate)]
    for step in range(1, 4):
        near = lax.rem(chip + 4 - step, 4)
        at1 = pl.ds(pl.multiple_of(core * h1 + near * e1, e1), e1)
        at2 = pl.ds(pl.multiple_of(core * h2 + near * e2, e2), e2)
        for copy in gathers[step - 1]:
            copy.wait()
        k = 14 + 2 * step
        tails.append(push(o1.at[at1], o1.at[at1], sem_s.at[k], sem_r.at[k], mate))
        tails.append(push(o2.at[at2], o2.at[at2], sem_s.at[k + 1], sem_r.at[k + 1], mate))
    for copy in scalar:
        copy.wait()
    total = loss[...]
    for step in range(num_dev - 1):
        total = total + lslots[step]
    lo[...] = total
    for copy in tails:
        copy.wait()


def solution(mesh):
    num_dev = mesh.shape[GRAPH_AXIS]
    to_next = [(dev_id, (dev_id + 1) % num_dev) for dev_id in range(num_dev)]
    to_prev = [(dev_id, (dev_id - 1) % num_dev) for dev_id in range(num_dev)]

    def shift_next(a):
        return lax.ppermute(a, GRAPH_AXIS, to_next)

    def shift_prev(a):
        return lax.ppermute(a, GRAPH_AXIS, to_prev)

    def compact(edge_src, edge_dst, edge_w, n_loc):
        rows = edge_src.shape[0] // CHUNK
        src, dst, w = (a.reshape(rows, CHUNK) for a in (edge_src, edge_dst, edge_w))
        live = w != 0.0
        own = live & (src < n_loc)
        hal = live & (src >= n_loc)
        tri = (jnp.arange(CHUNK)[:, None] < jnp.arange(CHUNK)[None, :]).astype(BF16)
        both = jnp.concatenate([own, hal], axis=0).astype(BF16)
        rank = jnp.dot(both, tri, preferred_element_type=F32).astype(jnp.int32)
        place = jnp.where(own, rank[:rows], jnp.where(hal, SLOT - 1 - rank[rows:], SLOT))
        hit = place[:, :, None] == jnp.arange(SLOT)[None, None, :]
        code = jnp.where(src < n_loc, src, src - n_loc) + dst * n_loc
        code = jnp.sum(jnp.where(hit, code[:, :, None], 0), axis=1).reshape(-1)
        wc = jnp.sum(jnp.where(hit, w[:, :, None], 0.0), axis=1).reshape(-1)
        s, d = code % n_loc, code // n_loc
        counts = jnp.sum(both.astype(F32), axis=1).astype(jnp.int32)
        return s, d, s * 4, d * 4, wc, counts[:rows], counts[rows:]

    def device_step(node_feats, w_one, w_two, send_rows, edge_src, edge_dst, edge_w, labels, label_mask):
        n_loc, f_in = node_feats.shape
        halo = send_rows.shape[1]
        f_hid, classes = w_two.shape
        quad = 4 * n_loc
        sds = jax.ShapeDtypeStruct
        x = jnp.pad(node_feats, ((0, 0), (0, 256 - f_in)))
        w1 = jnp.pad(w_one.astype(BF16), ((0, 256 - f_in), (0, 0)))
        w2 = jnp.pad(w_two.astype(BF16), ((0, 0), (0, LANES - classes)))
        ids = jnp.concatenate([send_rows[1], send_rows[0]])
        x_next, x_prev = pl.pallas_call(
            halo_rows_kernel,
            out_shape=[sds((halo, 256), BF16)] * 2,
            in_specs=[SMEM_SPEC, VMEM_SPEC],
            out_specs=[VMEM_SPEC] * 2,
            scratch_shapes=[pltpu.VMEM((2 * n_loc, LANES), F32), pltpu.VMEM((4 * halo, LANES), F32)],
            compiler_params=params(),
            name="halo_rows",
        )(ids * 2, x)
        xh_prev = shift_next(x_next)
        xh_next = shift_prev(x_prev)
        mask_count = jnp.sum(label_mask.astype(F32))
        count = pl.pallas_call(
            functools.partial(count_kernel, num_dev),
            out_shape=sds((8, LANES), F32),
            in_specs=[VMEM_SPEC],
            out_specs=VMEM_SPEC,
            scratch_shapes=[pltpu.VMEM((num_dev - 1, 8, LANES), F32), pltpu.SemaphoreType.DMA((num_dev - 1,)), pltpu.SemaphoreType.DMA((num_dev - 1,))],
            compiler_params=params(collective_id=0, has_side_effects=True),
            name="count",
        )(jnp.broadcast_to(mask_count, (8, LANES)))
        count = jnp.maximum(count, 1.0)
        s, d, s4, d4, wc, n_own, n_hal = compact(edge_src, edge_dst, edge_w, n_loc)
        wide4 = [pltpu.VMEM((quad, LANES), F32)] * 4
        thin4 = [pltpu.VMEM((n_loc, LANES), F32)] * 4
        y_own = pl.pallas_call(
            one_own_kernel,
            out_shape=sds((quad, LANES), F32),
            in_specs=[SMEM_SPEC] * 4 + [VMEM_SPEC] * 2,
            out_specs=VMEM_SPEC,
            scratch_shapes=[pltpu.VMEM((quad, LANES), F32)] + wide4,
            compiler_params=params(),
            cost_estimate=pl.CostEstimate(flops=200000000000, bytes_accessed=8000000, transcendentals=0),
            name="one_own",
        )(s4, d4, wc, n_own, x, w1)
        hid, t2, t_next, t_prev = pl.pallas_call(
            one_halo_kernel,
            out_shape=[sds((n_loc, f_hid), BF16), sds((n_loc, LANES), F32), sds((halo, LANES), BF16), sds((halo, LANES), BF16)],
            in_specs=[SMEM_SPEC] * 5 + [VMEM_SPEC] * 5,
            out_specs=[VMEM_SPEC] * 4,
            scratch_shapes=[pltpu.VMEM((4 * 2 * halo, LANES), F32), pltpu.VMEM((2 * halo, LANES), F32)] + wide4,
            compiler_params=params(),
            name="one_halo",
        )(s4, d4, wc, n_hal, ids, y_own, xh_prev, xh_next, w1, w2)
        th_prev = shift_next(t_next)
        th_next = shift_prev(t_prev)
        narrow_own = functools.partial(
            pl.pallas_call,
            narrow_own_kernel,
            out_shape=sds((n_loc, LANES), F32),
            in_specs=[SMEM_SPEC] * 4 + [VMEM_SPEC],
            out_specs=VMEM_SPEC,
            scratch_shapes=thin4,
            compiler_params=params(),
            cost_estimate=pl.CostEstimate(flops=200000000000, bytes_accessed=8000000, transcendentals=0),
        )
        z_own = narrow_own(name="two_own")(s, d, wc, n_own, t2)
        marks = jnp.broadcast_to(jnp.where(label_mask == 1, labels, -1)[:, None], (n_loc, LANES))
        dz, bz_prev, bz_next, loss = pl.pallas_call(
            functools.partial(logits_kernel, classes),
            out_shape=[sds((n_loc, LANES), F32), sds((halo, LANES), F32), sds((halo, LANES), F32), sds((8, LANES), F32)],
            in_specs=[SMEM_SPEC] * 4 + [VMEM_SPEC] * 5,
            out_specs=[VMEM_SPEC] * 4,
            scratch_shapes=[pltpu.VMEM((2 * halo, LANES), F32)] + thin4,
            compiler_params=params(),
            name="logits",
        )(s, d, wc, n_hal, z_own, th_prev, th_next, marks, count)
        rz_next = shift_prev(bz_prev)
        rz_prev = shift_next(bz_next)
        dt2_own = narrow_own(name="two_back_own")(d, s, wc, n_own, dz)
        dt2, dy, by_prev, by_next = pl.pallas_call(
            hidden_grad_kernel,
            out_shape=[sds((n_loc, LANES), BF16), sds((quad, LANES), F32), sds((4 * halo, LANES), F32), sds((4 * halo, LANES), F32)],
            in_specs=[SMEM_SPEC] * 5 + [VMEM_SPEC] * 5,
            out_specs=[VMEM_SPEC] * 4,
            scratch_shapes=wide4,
            compiler_params=params(),
            name="hidden_grad",
        )(s4, d4, wc, n_hal, ids, dt2_own, rz_next, rz_prev, hid, w2.T)
        ry_next = shift_prev(by_prev)
        ry_prev = shift_next(by_next)
        dt1_own = pl.pallas_call(
            wide_own_kernel,
            out_shape=sds((quad, LANES), F32),
            in_specs=[SMEM_SPEC] * 4 + [VMEM_SPEC],
            out_specs=VMEM_SPEC,
            scratch_shapes=wide4,
            compiler_params=params(),
            cost_estimate=pl.CostEstimate(flops=200000000000, bytes_accessed=8000000, transcendentals=0),
            name="one_back_own",
        )(d4, s4, wc, n_own, dy)
        grad_two = lax.dot_general(hid, dt2, CONTRACT_ROWS, preferred_element_type=F32)
        dt1 = pl.pallas_call(
            table_grad_kernel,
            out_shape=sds((n_loc, f_hid), BF16),
            in_specs=[SMEM_SPEC] + [VMEM_SPEC] * 3,
            out_specs=VMEM_SPEC,
            scratch_shapes=wide4,
            compiler_params=params(),
            name="table_grad",
        )(ids * 4, dt1_own, ry_next, ry_prev)
        grad_one = lax.dot_general(x, dt1, CONTRACT_ROWS, preferred_element_type=F32)
        grad_one, grad_two, loss = pl.pallas_call(
            functools.partial(reduce_kernel, num_dev),
            out_shape=[sds((256, f_hid), F32), sds((f_hid, LANES), F32), sds((8, LANES), F32)],
            in_specs=[VMEM_SPEC] * 3,
            out_specs=[VMEM_SPEC] * 3,
            scratch_shapes=[
                pltpu.VMEM((128, f_hid), F32), pltpu.VMEM((f_hid // 2, LANES), F32),
                pltpu.VMEM((128, f_hid), F32), pltpu.VMEM((f_hid // 2, LANES), F32),
                pltpu.VMEM((3, 32, f_hid), F32), pltpu.VMEM((3, f_hid // 8, LANES), F32),
                pltpu.VMEM((num_dev - 1, 8, LANES), F32),
                pltpu.SemaphoreType.DMA((22,)), pltpu.SemaphoreType.DMA((22,)),
                pltpu.SemaphoreType.DMA((num_dev - 1,)), pltpu.SemaphoreType.DMA((num_dev - 1,)),
            ],
            compiler_params=params(collective_id=1, has_side_effects=True),
            name="reduce",
        )(grad_one, grad_two, loss)
        mean_loss = jnp.sum(loss) / count[0, 0]
        return mean_loss, grad_one[:f_in], grad_two[:, :classes]

    row_spec = P(GRAPH_AXIS)
    return jax.shard_map(device_step, mesh=mesh, in_specs=(row_spec, P(), P(), row_spec, row_spec, row_spec, row_spec, row_spec, row_spec), out_specs=(P(), P(), P()), check_vma=False)
```

```python
import functools

import jax
import jax.numpy as jnp
from jax import lax
from jax.experimental import pallas as pl
from jax.experimental.pallas import tpu as pltpu
from jax.sharding import PartitionSpec as P


GRAPH_AXIS = "graph"
CONTRACT_ROWS = (((0,), (0,)), ((), ()))
MESH = pl.DeviceIdType.MESH
F32 = jnp.float32
BF16 = jnp.bfloat16
LANES = 128
CHUNK = 256
SLOT = 384

SMEM_SPEC = pl.BlockSpec(memory_space=pltpu.SMEM)
VMEM_SPEC = pl.BlockSpec(memory_space=pltpu.VMEM)


def params(mib, **kw):
    return pltpu.CompilerParams(vmem_limit_bytes=mib * 2**20, **kw)


def zero_rows(refs):
    rows = refs[0].shape[0]

    def body(i, _):
        for ref in refs:
            ref[pl.ds(i * 64, 64), :] = jnp.zeros((64, LANES), F32)
        return 0

    lax.fori_loop(0, rows // 64, body, 0)


def sum_rows(out, refs):
    rows = refs[0].shape[0]

    def body(i, _):
        total = refs[0][pl.ds(i * 64, 64), :]
        for ref in refs[1:]:
            total = total + ref[pl.ds(i * 64, 64), :]
        out[pl.ds(i * 64, 64), :] = total
        return 0

    lax.fori_loop(0, rows // 64, body, 0)


def edge_pass(from_ref, to_ref, w_ref, cnt_ref, table, accs, width, unroll, back):
    n_acc = len(accs)
    shift = unroll.bit_length() - 1

    def row(r, _):
        blocks = lax.shift_right_logical(cnt_ref[r] + (unroll - 1), shift)

        def body(j, _):
            off = r * SLOT + (SLOT - unroll - j * unroll if back else j * unroll)
            frm, to, wgt = (ref.at[pl.ds(off, unroll)] for ref in (from_ref, to_ref, w_ref))
            for u in range(unroll):
                acc = accs[u % n_acc]
                val = table[pl.ds(pl.multiple_of(frm[u], width), width), :] * wgt[u]
                at = pl.ds(pl.multiple_of(to[u], width), width)
                acc[at, :] = acc[at, :] + val
            return 0

        lax.fori_loop(0, blocks, body, 0)
        return 0

    lax.fori_loop(0, cnt_ref.shape[0], row, 0)


def scatter_pass(ids_ref, table, accs, width, unroll):
    n_acc = len(accs)

    def body(j, _):
        off = j * unroll
        for g in range(unroll // n_acc):
            rows = [pl.multiple_of(ids_ref[off + g * n_acc + k], width) for k in range(n_acc)]
            vals = [table[pl.ds(pl.multiple_of((off + g * n_acc + k) * width, width), width), :] for k in range(n_acc)]
            old = [accs[k][pl.ds(rows[k], width), :] for k in range(n_acc)]
            for k in range(n_acc):
                accs[k][pl.ds(rows[k], width), :] = old[k] + vals[k]
        return 0

    lax.fori_loop(0, ids_ref.shape[0] // unroll, body, 0)


def gather_pass(ids_ref, table, out, width, unroll=8):
    def body(j, _):
        for u in range(unroll):
            i = j * unroll + u
            out[pl.ds(pl.multiple_of(i * width, width), width), :] = table[pl.ds(pl.multiple_of(ids_ref[i], width), width), :]
        return 0

    lax.fori_loop(0, ids_ref.shape[0] // unroll, body, 0)


def spread(table, start, block):
    tiles = block.shape[1] // LANES
    for c in range(tiles):
        table[pl.ds(start * tiles + c, block.shape[0], tiles), :] = block[:, c * LANES:(c + 1) * LANES]


def unspread(table, start, rows, tiles):
    return jnp.concatenate([table[pl.ds(start * tiles + c, rows, tiles), :] for c in range(tiles)], axis=1)


def enter(me, num_dev):
    barrier = pltpu.get_barrier_semaphore()
    for step in range(1, num_dev):
        pl.semaphore_signal(barrier, inc=1, device_id=(lax.rem(me + step, num_dev),), device_id_type=MESH)
    pl.semaphore_wait(barrier, num_dev - 1)


def push(src, dst, send_sem, recv_sem, dev):
    copy = pltpu.make_async_remote_copy(src_ref=src, dst_ref=dst, send_sem=send_sem, recv_sem=recv_sem, device_id=(dev,), device_id_type=MESH)
    copy.start()
    return copy


def lists_kernel(num_dev, part, code, wgt, count, code_prev, code_next, w_prev, w_next, slots, send_sem, recv_sem, lsend, lrecv):
    me = lax.axis_index(GRAPH_AXIS)
    succ, pred = lax.rem(me + 1, num_dev), lax.rem(me + num_dev - 1, num_dev)
    enter(me, num_dev)
    copies = []
    for step in range(1, num_dev):
        copies.append(push(part, slots.at[step - 1], send_sem.at[step - 1], recv_sem.at[step - 1], lax.rem(me + step, num_dev)))
    copies.append(push(code, code_prev, lsend.at[0], lrecv.at[0], succ))
    copies.append(push(code, code_next, lsend.at[1], lrecv.at[1], pred))
    copies.append(push(wgt, w_prev, lsend.at[2], lrecv.at[2], succ))
    copies.append(push(wgt, w_next, lsend.at[3], lrecv.at[3], pred))
    for copy in copies:
        copy.wait()
    total = part[...]
    for step in range(num_dev - 1):
        total = total + slots[step]
    count[...] = jnp.maximum(total, 1.0)


def halo_rows_kernel(ids2, x, to_next, to_prev, table, picked):
    rows = x.shape[0]

    def put(i, _):
        spread(table, i * 256, x[pl.ds(i * 256, 256), :].astype(F32))
        return 0

    lax.fori_loop(0, rows // 256, put, 0)
    gather_pass(ids2, table, picked, 2)
    half = to_next.shape[0]

    def take(i, _):
        to_next[pl.ds(i * 256, 256), :] = unspread(picked, i * 256, 256, 2).astype(BF16)
        to_prev[pl.ds(i * 256, 256), :] = unspread(picked, half + i * 256, 256, 2).astype(BF16)
        return 0

    lax.fori_loop(0, half // 256, take, 0)


def one_own_kernel(s4, d4, w, cnt, x, w1, y, table, *accs):
    zero_rows(accs)

    def put(i, _):
        t = jnp.dot(x[pl.ds(i * 256, 256), :], w1[...], preferred_element_type=F32)
        spread(table, i * 256, t.astype(BF16).astype(F32))
        return 0

    lax.fori_loop(0, x.shape[0] // 256, put, 0)
    edge_pass(s4, d4, w, cnt, table, accs, 4, 32, False)
    sum_rows(y, accs)


def one_halo_kernel(s4, d4, w, cnt, ids, y_own, x_prev, x_next, w1, w2, hid_a, hid_b, t2, to_next, to_prev, table, picked, *accs):
    zero_rows(accs)
    half = x_prev.shape[0]

    def put(i, _):
        t = jnp.dot(x_prev[pl.ds(i * 256, 256), :], w1[...], preferred_element_type=F32)
        spread(table, i * 256, t.astype(BF16).astype(F32))
        t = jnp.dot(x_next[pl.ds(i * 256, 256), :], w1[...], preferred_element_type=F32)
        spread(table, half + i * 256, t.astype(BF16).astype(F32))
        return 0

    lax.fori_loop(0, half // 256, put, 0)
    edge_pass(s4, d4, w, cnt, table, accs, 4, 8, True)
    sum_rows(accs[0], (y_own,) + accs)

    def act(i, _):
        h = jnp.maximum(unspread(accs[0], i * 256, 256, 4), 0.0).astype(BF16)
        cut = hid_a.shape[1]
        hid_a[pl.ds(i * 256, 256), :] = h[:, :cut]
        hid_b[pl.ds(i * 256, 256), :] = h[:, cut:]
        t = jnp.dot(h, w2[...], preferred_element_type=F32)
        t2[pl.ds(i * 256, 256), :] = t.astype(BF16).astype(F32)
        return 0

    lax.fori_loop(0, t2.shape[0] // 256, act, 0)
    gather_pass(ids, t2, picked, 1)

    def take(i, _):
        to_next[pl.ds(i * 256, 256), :] = picked[pl.ds(i * 256, 256), :].astype(BF16)
        to_prev[pl.ds(i * 256, 256), :] = picked[pl.ds(half + i * 256, 256), :].astype(BF16)
        return 0

    lax.fori_loop(0, half // 256, take, 0)


def narrow_own_kernel(frm, to, w, cnt, table, out, *accs):
    zero_rows(accs)
    edge_pass(frm, to, w, cnt, table, accs, 1, 32, False)
    sum_rows(out, accs)


def wide_own_kernel(frm, to, w, cnt, table, out, *accs):
    zero_rows(accs)
    edge_pass(frm, to, w, cnt, table, accs, 4, 32, False)
    sum_rows(out, accs)


def logits_kernel(classes, s, d, w, cnt, z_own, t_prev, t_next, labels, count, dz, back_prev, back_next, loss, table, *accs):
    zero_rows(accs)
    half = t_prev.shape[0]

    def put(i, _):
        table[pl.ds(i * 256, 256), :] = t_prev[pl.ds(i * 256, 256), :].astype(F32)
        table[pl.ds(half + i * 256, 256), :] = t_next[pl.ds(i * 256, 256), :].astype(F32)
        return 0

    lax.fori_loop(0, half // 256, put, 0)
    edge_pass(s, d, w, cnt, table, accs, 1, 8, True)
    denom = count[0:1, :]
    loss[...] = jnp.zeros_like(loss)

    def soft(i, _):
        at = pl.ds(i * 64, 64)
        z = z_own[at, :]
        for acc in accs:
            z = z + acc[at, :]
        lane = lax.broadcasted_iota(jnp.int32, z.shape, 1)
        lab = labels[at, :]
        hot = lab == lane
        keep = lab >= 0
        zm = jnp.where(lane < classes, z, -jnp.inf)
        top = jnp.max(zm, axis=1, keepdims=True)
        ex = jnp.exp(zm - top)
        log_norm = jnp.log(jnp.sum(ex, axis=1, keepdims=True)) + top
        hot_f = jnp.where(hot, 1.0, 0.0)
        term = jnp.where(hot, log_norm - z, 0.0)
        part = term[0:8]
        for b in range(1, 8):
            part = part + term[b * 8:b * 8 + 8]
        loss[...] += part
        mask_f = jnp.where(keep, 1.0, 0.0)
        dz[at, :] = jnp.where(lane < classes, (jnp.exp(zm - log_norm) - hot_f) * (mask_f / denom), 0.0)
        return 0

    lax.fori_loop(0, dz.shape[0] // 64, soft, 0)
    zero_rows(accs)
    edge_pass(d, s, w, cnt, dz, accs, 1, 8, True)

    def fin(i, _):
        at = pl.ds(i * 64, 64)
        bt = pl.ds(half + i * 64, 64)
        a, b = accs[0][at, :], accs[0][bt, :]
        for acc in accs[1:]:
            a, b = a + acc[at, :], b + acc[bt, :]
        back_prev[at, :] = a
        back_next[at, :] = b
        return 0

    lax.fori_loop(0, half // 64, fin, 0)


def masked(grad, hid_a, hid_b):
    cut = hid_a.shape[1]
    lo = jnp.where(hid_a.astype(F32) > 0.0, grad[:, :cut], 0.0)
    hi = jnp.where(hid_b.astype(F32) > 0.0, grad[:, cut:], 0.0)
    return jnp.concatenate([lo, hi], axis=1)


def hidden_grad_kernel(ids, own, ret_next, ret_prev, hid_a, hid_b, w2t, dt2, dy, *accs):
    n_loc, half = own.shape[0], ret_next.shape[0]
    zero_rows(accs)
    scatter_pass(ids.at[pl.ds(0, half)], ret_next, accs, 1, 8)
    scatter_pass(ids.at[pl.ds(half, half)], ret_prev, accs, 1, 8)

    def fold(i, _):
        at = pl.ds(i * 256, 256)
        total = own[at, :]
        for acc in accs:
            total = total + acc[at, :]
        dt = total.astype(BF16)
        dt2[at, :] = dt
        dh = jnp.dot(dt, w2t[...], preferred_element_type=F32)
        spread(dy, i * 256, masked(dh, hid_a[at, :], hid_b[at, :]))
        return 0

    lax.fori_loop(0, n_loc // 256, fold, 0)


def peer_pass(ids4, code_ref, w_ref, rows, far, table, accs):
    n_acc = len(accs)
    tally = rows * SLOT
    n_loc = ids4.shape[0]
    shift = n_loc.bit_length() - 1

    def row(r, _):
        first = SLOT - 8 - (code_ref[tally + 2 * rows + r] if far else 0)
        edges = code_ref[tally + far * rows + r]

        def body(j, _):
            off = r * SLOT + first - j * 8
            codes, wgt = (ref.at[pl.ds(off, 8)] for ref in (code_ref, w_ref))
            for u in range(8):
                acc = accs[u % n_acc]
                code = codes[u]
                frm = lax.shift_right_logical(code, shift) * 4
                val = table[pl.ds(pl.multiple_of(frm, 4), 4), :] * wgt[u]
                at = pl.ds(pl.multiple_of(ids4[code & (n_loc - 1)], 4), 4)
                acc[at, :] = acc[at, :] + val
            return 0

        lax.fori_loop(0, lax.shift_right_logical(edges + 7, 3), body, 0)
        return 0

    lax.fori_loop(0, rows, row, 0)


def table_grad_kernel(rows, ids4, cn, wn, cp, wp, own, tn, han, hbn, tp, hap, hbp, w2t, dt1, table, *accs):
    zero_rows(accs)

    def fill(dt, hid_a, hid_b):
        def put(i, _):
            at = pl.ds(i * 256, 256)
            dh = jnp.dot(dt[at, :], w2t[...], preferred_element_type=F32)
            spread(table, i * 256, masked(dh, hid_a[at, :], hid_b[at, :]))
            return 0

        lax.fori_loop(0, dt.shape[0] // 256, put, 0)

    fill(tn, han, hbn)
    peer_pass(ids4, cn, wn, rows, 0, table, accs)
    fill(tp, hap, hbp)
    peer_pass(ids4, cp, wp, rows, 1, table, accs)

    def fold(i, _):
        total = unspread(own, i * 128, 128, 4)
        for acc in accs:
            total = total + unspread(acc, i * 128, 128, 4)
        dt1[pl.ds(i * 128, 128), :] = total.astype(BF16)
        return 0

    lax.fori_loop(0, dt1.shape[0] // 128, fold, 0)


def reduce_kernel(num_dev, g1, g2, loss, o1, o2, lo, r1, r2, s1, s2, q1, q2, lslots, sem_s, sem_r, lsem_s, lsem_r):
    me = lax.axis_index(GRAPH_AXIS)
    core = lax.rem(me, 2)
    chip = me // 2
    mate = me + 1 - 2 * core
    h1, h2 = g1.shape[0] // 2, g2.shape[0] // 2
    e1, e2 = h1 // 4, h2 // 4
    enter(me, num_dev)
    other = 1 - core
    pair = [
        push(g1.at[pl.ds(pl.multiple_of(other * h1, h1), h1)], r1, sem_s.at[0], sem_r.at[0], mate),
        push(g2.at[pl.ds(pl.multiple_of(other * h2, h2), h2)], r2, sem_s.at[1], sem_r.at[1], mate),
    ]
    scalar = []
    for step in range(1, num_dev):
        scalar.append(push(loss, lslots.at[step - 1], lsem_s.at[step - 1], lsem_r.at[step - 1], lax.rem(me + step, num_dev)))
    for copy in pair:
        copy.wait()
    s1[...] = g1[pl.ds(pl.multiple_of(core * h1, h1), h1), :] + r1[...]
    s2[...] = g2[pl.ds(pl.multiple_of(core * h2, h2), h2), :] + r2[...]
    spreads = []
    for step in range(1, 4):
        far = lax.rem(chip + step, 4)
        dev = far * 2 + core
        k = 2 * step
        spreads.append(push(s1.at[pl.ds(pl.multiple_of(far * e1, e1), e1)], q1.at[step - 1], sem_s.at[k], sem_r.at[k], dev))
        spreads.append(push(s2.at[pl.ds(pl.multiple_of(far * e2, e2), e2)], q2.at[step - 1], sem_s.at[k + 1], sem_r.at[k + 1], dev))
    for copy in spreads:
        copy.wait()
    mine1 = pl.ds(pl.multiple_of(core * h1 + chip * e1, e1), e1)
    mine2 = pl.ds(pl.multiple_of(core * h2 + chip * e2, e2), e2)
    t1 = s1[pl.ds(pl.multiple_of(chip * e1, e1), e1), :]
    t2 = s2[pl.ds(pl.multiple_of(chip * e2, e2), e2), :]
    for step in range(3):
        t1 = t1 + q1[step]
        t2 = t2 + q2[step]
    o1[mine1, :] = t1
    o2[mine2, :] = t2
    gathers = []
    for step in range(1, 4):
        dev = lax.rem(chip + step, 4) * 2 + core
        k = 6 + 2 * step
        gathers.append((push(o1.at[mine1], o1.at[mine1], sem_s.at[k], sem_r.at[k], dev), push(o2.at[mine2], o2.at[mine2], sem_s.at[k + 1], sem_r.at[k + 1], dev)))
    tails = [push(o1.at[mine1], o1.at[mine1], sem_s.at[14], sem_r.at[14], mate), push(o2.at[mine2], o2.at[mine2], sem_s.at[15], sem_r.at[15], mate)]
    for step in range(1, 4):
        near = lax.rem(chip + 4 - step, 4)
        at1 = pl.ds(pl.multiple_of(core * h1 + near * e1, e1), e1)
        at2 = pl.ds(pl.multiple_of(core * h2 + near * e2, e2), e2)
        for copy in gathers[step - 1]:
            copy.wait()
        k = 14 + 2 * step
        tails.append(push(o1.at[at1], o1.at[at1], sem_s.at[k], sem_r.at[k], mate))
        tails.append(push(o2.at[at2], o2.at[at2], sem_s.at[k + 1], sem_r.at[k + 1], mate))
    for copy in scalar:
        copy.wait()
    total = loss[...]
    for step in range(num_dev - 1):
        total = total + lslots[step]
    lo[...] = total
    for copy in tails:
        copy.wait()


def solution(mesh):
    num_dev = mesh.shape[GRAPH_AXIS]
    to_next = [(dev_id, (dev_id + 1) % num_dev) for dev_id in range(num_dev)]
    to_prev = [(dev_id, (dev_id - 1) % num_dev) for dev_id in range(num_dev)]

    def shift_next(a):
        return lax.ppermute(a, GRAPH_AXIS, to_next)

    def shift_prev(a):
        return lax.ppermute(a, GRAPH_AXIS, to_prev)

    def compact(edge_src, edge_dst, edge_w, n_loc, halo):
        rows = edge_src.shape[0] // CHUNK
        src, dst, w = (a.reshape(rows, CHUNK) for a in (edge_src, edge_dst, edge_w))
        live = w != 0.0
        own = live & (src < n_loc)
        far = live & (src >= n_loc + halo)
        near = live & (src >= n_loc) & (src < n_loc + halo)
        tri = (jnp.arange(CHUNK)[:, None] < jnp.arange(CHUNK)[None, :]).astype(BF16)
        sets = jnp.concatenate([own, near, far], axis=0).astype(BF16)
        rank = jnp.dot(sets, tri, preferred_element_type=F32).astype(jnp.int32)
        counts = jnp.sum(sets.astype(F32), axis=1).astype(jnp.int32)
        n_own, n_near, n_far = counts[:rows], counts[rows:2 * rows], counts[2 * rows:]
        skip = (n_near + 7) // 8 * 8
        place = jnp.where(far, SLOT - 1 - skip[:, None] - rank[2 * rows:], SLOT)
        place = jnp.where(near, SLOT - 1 - rank[rows:2 * rows], place)
        place = jnp.where(own, rank[:rows], place)
        hit = place[:, :, None] == jnp.arange(SLOT)[None, None, :]
        code = jnp.where(src < n_loc, src, src - n_loc) + dst * n_loc
        code = jnp.sum(jnp.where(hit, code[:, :, None], 0), axis=1)
        wc = jnp.sum(jnp.where(hit, w[:, :, None], 0.0), axis=1)
        n_hal = jnp.where(n_far > 0, skip + n_far, n_near)
        return code, wc, n_own, n_hal, n_near, n_far, skip

    def device_step(node_feats, w_one, w_two, send_rows, edge_src, edge_dst, edge_w, labels, label_mask):
        n_loc, f_in = node_feats.shape
        halo = send_rows.shape[1]
        f_hid, classes = w_two.shape
        quad = 4 * n_loc
        sds = jax.ShapeDtypeStruct
        x = jnp.pad(node_feats, ((0, 0), (0, 256 - f_in)))
        w1 = jnp.pad(w_one.astype(BF16), ((0, 256 - f_in), (0, 0)))
        w2 = jnp.pad(w_two.astype(BF16), ((0, 0), (0, LANES - classes)))
        ids = jnp.concatenate([send_rows[1], send_rows[0]])
        mask_count = jnp.sum(label_mask.astype(F32))
        code, wc, n_own, n_hal, n_near, n_far, skip = compact(edge_src, edge_dst, edge_w, n_loc, halo)
        rows = n_own.shape[0]
        slots = code.size // LANES
        code, wc = code.reshape(-1), wc.reshape(-1)
        tally = jnp.concatenate([n_near, n_far, skip, jnp.zeros((8 * LANES - 3 * rows,), jnp.int32)])
        lists = jnp.concatenate([code, tally]).reshape(slots + 8, LANES)
        count, code_prev, code_next, w_prev, w_next = pl.pallas_call(
            functools.partial(lists_kernel, num_dev),
            out_shape=[sds((8, LANES), F32)] + [sds((slots + 8, LANES), jnp.int32)] * 2 + [sds((slots, LANES), F32)] * 2,
            in_specs=[VMEM_SPEC] * 3,
            out_specs=[VMEM_SPEC] * 5,
            scratch_shapes=[pltpu.VMEM((num_dev - 1, 8, LANES), F32)] + [pltpu.SemaphoreType.DMA((n,)) for n in (num_dev - 1, num_dev - 1, 4, 4)],
            compiler_params=params(1, collective_id=0, has_side_effects=True),
            name="lists",
        )(jnp.broadcast_to(mask_count, (8, LANES)), lists, wc.reshape(slots, LANES))
        s, d = code % n_loc, code // n_loc
        s4, d4 = s * 4, d * 4
        count, x_src = lax.optimization_barrier((count, x))
        x_next, x_prev = pl.pallas_call(
            halo_rows_kernel,
            out_shape=[sds((halo, 256), BF16)] * 2,
            in_specs=[SMEM_SPEC, VMEM_SPEC],
            out_specs=[VMEM_SPEC] * 2,
            scratch_shapes=[pltpu.VMEM((2 * n_loc, LANES), F32), pltpu.VMEM((4 * halo, LANES), F32)],
            compiler_params=params(12),
            name="halo_rows",
        )(ids * 2, x_src)
        xh_prev = shift_next(x_next)
        xh_next = shift_prev(x_prev)
        wide4 = [pltpu.VMEM((quad, LANES), F32)] * 4
        thin4 = [pltpu.VMEM((n_loc, LANES), F32)] * 4
        y_own = pl.pallas_call(
            one_own_kernel,
            out_shape=sds((quad, LANES), F32),
            in_specs=[SMEM_SPEC] * 4 + [VMEM_SPEC] * 2,
            out_specs=VMEM_SPEC,
            scratch_shapes=[pltpu.VMEM((quad, LANES), F32)] + wide4,
            compiler_params=params(28),
            cost_estimate=pl.CostEstimate(flops=200000000000, bytes_accessed=8000000, transcendentals=0),
            name="one_own",
        )(s4, d4, wc, n_own, x, w1)
        hid_a, hid_b, t2, t_next, t_prev = pl.pallas_call(
            one_halo_kernel,
            out_shape=[sds((n_loc, f_hid // 2), BF16)] * 2 + [sds((n_loc, LANES), F32), sds((halo, LANES), BF16), sds((halo, LANES), BF16)],
            in_specs=[SMEM_SPEC] * 5 + [VMEM_SPEC] * 5,
            out_specs=[VMEM_SPEC] * 5,
            scratch_shapes=[pltpu.VMEM((4 * 2 * halo, LANES), F32), pltpu.VMEM((2 * halo, LANES), F32)] + wide4,
            compiler_params=params(30),
            name="one_halo",
        )(s4, d4, wc, n_hal, ids, y_own, xh_prev, xh_next, w1, w2)
        th_prev = shift_next(t_next)
        th_next = shift_prev(t_prev)
        ha_prev, ha_next = shift_next(hid_a), shift_prev(hid_a)
        narrow_own = functools.partial(
            pl.pallas_call,
            narrow_own_kernel,
            out_shape=sds((n_loc, LANES), F32),
            in_specs=[SMEM_SPEC] * 4 + [VMEM_SPEC],
            out_specs=VMEM_SPEC,
            scratch_shapes=thin4,
            compiler_params=params(10),
            cost_estimate=pl.CostEstimate(flops=200000000000, bytes_accessed=8000000, transcendentals=0),
        )
        z_own = narrow_own(name="two_own")(s, d, wc, n_own, t2)
        marks = jnp.broadcast_to(jnp.where(label_mask == 1, labels, -1)[:, None], (n_loc, LANES))
        dz, bz_prev, bz_next, loss = pl.pallas_call(
            functools.partial(logits_kernel, classes),
            out_shape=[sds((n_loc, LANES), F32), sds((halo, LANES), F32), sds((halo, LANES), F32), sds((8, LANES), F32)],
            in_specs=[SMEM_SPEC] * 4 + [VMEM_SPEC] * 5,
            out_specs=[VMEM_SPEC] * 4,
            scratch_shapes=[pltpu.VMEM((2 * halo, LANES), F32)] + thin4,
            compiler_params=params(12),
            name="logits",
        )(s, d, wc, n_hal, z_own, th_prev, th_next, marks, count)
        rz_next = shift_prev(bz_prev)
        rz_prev = shift_next(bz_next)
        late_b, _ = lax.optimization_barrier((hid_b, bz_prev))
        hb_prev, hb_next = shift_next(late_b), shift_prev(late_b)
        dt2_own = narrow_own(name="two_back_own")(d, s, wc, n_own, dz)
        w2t = w2.T
        dt2, dy = pl.pallas_call(
            hidden_grad_kernel,
            out_shape=[sds((n_loc, LANES), BF16), sds((quad, LANES), F32)],
            in_specs=[SMEM_SPEC] + [VMEM_SPEC] * 6,
            out_specs=[VMEM_SPEC] * 2,
            scratch_shapes=thin4,
            compiler_params=params(16),
            name="hidden_grad",
        )(ids, dt2_own, rz_next, rz_prev, hid_a, hid_b, w2t)
        dt_prev, dt_next = shift_next(dt2), shift_prev(dt2)
        dt1_own = pl.pallas_call(
            wide_own_kernel,
            out_shape=sds((quad, LANES), F32),
            in_specs=[SMEM_SPEC] * 4 + [VMEM_SPEC],
            out_specs=VMEM_SPEC,
            scratch_shapes=wide4,
            compiler_params=params(28),
            cost_estimate=pl.CostEstimate(flops=200000000000, bytes_accessed=8000000, transcendentals=0),
            name="one_back_own",
        )(d4, s4, wc, n_own, dy)
        grad_two = jnp.concatenate([lax.dot_general(h, dt2, CONTRACT_ROWS, preferred_element_type=F32) for h in (hid_a, hid_b)])
        dt1 = pl.pallas_call(
            functools.partial(table_grad_kernel, rows),
            out_shape=sds((n_loc, f_hid), BF16),
            in_specs=[SMEM_SPEC] * 5 + [VMEM_SPEC] * 8,
            out_specs=VMEM_SPEC,
            scratch_shapes=[pltpu.VMEM((quad, LANES), F32)] + wide4,
            compiler_params=params(40),
            name="table_grad",
        )(ids * 4, code_next.reshape(-1), w_next.reshape(-1), code_prev.reshape(-1), w_prev.reshape(-1), dt1_own, dt_next, ha_next, hb_next, dt_prev, ha_prev, hb_prev, w2t)
        grad_one = lax.dot_general(x, dt1, CONTRACT_ROWS, preferred_element_type=F32)
        grad_one, grad_two, loss = pl.pallas_call(
            functools.partial(reduce_kernel, num_dev),
            out_shape=[sds((256, f_hid), F32), sds((f_hid, LANES), F32), sds((8, LANES), F32)],
            in_specs=[VMEM_SPEC] * 3,
            out_specs=[VMEM_SPEC] * 3,
            scratch_shapes=[
                pltpu.VMEM((128, f_hid), F32), pltpu.VMEM((f_hid // 2, LANES), F32),
                pltpu.VMEM((128, f_hid), F32), pltpu.VMEM((f_hid // 2, LANES), F32),
                pltpu.VMEM((3, 32, f_hid), F32), pltpu.VMEM((3, f_hid // 8, LANES), F32),
                pltpu.VMEM((num_dev - 1, 8, LANES), F32),
                pltpu.SemaphoreType.DMA((22,)), pltpu.SemaphoreType.DMA((22,)),
                pltpu.SemaphoreType.DMA((num_dev - 1,)), pltpu.SemaphoreType.DMA((num_dev - 1,)),
            ],
            compiler_params=params(8, collective_id=1, has_side_effects=True),
            name="reduce",
        )(grad_one, grad_two, loss)
        mean_loss = jnp.sum(loss) / count[0, 0]
        return mean_loss, grad_one[:f_in], grad_two[:, :classes]

    row_spec = P(GRAPH_AXIS)
    return jax.shard_map(device_step, mesh=mesh, in_specs=(row_spec, P(), P(), row_spec, row_spec, row_spec, row_spec, row_spec, row_spec), out_specs=(P(), P(), P()), check_vma=False)
```

```python
import functools

import jax
import jax.numpy as jnp
from jax import lax
from jax.experimental import pallas as pl
from jax.experimental.pallas import tpu as pltpu
from jax.sharding import PartitionSpec as P


GRAPH_AXIS = "graph"
CONTRACT_ROWS = (((0,), (0,)), ((), ()))
CONTRACT_COLS = (((1,), (1,)), ((), ()))
MESH = pl.DeviceIdType.MESH
F32 = jnp.float32
BF16 = jnp.bfloat16
LANES = 128
CHUNK = 256
SLOT = 384

SMEM_SPEC = pl.BlockSpec(memory_space=pltpu.SMEM)
VMEM_SPEC = pl.BlockSpec(memory_space=pltpu.VMEM)


def params(mib, **kw):
    return pltpu.CompilerParams(vmem_limit_bytes=mib * 2**20, **kw)


def zero_rows(refs):
    rows = refs[0].shape[0]

    def body(i, _):
        for ref in refs:
            ref[pl.ds(i * 64, 64), :] = jnp.zeros((64, LANES), F32)
        return 0

    lax.fori_loop(0, rows // 64, body, 0)


def sum_rows(out, refs):
    rows = refs[0].shape[0]

    def body(i, _):
        total = refs[0][pl.ds(i * 64, 64), :]
        for ref in refs[1:]:
            total = total + ref[pl.ds(i * 64, 64), :]
        out[pl.ds(i * 64, 64), :] = total
        return 0

    lax.fori_loop(0, rows // 64, body, 0)


def edge_pass(from_ref, to_ref, w_ref, cnt_ref, table, accs, width, unroll, back):
    n_acc = len(accs)
    shift = unroll.bit_length() - 1

    def row(r, _):
        blocks = lax.shift_right_logical(cnt_ref[r] + (unroll - 1), shift)

        def body(j, _):
            off = r * SLOT + (SLOT - unroll - j * unroll if back else j * unroll)
            vals = [table[pl.ds(pl.multiple_of(from_ref[off + u], width), width), :] * w_ref[off + u] for u in range(unroll)]
            for g in range(unroll // n_acc):
                rows = [pl.multiple_of(to_ref[off + g * n_acc + k], width) for k in range(n_acc)]
                old = [accs[k][pl.ds(rows[k], width), :] for k in range(n_acc)]
                for k in range(n_acc):
                    accs[k][pl.ds(rows[k], width), :] = old[k] + vals[g * n_acc + k]
            return 0

        lax.fori_loop(0, blocks, body, 0)
        return 0

    lax.fori_loop(0, cnt_ref.shape[0], row, 0)


def scatter_pass(ids_ref, table, accs, width, unroll):
    n_acc = len(accs)

    def body(j, _):
        off = j * unroll
        for g in range(unroll // n_acc):
            rows = [pl.multiple_of(ids_ref[off + g * n_acc + k], width) for k in range(n_acc)]
            vals = [table[pl.ds(pl.multiple_of((off + g * n_acc + k) * width, width), width), :] for k in range(n_acc)]
            old = [accs[k][pl.ds(rows[k], width), :] for k in range(n_acc)]
            for k in range(n_acc):
                accs[k][pl.ds(rows[k], width), :] = old[k] + vals[k]
        return 0

    lax.fori_loop(0, ids_ref.shape[0] // unroll, body, 0)


def gather_pass(ids_ref, table, out, width, unroll=8):
    def body(j, _):
        for u in range(unroll):
            i = j * unroll + u
            out[pl.ds(pl.multiple_of(i * width, width), width), :] = table[pl.ds(pl.multiple_of(ids_ref[i], width), width), :]
        return 0

    lax.fori_loop(0, ids_ref.shape[0] // unroll, body, 0)


def spread(table, start, block):
    tiles = block.shape[1] // LANES
    for c in range(tiles):
        table[pl.ds(start * tiles + c, block.shape[0], tiles), :] = block[:, c * LANES:(c + 1) * LANES]


def unspread(table, start, rows, tiles):
    return jnp.concatenate([table[pl.ds(start * tiles + c, rows, tiles), :] for c in range(tiles)], axis=1)


def enter(me, num_dev):
    barrier = pltpu.get_barrier_semaphore()
    for step in range(1, num_dev):
        pl.semaphore_signal(barrier, inc=1, device_id=(lax.rem(me + step, num_dev),), device_id_type=MESH)
    pl.semaphore_wait(barrier, num_dev - 1)


def push(src, dst, send_sem, recv_sem, dev):
    copy = pltpu.make_async_remote_copy(src_ref=src, dst_ref=dst, send_sem=send_sem, recv_sem=recv_sem, device_id=(dev,), device_id_type=MESH)
    copy.start()
    return copy


def lists_kernel(num_dev, mask, code, wgt, count, code_prev, code_next, w_prev, w_next, part, slots, send_sem, recv_sem, lsend, lrecv):
    ones = jnp.sum(jnp.sum(mask[...].astype(F32), axis=1, keepdims=True), axis=0, keepdims=True)
    part[...] = jnp.broadcast_to(ones, part.shape)
    me = lax.axis_index(GRAPH_AXIS)
    succ, pred = lax.rem(me + 1, num_dev), lax.rem(me + num_dev - 1, num_dev)
    enter(me, num_dev)
    copies = []
    for step in range(1, num_dev):
        copies.append(push(part, slots.at[step - 1], send_sem.at[step - 1], recv_sem.at[step - 1], lax.rem(me + step, num_dev)))
    copies.append(push(code, code_prev, lsend.at[0], lrecv.at[0], succ))
    copies.append(push(code, code_next, lsend.at[1], lrecv.at[1], pred))
    copies.append(push(wgt, w_prev, lsend.at[2], lrecv.at[2], succ))
    copies.append(push(wgt, w_next, lsend.at[3], lrecv.at[3], pred))
    for copy in copies:
        copy.wait()
    total = part[...]
    for step in range(num_dev - 1):
        total = total + slots[step]
    count[...] = jnp.maximum(total, 1.0)


def halo_rows_kernel(ids2, x, to_next, to_prev, table, picked):
    rows = x.shape[0]

    def put(i, _):
        block = x[pl.ds(i * 256, 256), :].astype(F32)
        pad = jnp.zeros((256, 2 * LANES - block.shape[1]), F32)
        spread(table, i * 256, jnp.concatenate([block, pad], axis=1))
        return 0

    lax.fori_loop(0, rows // 256, put, 0)
    gather_pass(ids2, table, picked, 2)
    half = to_next.shape[0]

    def take(i, _):
        to_next[pl.ds(i * 256, 256), :] = unspread(picked, i * 256, 256, 2).astype(BF16)
        to_prev[pl.ds(i * 256, 256), :] = unspread(picked, half + i * 256, 256, 2).astype(BF16)
        return 0

    lax.fori_loop(0, half // 256, take, 0)


def one_own_kernel(s4, d4, w, cnt, x, w1, y, table, *accs):
    zero_rows(accs)

    def put(i, _):
        t = jnp.dot(x[pl.ds(i * 256, 256), :], w1[...], preferred_element_type=F32)
        spread(table, i * 256, t.astype(BF16).astype(F32))
        return 0

    lax.fori_loop(0, x.shape[0] // 256, put, 0)
    edge_pass(s4, d4, w, cnt, table, accs, 4, 16, False)
    sum_rows(y, accs)


def one_halo_kernel(s4, d4, w, cnt, ids, y_own, x_prev, x_next, w1, w2t, hid_a, hid_b, t2, to_next, to_prev, table, picked, *accs):
    zero_rows(accs)
    half = x_prev.shape[0]

    def put(i, _):
        t = jnp.dot(x_prev[pl.ds(i * 256, 256), :w1.shape[0]], w1[...], preferred_element_type=F32)
        spread(table, i * 256, t.astype(BF16).astype(F32))
        t = jnp.dot(x_next[pl.ds(i * 256, 256), :w1.shape[0]], w1[...], preferred_element_type=F32)
        spread(table, half + i * 256, t.astype(BF16).astype(F32))
        return 0

    lax.fori_loop(0, half // 256, put, 0)
    edge_pass(s4, d4, w, cnt, table, accs, 4, 16, True)
    sum_rows(accs[0], (y_own,) + accs)

    def act(i, _):
        h = jnp.maximum(unspread(accs[0], i * 256, 256, 4), 0.0).astype(BF16)
        cut = hid_a.shape[1]
        hid_a[pl.ds(i * 256, 256), :] = h[:, :cut]
        hid_b[pl.ds(i * 256, 256), :] = h[:, cut:]
        t = lax.dot_general(h, w2t[...], CONTRACT_COLS, preferred_element_type=F32)
        t2[pl.ds(i * 256, 256), :] = t.astype(BF16).astype(F32)
        return 0

    lax.fori_loop(0, t2.shape[0] // 256, act, 0)
    gather_pass(ids, t2, picked, 1)

    def take(i, _):
        to_next[pl.ds(i * 256, 256), :] = picked[pl.ds(i * 256, 256), :].astype(BF16)
        to_prev[pl.ds(i * 256, 256), :] = picked[pl.ds(half + i * 256, 256), :].astype(BF16)
        return 0

    lax.fori_loop(0, half // 256, take, 0)


def narrow_own_kernel(frm, to, w, cnt, table, out, *accs):
    zero_rows(accs)
    edge_pass(frm, to, w, cnt, table, accs, 1, 16, False)
    sum_rows(out, accs)


def wide_own_kernel(frm, to, w, cnt, table, out, *accs):
    zero_rows(accs)
    edge_pass(frm, to, w, cnt, table, accs, 4, 16, False)
    sum_rows(out, accs)


def logits_kernel(classes, s, d, w, cnt, z_own, t_prev, t_next, labels, count, dz, back_prev, back_next, loss, table, *accs):
    zero_rows(accs)
    half = t_prev.shape[0]

    def put(i, _):
        table[pl.ds(i * 256, 256), :] = t_prev[pl.ds(i * 256, 256), :].astype(F32)
        table[pl.ds(half + i * 256, 256), :] = t_next[pl.ds(i * 256, 256), :].astype(F32)
        return 0

    lax.fori_loop(0, half // 256, put, 0)
    edge_pass(s, d, w, cnt, table, accs, 1, 16, True)
    denom = count[0:1, :]
    loss[...] = jnp.zeros_like(loss)

    def soft(i, _):
        at = pl.ds(i * 64, 64)
        z = z_own[at, :]
        for acc in accs:
            z = z + acc[at, :]
        lane = lax.broadcasted_iota(jnp.int32, z.shape, 1)
        lab = labels[at, :]
        hot = lab == lane
        keep = lab >= 0
        zm = jnp.where(lane < classes, z, -jnp.inf)
        top = jnp.max(zm, axis=1, keepdims=True)
        ex = jnp.exp(zm - top)
        log_norm = jnp.log(jnp.sum(ex, axis=1, keepdims=True)) + top
        hot_f = jnp.where(hot, 1.0, 0.0)
        term = jnp.where(hot, log_norm - z, 0.0)
        part = term[0:8]
        for b in range(1, 8):
            part = part + term[b * 8:b * 8 + 8]
        loss[...] += part
        mask_f = jnp.where(keep, 1.0, 0.0)
        dz[at, :] = jnp.where(lane < classes, (jnp.exp(zm - log_norm) - hot_f) * (mask_f / denom), 0.0)
        return 0

    lax.fori_loop(0, dz.shape[0] // 64, soft, 0)
    zero_rows(accs)
    edge_pass(d, s, w, cnt, dz, accs, 1, 16, True)

    def fin(i, _):
        at = pl.ds(i * 64, 64)
        bt = pl.ds(half + i * 64, 64)
        a, b = accs[0][at, :], accs[0][bt, :]
        for acc in accs[1:]:
            a, b = a + acc[at, :], b + acc[bt, :]
        back_prev[at, :] = a
        back_next[at, :] = b
        return 0

    lax.fori_loop(0, half // 64, fin, 0)


def masked(grad, hid_a, hid_b):
    cut = hid_a.shape[1]
    lo = jnp.where(hid_a.astype(F32) > 0.0, grad[:, :cut], 0.0)
    hi = jnp.where(hid_b.astype(F32) > 0.0, grad[:, cut:], 0.0)
    return jnp.concatenate([lo, hi], axis=1)


def hidden_grad_kernel(ids, own, ret_next, ret_prev, hid_a, hid_b, w2t, dt2, dy, g2, *accs):
    n_loc, half = own.shape[0], ret_next.shape[0]
    zero_rows(accs)
    scatter_pass(ids.at[pl.ds(0, half)], ret_next, accs, 1, 8)
    scatter_pass(ids.at[pl.ds(half, half)], ret_prev, accs, 1, 8)
    g2[...] = jnp.zeros_like(g2)

    def fold(i, _):
        at = pl.ds(i * 256, 256)
        total = own[at, :]
        for acc in accs:
            total = total + acc[at, :]
        dt = total.astype(BF16)
        dt2[at, :] = dt
        cut = hid_a.shape[1]
        g2[:cut, :] += lax.dot_general(hid_a[at, :], dt, CONTRACT_ROWS, preferred_element_type=F32)
        g2[cut:, :] += lax.dot_general(hid_b[at, :], dt, CONTRACT_ROWS, preferred_element_type=F32)
        dh = jnp.dot(dt, w2t[...], preferred_element_type=F32)
        spread(dy, i * 256, masked(dh, hid_a[at, :], hid_b[at, :]))
        return 0

    lax.fori_loop(0, n_loc // 256, fold, 0)


def peer_pass(ids4, code_ref, w_ref, rows, far, table, accs):
    n_acc = len(accs)
    tally = rows * SLOT
    n_loc = ids4.shape[0]
    shift = n_loc.bit_length() - 1

    def row(r, _):
        first = SLOT - 16 - (code_ref[tally + 2 * rows + r] if far else 0)
        edges = code_ref[tally + far * rows + r]

        def body(j, _):
            off = r * SLOT + first - j * 16
            codes, wgt = (ref.at[pl.ds(off, 16)] for ref in (code_ref, w_ref))
            for u in range(16):
                acc = accs[u % n_acc]
                code = codes[u]
                frm = lax.shift_right_logical(code, shift) * 4
                val = table[pl.ds(pl.multiple_of(frm, 4), 4), :] * wgt[u]
                at = pl.ds(pl.multiple_of(ids4[code & (n_loc - 1)], 4), 4)
                acc[at, :] = acc[at, :] + val
            return 0

        lax.fori_loop(0, lax.shift_right_logical(edges + 15, 4), body, 0)
        return 0

    lax.fori_loop(0, rows, row, 0)


def table_grad_kernel(rows, ids4, cn, wn, cp, wp, own, tn, han, hbn, tp, hap, hbp, w2t, x, g1, table, *accs):
    zero_rows(accs)
    g1[...] = jnp.zeros_like(g1)

    def fill(dt, hid_a, hid_b):
        def put(i, _):
            at = pl.ds(i * 256, 256)
            dh = jnp.dot(dt[at, :], w2t[...], preferred_element_type=F32)
            spread(table, i * 256, masked(dh, hid_a[at, :], hid_b[at, :]))
            return 0

        lax.fori_loop(0, dt.shape[0] // 256, put, 0)

    fill(tn, han, hbn)
    peer_pass(ids4, cn, wn, rows, 0, table, accs)
    fill(tp, hap, hbp)
    peer_pass(ids4, cp, wp, rows, 1, table, accs)

    def fold(i, _):
        total = unspread(own, i * 256, 256, 4)
        for acc in accs:
            total = total + unspread(acc, i * 256, 256, 4)
        g1[:x.shape[1], :] += lax.dot_general(x[pl.ds(i * 256, 256), :], total.astype(BF16), CONTRACT_ROWS, preferred_element_type=F32)
        return 0

    lax.fori_loop(0, x.shape[0] // 256, fold, 0)


def reduce_kernel(num_dev, g1, g2, loss, o1, o2, lo, r1, r2, s1, s2, q1, q2, lslots, sem_s, sem_r, lsem_s, lsem_r):
    me = lax.axis_index(GRAPH_AXIS)
    core = lax.rem(me, 2)
    chip = me // 2
    mate = me + 1 - 2 * core
    h1, h2 = g1.shape[0] // 2, g2.shape[0] // 2
    e1, e2 = h1 // 4, h2 // 4
    enter(me, num_dev)
    other = 1 - core
    pair = [
        push(g1.at[pl.ds(pl.multiple_of(other * h1, h1), h1)], r1, sem_s.at[0], sem_r.at[0], mate),
        push(g2.at[pl.ds(pl.multiple_of(other * h2, h2), h2)], r2, sem_s.at[1], sem_r.at[1], mate),
    ]
    scalar = []
    for step in range(1, num_dev):
        scalar.append(push(loss, lslots.at[step - 1], lsem_s.at[step - 1], lsem_r.at[step - 1], lax.rem(me + step, num_dev)))
    for copy in pair:
        copy.wait()
    s1[...] = g1[pl.ds(pl.multiple_of(core * h1, h1), h1), :] + r1[...]
    s2[...] = g2[pl.ds(pl.multiple_of(core * h2, h2), h2), :] + r2[...]
    spreads = []
    for step in range(1, 4):
        far = lax.rem(chip + step, 4)
        dev = far * 2 + core
        k = 2 * step
        spreads.append(push(s1.at[pl.ds(pl.multiple_of(far * e1, e1), e1)], q1.at[step - 1], sem_s.at[k], sem_r.at[k], dev))
        spreads.append(push(s2.at[pl.ds(pl.multiple_of(far * e2, e2), e2)], q2.at[step - 1], sem_s.at[k + 1], sem_r.at[k + 1], dev))
    for copy in spreads:
        copy.wait()
    mine1 = pl.ds(pl.multiple_of(core * h1 + chip * e1, e1), e1)
    mine2 = pl.ds(pl.multiple_of(core * h2 + chip * e2, e2), e2)
    t1 = s1[pl.ds(pl.multiple_of(chip * e1, e1), e1), :]
    t2 = s2[pl.ds(pl.multiple_of(chip * e2, e2), e2), :]
    for step in range(3):
        t1 = t1 + q1[step]
        t2 = t2 + q2[step]
    o1[mine1, :] = t1
    o2[mine2, :] = t2
    gathers = []
    for step in range(1, 4):
        dev = lax.rem(chip + step, 4) * 2 + core
        k = 6 + 2 * step
        gathers.append((push(o1.at[mine1], o1.at[mine1], sem_s.at[k], sem_r.at[k], dev), push(o2.at[mine2], o2.at[mine2], sem_s.at[k + 1], sem_r.at[k + 1], dev)))
    tails = [push(o1.at[mine1], o1.at[mine1], sem_s.at[14], sem_r.at[14], mate), push(o2.at[mine2], o2.at[mine2], sem_s.at[15], sem_r.at[15], mate)]
    for step in range(1, 4):
        near = lax.rem(chip + 4 - step, 4)
        at1 = pl.ds(pl.multiple_of(core * h1 + near * e1, e1), e1)
        at2 = pl.ds(pl.multiple_of(core * h2 + near * e2, e2), e2)
        for copy in gathers[step - 1]:
            copy.wait()
        k = 14 + 2 * step
        tails.append(push(o1.at[at1], o1.at[at1], sem_s.at[k], sem_r.at[k], mate))
        tails.append(push(o2.at[at2], o2.at[at2], sem_s.at[k + 1], sem_r.at[k + 1], mate))
    for copy in scalar:
        copy.wait()
    total = loss[...]
    for step in range(num_dev - 1):
        total = total + lslots[step]
    lo[...] = total
    for copy in tails:
        copy.wait()


def solution(mesh):
    num_dev = mesh.shape[GRAPH_AXIS]
    to_next = [(dev_id, (dev_id + 1) % num_dev) for dev_id in range(num_dev)]
    to_prev = [(dev_id, (dev_id - 1) % num_dev) for dev_id in range(num_dev)]

    def shift_next(a):
        return lax.ppermute(a, GRAPH_AXIS, to_next)

    def shift_prev(a):
        return lax.ppermute(a, GRAPH_AXIS, to_prev)

    def compact(edge_src, edge_dst, edge_w, n_loc, halo):
        rows = edge_src.shape[0] // CHUNK
        src, dst, w = (a.reshape(rows, CHUNK) for a in (edge_src, edge_dst, edge_w))
        live = w != 0.0
        own = live & (src < n_loc)
        far = live & (src >= n_loc + halo)
        near = live & (src >= n_loc) & (src < n_loc + halo)
        tri = (jnp.arange(CHUNK)[:, None] < jnp.arange(CHUNK)[None, :]).astype(BF16)
        sets = jnp.concatenate([own, near, far], axis=0).astype(BF16)
        rank = jnp.dot(sets, tri, preferred_element_type=F32).astype(jnp.int32)
        counts = jnp.sum(sets.astype(F32), axis=1).astype(jnp.int32)
        n_own, n_near, n_far = counts[:rows], counts[rows:2 * rows], counts[2 * rows:]
        skip = (n_near + 15) // 16 * 16
        place = jnp.where(far, SLOT - 1 - skip[:, None] - rank[2 * rows:], SLOT)
        place = jnp.where(near, SLOT - 1 - rank[rows:2 * rows], place)
        place = jnp.where(own, rank[:rows], place)
        hit = place[:, :, None] == jnp.arange(SLOT)[None, None, :]
        code = jnp.where(src < n_loc, src, src - n_loc) + dst * n_loc
        picks = (jnp.where(hit, code[:, :, None], 0), jnp.where(hit, w[:, :, None], 0.0))
        code, wc = lax.reduce(picks, (jnp.int32(0), jnp.float32(0.0)), lambda a, b: (a[0] + b[0], a[1] + b[1]), (1,))
        n_hal = jnp.where(n_far > 0, skip + n_far, n_near)
        return code, wc, n_own, n_hal, n_near, n_far, skip

    def device_step(node_feats, w_one, w_two, send_rows, edge_src, edge_dst, edge_w, labels, label_mask):
        n_loc, f_in = node_feats.shape
        halo = send_rows.shape[1]
        f_hid, classes = w_two.shape
        quad = 4 * n_loc
        sds = jax.ShapeDtypeStruct
        x = node_feats
        w1 = w_one.astype(BF16)
        w2t = jnp.pad(w_two.T.astype(BF16), ((0, LANES - classes), (0, 0)))
        ids = jnp.concatenate([send_rows[1], send_rows[0]])
        code, wc, n_own, n_hal, n_near, n_far, skip = compact(edge_src, edge_dst, edge_w, n_loc, halo)
        rows = n_own.shape[0]
        slots = code.size // LANES
        code, wc = code.reshape(-1), wc.reshape(-1)
        tally = jnp.concatenate([n_near, n_far, skip, jnp.zeros((8 * LANES - 3 * rows,), jnp.int32)])
        lists = jnp.concatenate([code, tally]).reshape(slots + 8, LANES)
        count, code_prev, code_next, w_prev, w_next = pl.pallas_call(
            functools.partial(lists_kernel, num_dev),
            out_shape=[sds((8, LANES), F32)] + [sds((slots + 8, LANES), jnp.int32)] * 2 + [sds((slots, LANES), F32)] * 2,
            in_specs=[VMEM_SPEC] * 3,
            out_specs=[VMEM_SPEC] * 5,
            scratch_shapes=[pltpu.VMEM((8, LANES), F32), pltpu.VMEM((num_dev - 1, 8, LANES), F32)] + [pltpu.SemaphoreType.DMA((n,)) for n in (num_dev - 1, num_dev - 1, 4, 4)],
            compiler_params=params(1, collective_id=0, has_side_effects=True),
            name="lists",
        )(label_mask.reshape(-1, LANES), lists, wc.reshape(slots, LANES))
        s, d = code % n_loc, code // n_loc
        s4, d4 = s * 4, d * 4
        count, x = lax.optimization_barrier((count, x))
        x_next, x_prev = pl.pallas_call(
            halo_rows_kernel,
            out_shape=[sds((halo, 256), BF16)] * 2,
            in_specs=[SMEM_SPEC, VMEM_SPEC],
            out_specs=[VMEM_SPEC] * 2,
            scratch_shapes=[pltpu.VMEM((2 * n_loc, LANES), F32), pltpu.VMEM((4 * halo, LANES), F32)],
            compiler_params=params(12),
            name="halo_rows",
        )(ids * 2, x)
        xh_prev = shift_next(x_next)
        xh_next = shift_prev(x_prev)
        wide4 = [pltpu.VMEM((quad, LANES), F32)] * 4
        thin4 = [pltpu.VMEM((n_loc, LANES), F32)] * 4
        marks = jnp.where(label_mask == 1, labels, -1)
        ids4 = ids * 4
        s4, w2t, marks, ids4 = lax.optimization_barrier((s4, w2t, marks, ids4))
        y_own = pl.pallas_call(
            one_own_kernel,
            out_shape=sds((quad, LANES), F32),
            in_specs=[SMEM_SPEC] * 4 + [VMEM_SPEC] * 2,
            out_specs=VMEM_SPEC,
            scratch_shapes=[pltpu.VMEM((quad, LANES), F32)] + wide4,
            compiler_params=params(28),
            cost_estimate=pl.CostEstimate(flops=200000000000, bytes_accessed=8000000, transcendentals=0),
            name="one_own",
        )(s4, d4, wc, n_own, x, w1)
        hid_a, hid_b, t2, t_next, t_prev = pl.pallas_call(
            one_halo_kernel,
            out_shape=[sds((n_loc, f_hid // 2), BF16)] * 2 + [sds((n_loc, LANES), F32), sds((halo, LANES), BF16), sds((halo, LANES), BF16)],
            in_specs=[SMEM_SPEC] * 5 + [VMEM_SPEC] * 5,
            out_specs=[VMEM_SPEC] * 5,
            scratch_shapes=[pltpu.VMEM((4 * 2 * halo, LANES), F32), pltpu.VMEM((2 * halo, LANES), F32)] + wide4,
            compiler_params=params(32),
            name="one_halo",
        )(s4, d4, wc, n_hal, ids, y_own, xh_prev, xh_next, w1, w2t)
        th_prev = shift_next(t_next)
        th_next = shift_prev(t_prev)
        ha_prev, ha_next = shift_next(hid_a), shift_prev(hid_a)
        narrow_own = functools.partial(
            pl.pallas_call,
            narrow_own_kernel,
            out_shape=sds((n_loc, LANES), F32),
            in_specs=[SMEM_SPEC] * 4 + [VMEM_SPEC],
            out_specs=VMEM_SPEC,
            scratch_shapes=thin4,
            compiler_params=params(10),
            cost_estimate=pl.CostEstimate(flops=200000000000, bytes_accessed=8000000, transcendentals=0),
        )
        z_own = narrow_own(name="two_own")(s, d, wc, n_own, t2)
        marks = jnp.broadcast_to(marks[:, None], (n_loc, LANES))
        dz, bz_prev, bz_next, loss = pl.pallas_call(
            functools.partial(logits_kernel, classes),
            out_shape=[sds((n_loc, LANES), F32), sds((halo, LANES), F32), sds((halo, LANES), F32), sds((8, LANES), F32)],
            in_specs=[SMEM_SPEC] * 4 + [VMEM_SPEC] * 5,
            out_specs=[VMEM_SPEC] * 4,
            scratch_shapes=[pltpu.VMEM((2 * halo, LANES), F32)] + thin4,
            compiler_params=params(12),
            name="logits",
        )(s, d, wc, n_hal, z_own, th_prev, th_next, marks, count)
        rz_next = shift_prev(bz_prev)
        rz_prev = shift_next(bz_next)
        late_b, _ = lax.optimization_barrier((hid_b, bz_prev))
        hb_prev, hb_next = shift_next(late_b), shift_prev(late_b)
        dt2_own = narrow_own(name="two_back_own")(d, s, wc, n_own, dz)
        dt2, dy, grad_two = pl.pallas_call(
            hidden_grad_kernel,
            out_shape=[sds((n_loc, LANES), BF16), sds((quad, LANES), F32), sds((f_hid, LANES), F32)],
            in_specs=[SMEM_SPEC] + [VMEM_SPEC] * 6,
            out_specs=[VMEM_SPEC] * 3,
            scratch_shapes=thin4,
            compiler_params=params(16),
            name="hidden_grad",
        )(ids, dt2_own, rz_next, rz_prev, hid_a, hid_b, w2t)
        dt_prev, dt_next = shift_next(dt2), shift_prev(dt2)
        dt1_own = pl.pallas_call(
            wide_own_kernel,
            out_shape=sds((quad, LANES), F32),
            in_specs=[SMEM_SPEC] * 4 + [VMEM_SPEC],
            out_specs=VMEM_SPEC,
            scratch_shapes=wide4,
            compiler_params=params(28),
            cost_estimate=pl.CostEstimate(flops=200000000000, bytes_accessed=8000000, transcendentals=0),
            name="one_back_own",
        )(d4, s4, wc, n_own, dy)
        grad_one = pl.pallas_call(
            functools.partial(table_grad_kernel, rows),
            out_shape=sds((256, f_hid), F32),
            in_specs=[SMEM_SPEC] * 5 + [VMEM_SPEC] * 9,
            out_specs=VMEM_SPEC,
            scratch_shapes=[pltpu.VMEM((quad, LANES), F32)] + wide4,
            compiler_params=params(36),
            name="table_grad",
        )(ids4, code_next.reshape(-1), w_next.reshape(-1), code_prev.reshape(-1), w_prev.reshape(-1), dt1_own, dt_next, ha_next, hb_next, dt_prev, ha_prev, hb_prev, w2t, x)
        grad_one, grad_two, loss = pl.pallas_call(
            functools.partial(reduce_kernel, num_dev),
            out_shape=[sds((256, f_hid), F32), sds((f_hid, LANES), F32), sds((8, LANES), F32)],
            in_specs=[VMEM_SPEC] * 3,
            out_specs=[VMEM_SPEC] * 3,
            scratch_shapes=[
                pltpu.VMEM((128, f_hid), F32), pltpu.VMEM((f_hid // 2, LANES), F32),
                pltpu.VMEM((128, f_hid), F32), pltpu.VMEM((f_hid // 2, LANES), F32),
                pltpu.VMEM((3, 32, f_hid), F32), pltpu.VMEM((3, f_hid // 8, LANES), F32),
                pltpu.VMEM((num_dev - 1, 8, LANES), F32),
                pltpu.SemaphoreType.DMA((22,)), pltpu.SemaphoreType.DMA((22,)),
                pltpu.SemaphoreType.DMA((num_dev - 1,)), pltpu.SemaphoreType.DMA((num_dev - 1,)),
            ],
            compiler_params=params(8, collective_id=1, has_side_effects=True),
            name="reduce",
        )(grad_one, grad_two, loss)
        mean_loss = jnp.sum(loss) / count[0, 0]
        return mean_loss, grad_one[:f_in], grad_two[:, :classes]

    row_spec = P(GRAPH_AXIS)
    return jax.shard_map(device_step, mesh=mesh, in_specs=(row_spec, P(), P(), row_spec, row_spec, row_spec, row_spec, row_spec, row_spec), out_specs=(P(), P(), P()), check_vma=False)
```

```python
import functools

import jax
import jax.numpy as jnp
from jax import lax
from jax.experimental import pallas as pl
from jax.experimental.pallas import tpu as pltpu
from jax.sharding import PartitionSpec as P


GRAPH_AXIS = "graph"
CONTRACT_ROWS = (((0,), (0,)), ((), ()))
CONTRACT_COLS = (((1,), (1,)), ((), ()))
MESH = pl.DeviceIdType.MESH
F32 = jnp.float32
BF16 = jnp.bfloat16
LANES = 128
BLOCK = 256
CHUNK = 256
SLOT = 384

SMEM_SPEC = pl.BlockSpec(memory_space=pltpu.SMEM)
VMEM_SPEC = pl.BlockSpec(memory_space=pltpu.VMEM)


def rows_at(i, base=0, size=BLOCK):
    return pl.ds(base + i * size, size)


def loop(count, body):
    lax.fori_loop(0, count, lambda i, _: (body(i), 0)[1], 0)


def params(mib, **kw):
    return pltpu.CompilerParams(vmem_limit_bytes=mib * 2**20, **kw)


def zero_rows(refs):
    rows = refs[0].shape[0]

    def body(i):
        for ref in refs:
            ref[pl.ds(i * 64, 64), :] = jnp.zeros((64, LANES), F32)

    loop(rows // 64, body)


def sum_rows(out, refs):
    rows = refs[0].shape[0]

    def body(i):
        total = refs[0][pl.ds(i * 64, 64), :]
        for ref in refs[1:]:
            total = total + ref[pl.ds(i * 64, 64), :]
        out[pl.ds(i * 64, 64), :] = total

    loop(rows // 64, body)


def edge_pass(from_ref, to_ref, w_ref, cnt_ref, table, accs, width, unroll, back):
    n_acc = len(accs)
    shift = unroll.bit_length() - 1

    def row(r):
        blocks = lax.shift_right_logical(cnt_ref[r] + (unroll - 1), shift)

        def body(j):
            off = r * SLOT + (SLOT - unroll - j * unroll if back else j * unroll)
            frm, to, wgt = (ref.at[pl.ds(off, unroll)] for ref in (from_ref, to_ref, w_ref))
            for g in range(0, unroll, n_acc):
                vals = [table[pl.ds(pl.multiple_of(frm[g + k], width), width), :] * wgt[g + k] for k in range(n_acc)]
                rows = [pl.multiple_of(to[g + k], width) for k in range(n_acc)]
                old = [accs[k][pl.ds(rows[k], width), :] for k in range(n_acc)]
                for k in range(n_acc):
                    accs[k][pl.ds(rows[k], width), :] = old[k] + vals[k]

        loop(blocks, body)

    loop(cnt_ref.shape[0], row)


def scatter_pass(ids_ref, table, accs, width, unroll):
    n_acc = len(accs)

    def body(j):
        off = j * unroll
        for g in range(unroll // n_acc):
            rows = [pl.multiple_of(ids_ref[off + g * n_acc + k], width) for k in range(n_acc)]
            vals = [table[pl.ds(pl.multiple_of((off + g * n_acc + k) * width, width), width), :] for k in range(n_acc)]
            old = [accs[k][pl.ds(rows[k], width), :] for k in range(n_acc)]
            for k in range(n_acc):
                accs[k][pl.ds(rows[k], width), :] = old[k] + vals[k]

    loop(ids_ref.shape[0] // unroll, body)


def gather_pass(ids_ref, table, out, width, unroll=8):
    def body(j):
        for u in range(unroll):
            i = j * unroll + u
            out[pl.ds(pl.multiple_of(i * width, width), width), :] = table[pl.ds(pl.multiple_of(ids_ref[i], width), width), :]

    loop(ids_ref.shape[0] // unroll, body)


def spread(table, start, block):
    tiles = block.shape[1] // LANES
    for c in range(tiles):
        table[pl.ds(start * tiles + c, block.shape[0], tiles), :] = block[:, c * LANES:(c + 1) * LANES]


def unspread(table, start, rows, tiles):
    return jnp.concatenate([table[pl.ds(start * tiles + c, rows, tiles), :] for c in range(tiles)], axis=1)


def enter(me, num_dev):
    barrier = pltpu.get_barrier_semaphore()
    for step in range(1, num_dev):
        pl.semaphore_signal(barrier, inc=1, device_id=(lax.rem(me + step, num_dev),), device_id_type=MESH)
    pl.semaphore_wait(barrier, num_dev - 1)


def push(src, dst, send_sem, recv_sem, dev):
    copy = pltpu.make_async_remote_copy(src_ref=src, dst_ref=dst, send_sem=send_sem, recv_sem=recv_sem, device_id=(dev,), device_id_type=MESH)
    copy.start()
    return copy


def lists_kernel(num_dev, mask, code, wgt, count, code_prev, code_next, w_prev, w_next, part, slots, send_sem, recv_sem, lsend, lrecv):
    ones = jnp.sum(jnp.sum(mask[...].astype(F32), axis=1, keepdims=True), axis=0, keepdims=True)
    part[...] = jnp.broadcast_to(ones, part.shape)
    me = lax.axis_index(GRAPH_AXIS)
    succ, pred = lax.rem(me + 1, num_dev), lax.rem(me + num_dev - 1, num_dev)
    enter(me, num_dev)
    copies = []
    for step in range(1, num_dev):
        copies.append(push(part, slots.at[step - 1], send_sem.at[step - 1], recv_sem.at[step - 1], lax.rem(me + step, num_dev)))
    copies.append(push(code, code_prev, lsend.at[0], lrecv.at[0], succ))
    copies.append(push(code, code_next, lsend.at[1], lrecv.at[1], pred))
    copies.append(push(wgt, w_prev, lsend.at[2], lrecv.at[2], succ))
    copies.append(push(wgt, w_next, lsend.at[3], lrecv.at[3], pred))
    for copy in copies:
        copy.wait()
    total = part[...]
    for step in range(num_dev - 1):
        total = total + slots[step]
    count[...] = jnp.maximum(total, 1.0)


def halo_rows_kernel(ids2, x, to_next, to_prev, table, picked):
    rows = x.shape[0]

    def put(i):
        block = x[rows_at(i), :].astype(F32)
        pad = jnp.zeros((BLOCK, 2 * LANES - block.shape[1]), F32)
        spread(table, i * BLOCK, jnp.concatenate([block, pad], axis=1))

    loop(rows // BLOCK, put)
    gather_pass(ids2, table, picked, 2)
    half = to_next.shape[0]

    def take(i):
        to_next[rows_at(i), :] = unspread(picked, i * BLOCK, BLOCK, 2).astype(BF16)
        to_prev[rows_at(i), :] = unspread(picked, half + i * BLOCK, BLOCK, 2).astype(BF16)

    loop(half // BLOCK, take)


def one_own_kernel(s4, d4, w, cnt, x, w1, y, table, *accs):
    zero_rows(accs)

    def put(i):
        t = jnp.dot(x[rows_at(i), :], w1[...], preferred_element_type=F32)
        spread(table, i * BLOCK, t.astype(BF16).astype(F32))

    loop(x.shape[0] // BLOCK, put)
    edge_pass(s4, d4, w, cnt, table, accs, 4, 16, False)
    sum_rows(y, accs)


def one_halo_kernel(s4, d4, w, cnt, ids, y_own, x_prev, x_next, w1, w2t, hid_a, hid_b, t2, to_next, to_prev, table, picked, *accs):
    zero_rows(accs)
    half = x_prev.shape[0]

    def put(i):
        t = jnp.dot(x_prev[rows_at(i), :w1.shape[0]], w1[...], preferred_element_type=F32)
        spread(table, i * BLOCK, t.astype(BF16).astype(F32))
        t = jnp.dot(x_next[rows_at(i), :w1.shape[0]], w1[...], preferred_element_type=F32)
        spread(table, half + i * BLOCK, t.astype(BF16).astype(F32))

    loop(half // BLOCK, put)
    edge_pass(s4, d4, w, cnt, table, accs, 4, 16, True)
    sum_rows(accs[0], (y_own,) + accs)

    def act(i):
        h = jnp.maximum(unspread(accs[0], i * BLOCK, BLOCK, 4), 0.0).astype(BF16)
        cut = hid_a.shape[1]
        hid_a[rows_at(i), :] = h[:, :cut]
        hid_b[rows_at(i), :] = h[:, cut:]
        t = lax.dot_general(h, w2t[...], CONTRACT_COLS, preferred_element_type=F32)
        t2[rows_at(i), :] = t.astype(BF16).astype(F32)

    loop(t2.shape[0] // BLOCK, act)
    gather_pass(ids, t2, picked, 1)

    def take(i):
        to_next[rows_at(i), :] = picked[rows_at(i), :].astype(BF16)
        to_prev[rows_at(i), :] = picked[rows_at(i, half), :].astype(BF16)

    loop(half // BLOCK, take)


def narrow_own_kernel(frm, to, w, cnt, table, out, *accs):
    zero_rows(accs)
    edge_pass(frm, to, w, cnt, table, accs, 1, 16, False)
    sum_rows(out, accs)


def wide_own_kernel(frm, to, w, cnt, table, out, *accs):
    zero_rows(accs)
    edge_pass(frm, to, w, cnt, table, accs, 4, 16, False)
    sum_rows(out, accs)


def logits_kernel(classes, s, d, w, cnt, z_own, t_prev, t_next, labels, count, dz, back_prev, back_next, loss, table, *accs):
    zero_rows(accs)
    half = t_prev.shape[0]

    def put(i):
        table[rows_at(i), :] = t_prev[rows_at(i), :].astype(F32)
        table[rows_at(i, half), :] = t_next[rows_at(i), :].astype(F32)

    loop(half // BLOCK, put)
    edge_pass(s, d, w, cnt, table, accs, 1, 16, True)
    denom = count[0:1, :]
    loss[...] = jnp.zeros_like(loss)

    def soft(i):
        at = pl.ds(i * 64, 64)
        z = z_own[at, :]
        for acc in accs:
            z = z + acc[at, :]
        lane = lax.broadcasted_iota(jnp.int32, z.shape, 1)
        lab = labels[at, :]
        hot = lab == lane
        keep = lab >= 0
        zm = jnp.where(lane < classes, z, -jnp.inf)
        top = jnp.max(zm, axis=1, keepdims=True)
        ex = jnp.exp(zm - top)
        log_norm = jnp.log(jnp.sum(ex, axis=1, keepdims=True)) + top
        hot_f = jnp.where(hot, 1.0, 0.0)
        term = jnp.where(hot, log_norm - z, 0.0)
        part = term[0:8]
        for b in range(1, 8):
            part = part + term[b * 8:b * 8 + 8]
        loss[...] += part
        mask_f = jnp.where(keep, 1.0, 0.0)
        dz[at, :] = jnp.where(lane < classes, (jnp.exp(zm - log_norm) - hot_f) * (mask_f / denom), 0.0)

    loop(dz.shape[0] // 64, soft)
    zero_rows(accs)
    edge_pass(d, s, w, cnt, dz, accs, 1, 16, True)

    def fin(i):
        at = pl.ds(i * 64, 64)
        bt = pl.ds(half + i * 64, 64)
        a, b = accs[0][at, :], accs[0][bt, :]
        for acc in accs[1:]:
            a, b = a + acc[at, :], b + acc[bt, :]
        back_prev[at, :] = a
        back_next[at, :] = b

    loop(half // 64, fin)


def masked(grad, hid_a, hid_b):
    cut = hid_a.shape[1]
    lo = jnp.where(hid_a.astype(F32) > 0.0, grad[:, :cut], 0.0)
    hi = jnp.where(hid_b.astype(F32) > 0.0, grad[:, cut:], 0.0)
    return jnp.concatenate([lo, hi], axis=1)


def hidden_grad_kernel(ids, own, ret_next, ret_prev, hid_a, hid_b, w2t, dt2, dy, g2, *accs):
    n_loc, half = own.shape[0], ret_next.shape[0]
    zero_rows(accs)
    scatter_pass(ids.at[pl.ds(0, half)], ret_next, accs, 1, 8)
    scatter_pass(ids.at[pl.ds(half, half)], ret_prev, accs, 1, 8)
    g2[...] = jnp.zeros_like(g2)

    def fold(i):
        at = rows_at(i)
        total = own[at, :]
        for acc in accs:
            total = total + acc[at, :]
        dt = total.astype(BF16)
        dt2[at, :] = dt
        cut = hid_a.shape[1]
        g2[:cut, :] += lax.dot_general(hid_a[at, :], dt, CONTRACT_ROWS, preferred_element_type=F32)
        g2[cut:, :] += lax.dot_general(hid_b[at, :], dt, CONTRACT_ROWS, preferred_element_type=F32)
        dh = jnp.dot(dt, w2t[...], preferred_element_type=F32)
        spread(dy, i * BLOCK, masked(dh, hid_a[at, :], hid_b[at, :]))

    loop(n_loc // BLOCK, fold)


def peer_pass(ids4, code_ref, w_ref, rows, far, table, accs):
    n_acc = len(accs)
    tally = rows * SLOT
    n_loc = ids4.shape[0]
    shift = n_loc.bit_length() - 1

    def row(r):
        first = SLOT - 16 - (code_ref[tally + 2 * rows + r] if far else 0)
        edges = code_ref[tally + far * rows + r]

        def body(j):
            off = r * SLOT + first - j * 16
            codes, wgt = (ref.at[pl.ds(off, 16)] for ref in (code_ref, w_ref))
            for u in range(16):
                acc = accs[u % n_acc]
                code = codes[u]
                frm = lax.shift_right_logical(code, shift) * 4
                val = table[pl.ds(pl.multiple_of(frm, 4), 4), :] * wgt[u]
                at = pl.ds(pl.multiple_of(ids4[code & (n_loc - 1)], 4), 4)
                acc[at, :] = acc[at, :] + val

        loop(lax.shift_right_logical(edges + 15, 4), body)

    loop(rows, row)


def table_grad_kernel(rows, ids4, cn, wn, cp, wp, own, tn, han, hbn, tp, hap, hbp, w2t, x, g1, table, *accs):
    zero_rows(accs)
    g1[...] = jnp.zeros_like(g1)

    def fill(dt, hid_a, hid_b):
        def put(i):
            at = rows_at(i)
            dh = jnp.dot(dt[at, :], w2t[...], preferred_element_type=F32)
            spread(table, i * BLOCK, masked(dh, hid_a[at, :], hid_b[at, :]))

        loop(dt.shape[0] // BLOCK, put)

    fill(tn, han, hbn)
    peer_pass(ids4, cn, wn, rows, 0, table, accs)
    fill(tp, hap, hbp)
    peer_pass(ids4, cp, wp, rows, 1, table, accs)

    def fold(i):
        total = unspread(own, i * BLOCK, BLOCK, 4)
        for acc in accs:
            total = total + unspread(acc, i * BLOCK, BLOCK, 4)
        g1[:x.shape[1], :] += lax.dot_general(x[rows_at(i), :], total.astype(BF16), CONTRACT_ROWS, preferred_element_type=F32)

    loop(x.shape[0] // BLOCK, fold)


def reduce_kernel(num_dev, g1, g2, loss, o1, o2, lo, r1, r2, s1, s2, q1, q2, lslots, sem_s, sem_r, lsem_s, lsem_r):
    me = lax.axis_index(GRAPH_AXIS)
    core = lax.rem(me, 2)
    chip = me // 2
    mate = me + 1 - 2 * core
    h1, h2 = g1.shape[0] // 2, g2.shape[0] // 2
    e1, e2 = h1 // 4, h2 // 4
    enter(me, num_dev)
    other = 1 - core
    pair = [
        push(g1.at[pl.ds(pl.multiple_of(other * h1, h1), h1)], r1, sem_s.at[0], sem_r.at[0], mate),
        push(g2.at[pl.ds(pl.multiple_of(other * h2, h2), h2)], r2, sem_s.at[1], sem_r.at[1], mate),
    ]
    scalar = []
    for step in range(1, num_dev):
        scalar.append(push(loss, lslots.at[step - 1], lsem_s.at[step - 1], lsem_r.at[step - 1], lax.rem(me + step, num_dev)))
    for copy in pair:
        copy.wait()
    s1[...] = g1[pl.ds(pl.multiple_of(core * h1, h1), h1), :] + r1[...]
    s2[...] = g2[pl.ds(pl.multiple_of(core * h2, h2), h2), :] + r2[...]
    spreads = []
    for step in range(1, 4):
        far = lax.rem(chip + step, 4)
        dev = far * 2 + core
        k = 2 * step
        spreads.append(push(s1.at[pl.ds(pl.multiple_of(far * e1, e1), e1)], q1.at[step - 1], sem_s.at[k], sem_r.at[k], dev))
        spreads.append(push(s2.at[pl.ds(pl.multiple_of(far * e2, e2), e2)], q2.at[step - 1], sem_s.at[k + 1], sem_r.at[k + 1], dev))
    for copy in spreads:
        copy.wait()
    mine1 = pl.ds(pl.multiple_of(core * h1 + chip * e1, e1), e1)
    mine2 = pl.ds(pl.multiple_of(core * h2 + chip * e2, e2), e2)
    t1 = s1[pl.ds(pl.multiple_of(chip * e1, e1), e1), :]
    t2 = s2[pl.ds(pl.multiple_of(chip * e2, e2), e2), :]
    for step in range(3):
        t1 = t1 + q1[step]
        t2 = t2 + q2[step]
    o1[mine1, :] = t1
    o2[mine2, :] = t2
    gathers = []
    for step in range(1, 4):
        dev = lax.rem(chip + step, 4) * 2 + core
        k = 6 + 2 * step
        gathers.append((push(o1.at[mine1], o1.at[mine1], sem_s.at[k], sem_r.at[k], dev), push(o2.at[mine2], o2.at[mine2], sem_s.at[k + 1], sem_r.at[k + 1], dev)))
    tails = [push(o1.at[mine1], o1.at[mine1], sem_s.at[14], sem_r.at[14], mate), push(o2.at[mine2], o2.at[mine2], sem_s.at[15], sem_r.at[15], mate)]
    for step in range(1, 4):
        near = lax.rem(chip + 4 - step, 4)
        at1 = pl.ds(pl.multiple_of(core * h1 + near * e1, e1), e1)
        at2 = pl.ds(pl.multiple_of(core * h2 + near * e2, e2), e2)
        for copy in gathers[step - 1]:
            copy.wait()
        k = 14 + 2 * step
        tails.append(push(o1.at[at1], o1.at[at1], sem_s.at[k], sem_r.at[k], mate))
        tails.append(push(o2.at[at2], o2.at[at2], sem_s.at[k + 1], sem_r.at[k + 1], mate))
    for copy in scalar:
        copy.wait()
    total = loss[...]
    for step in range(num_dev - 1):
        total = total + lslots[step]
    lo[...] = total
    for copy in tails:
        copy.wait()


def solution(mesh):
    num_dev = mesh.shape[GRAPH_AXIS]
    to_next = [(dev_id, (dev_id + 1) % num_dev) for dev_id in range(num_dev)]
    to_prev = [(dev_id, (dev_id - 1) % num_dev) for dev_id in range(num_dev)]

    def shift_next(a):
        return lax.ppermute(a, GRAPH_AXIS, to_next)

    def shift_prev(a):
        return lax.ppermute(a, GRAPH_AXIS, to_prev)

    def compact(edge_src, edge_dst, edge_w, n_loc, halo):
        rows = edge_src.shape[0] // CHUNK
        src, dst, w = (a.reshape(rows, CHUNK) for a in (edge_src, edge_dst, edge_w))
        live = w != 0.0
        own = live & (src < n_loc)
        far = live & (src >= n_loc + halo)
        near = live & (src >= n_loc) & (src < n_loc + halo)
        tri = (jnp.arange(CHUNK)[:, None] < jnp.arange(CHUNK)[None, :]).astype(BF16)
        sets = jnp.concatenate([own, near, far], axis=0).astype(BF16)
        rank = jnp.dot(sets, tri, preferred_element_type=F32).astype(jnp.int32)
        counts = jnp.sum(sets.astype(F32), axis=1).astype(jnp.int32)
        n_own, n_near, n_far = counts[:rows], counts[rows:2 * rows], counts[2 * rows:]
        skip = (n_near + 15) // 16 * 16
        place = jnp.where(far, SLOT - 1 - skip[:, None] - rank[2 * rows:], SLOT)
        place = jnp.where(near, SLOT - 1 - rank[rows:2 * rows], place)
        place = jnp.where(own, rank[:rows], place)
        hit = place[:, :, None] == jnp.arange(SLOT)[None, None, :]
        code = jnp.where(src < n_loc, src, src - n_loc) + dst * n_loc
        picks = (jnp.where(hit, code[:, :, None], 0), jnp.where(hit, w[:, :, None], 0.0))
        code, wc = lax.reduce(picks, (jnp.int32(0), jnp.float32(0.0)), lambda a, b: (a[0] + b[0], a[1] + b[1]), (1,))
        n_hal = jnp.where(n_far > 0, skip + n_far, n_near)
        return code, wc, n_own, n_hal, n_near, n_far, skip

    def device_step(node_feats, w_one, w_two, send_rows, edge_src, edge_dst, edge_w, labels, label_mask):
        n_loc, f_in = node_feats.shape
        halo = send_rows.shape[1]
        f_hid, classes = w_two.shape
        quad = 4 * n_loc
        sds = jax.ShapeDtypeStruct
        x = node_feats
        w1 = w_one.astype(BF16)
        w2t = jnp.pad(w_two.T.astype(BF16), ((0, LANES - classes), (0, 0)))
        ids = jnp.concatenate([send_rows[1], send_rows[0]])
        code, wc, n_own, n_hal, n_near, n_far, skip = compact(edge_src, edge_dst, edge_w, n_loc, halo)
        rows = n_own.shape[0]
        slots = code.size // LANES
        code, wc = code.reshape(-1), wc.reshape(-1)
        tally = jnp.concatenate([n_near, n_far, skip, jnp.zeros((8 * LANES - 3 * rows,), jnp.int32)])
        lists = jnp.concatenate([code, tally]).reshape(slots + 8, LANES)
        count, code_prev, code_next, w_prev, w_next = pl.pallas_call(
            functools.partial(lists_kernel, num_dev),
            out_shape=[sds((8, LANES), F32)] + [sds((slots + 8, LANES), jnp.int32)] * 2 + [sds((slots, LANES), F32)] * 2,
            in_specs=[VMEM_SPEC] * 3,
            out_specs=[VMEM_SPEC] * 5,
            scratch_shapes=[pltpu.VMEM((8, LANES), F32), pltpu.VMEM((num_dev - 1, 8, LANES), F32)] + [pltpu.SemaphoreType.DMA((n,)) for n in (num_dev - 1, num_dev - 1, 4, 4)],
            compiler_params=params(1, collective_id=0, has_side_effects=True),
            name="lists",
        )(label_mask.reshape(-1, LANES), lists, wc.reshape(slots, LANES))
        s, d = code % n_loc, code // n_loc
        s4, d4 = s * 4, d * 4
        count, x = lax.optimization_barrier((count, x))
        x_next, x_prev = pl.pallas_call(
            halo_rows_kernel,
            out_shape=[sds((halo, 256), BF16)] * 2,
            in_specs=[SMEM_SPEC, VMEM_SPEC],
            out_specs=[VMEM_SPEC] * 2,
            scratch_shapes=[pltpu.VMEM((2 * n_loc, LANES), F32), pltpu.VMEM((4 * halo, LANES), F32)],
            compiler_params=params(12),
            name="halo_rows",
        )(ids * 2, x)
        xh_prev = shift_next(x_next)
        xh_next = shift_prev(x_prev)
        wide4 = [pltpu.VMEM((quad, LANES), F32)] * 4
        thin4 = [pltpu.VMEM((n_loc, LANES), F32)] * 4
        marks = jnp.where(label_mask == 1, labels, -1)
        ids4 = ids * 4
        s4, w2t, marks, ids4 = lax.optimization_barrier((s4, w2t, marks, ids4))
        y_own = pl.pallas_call(
            one_own_kernel,
            out_shape=sds((quad, LANES), F32),
            in_specs=[SMEM_SPEC] * 4 + [VMEM_SPEC] * 2,
            out_specs=VMEM_SPEC,
            scratch_shapes=[pltpu.VMEM((quad, LANES), F32)] + wide4,
            compiler_params=params(28),
            cost_estimate=pl.CostEstimate(flops=200000000000, bytes_accessed=8000000, transcendentals=0),
            name="one_own",
        )(s4, d4, wc, n_own, x, w1)
        hid_a, hid_b, t2, t_next, t_prev = pl.pallas_call(
            one_halo_kernel,
            out_shape=[sds((n_loc, f_hid // 2), BF16)] * 2 + [sds((n_loc, LANES), F32), sds((halo, LANES), BF16), sds((halo, LANES), BF16)],
            in_specs=[SMEM_SPEC] * 5 + [VMEM_SPEC] * 5,
            out_specs=[VMEM_SPEC] * 5,
            scratch_shapes=[pltpu.VMEM((4 * 2 * halo, LANES), F32), pltpu.VMEM((2 * halo, LANES), F32)] + wide4,
            compiler_params=params(32),
            name="one_halo",
        )(s4, d4, wc, n_hal, ids, y_own, xh_prev, xh_next, w1, w2t)
        th_prev = shift_next(t_next)
        th_next = shift_prev(t_prev)
        ha_prev, ha_next = shift_next(hid_a), shift_prev(hid_a)
        narrow_own = functools.partial(
            pl.pallas_call,
            narrow_own_kernel,
            out_shape=sds((n_loc, LANES), F32),
            in_specs=[SMEM_SPEC] * 4 + [VMEM_SPEC],
            out_specs=VMEM_SPEC,
            scratch_shapes=thin4,
            compiler_params=params(10),
            cost_estimate=pl.CostEstimate(flops=200000000000, bytes_accessed=8000000, transcendentals=0),
        )
        z_own = narrow_own(name="two_own")(s, d, wc, n_own, t2)
        marks = jnp.broadcast_to(marks[:, None], (n_loc, LANES))
        dz, bz_prev, bz_next, loss = pl.pallas_call(
            functools.partial(logits_kernel, classes),
            out_shape=[sds((n_loc, LANES), F32), sds((halo, LANES), F32), sds((halo, LANES), F32), sds((8, LANES), F32)],
            in_specs=[SMEM_SPEC] * 4 + [VMEM_SPEC] * 5,
            out_specs=[VMEM_SPEC] * 4,
            scratch_shapes=[pltpu.VMEM((2 * halo, LANES), F32)] + thin4,
            compiler_params=params(12),
            name="logits",
        )(s, d, wc, n_hal, z_own, th_prev, th_next, marks, count)
        rz_next = shift_prev(bz_prev)
        rz_prev = shift_next(bz_next)
        late_b, _ = lax.optimization_barrier((hid_b, bz_prev))
        hb_prev, hb_next = shift_next(late_b), shift_prev(late_b)
        dt2_own = narrow_own(name="two_back_own")(d, s, wc, n_own, dz)
        dt2, dy, grad_two = pl.pallas_call(
            hidden_grad_kernel,
            out_shape=[sds((n_loc, LANES), BF16), sds((quad, LANES), F32), sds((f_hid, LANES), F32)],
            in_specs=[SMEM_SPEC] + [VMEM_SPEC] * 6,
            out_specs=[VMEM_SPEC] * 3,
            scratch_shapes=thin4,
            compiler_params=params(16),
            name="hidden_grad",
        )(ids, dt2_own, rz_next, rz_prev, hid_a, hid_b, w2t)
        dt_prev, dt_next = shift_next(dt2), shift_prev(dt2)
        dt1_own = pl.pallas_call(
            wide_own_kernel,
            out_shape=sds((quad, LANES), F32),
            in_specs=[SMEM_SPEC] * 4 + [VMEM_SPEC],
            out_specs=VMEM_SPEC,
            scratch_shapes=wide4,
            compiler_params=params(28),
            cost_estimate=pl.CostEstimate(flops=200000000000, bytes_accessed=8000000, transcendentals=0),
            name="one_back_own",
        )(d4, s4, wc, n_own, dy)
        grad_one = pl.pallas_call(
            functools.partial(table_grad_kernel, rows),
            out_shape=sds((256, f_hid), F32),
            in_specs=[SMEM_SPEC] * 5 + [VMEM_SPEC] * 9,
            out_specs=VMEM_SPEC,
            scratch_shapes=[pltpu.VMEM((quad, LANES), F32)] + wide4,
            compiler_params=params(36),
            name="table_grad",
        )(ids4, code_next.reshape(-1), w_next.reshape(-1), code_prev.reshape(-1), w_prev.reshape(-1), dt1_own, dt_next, ha_next, hb_next, dt_prev, ha_prev, hb_prev, w2t, x)
        grad_one, grad_two, loss = pl.pallas_call(
            functools.partial(reduce_kernel, num_dev),
            out_shape=[sds((256, f_hid), F32), sds((f_hid, LANES), F32), sds((8, LANES), F32)],
            in_specs=[VMEM_SPEC] * 3,
            out_specs=[VMEM_SPEC] * 3,
            scratch_shapes=[
                pltpu.VMEM((128, f_hid), F32), pltpu.VMEM((f_hid // 2, LANES), F32),
                pltpu.VMEM((128, f_hid), F32), pltpu.VMEM((f_hid // 2, LANES), F32),
                pltpu.VMEM((3, 32, f_hid), F32), pltpu.VMEM((3, f_hid // 8, LANES), F32),
                pltpu.VMEM((num_dev - 1, 8, LANES), F32),
                pltpu.SemaphoreType.DMA((22,)), pltpu.SemaphoreType.DMA((22,)),
                pltpu.SemaphoreType.DMA((num_dev - 1,)), pltpu.SemaphoreType.DMA((num_dev - 1,)),
            ],
            compiler_params=params(8, collective_id=1, has_side_effects=True),
            name="reduce",
        )(grad_one, grad_two, loss)
        mean_loss = jnp.sum(loss) / count[0, 0]
        return mean_loss, grad_one[:f_in], grad_two[:, :classes]

    row_spec = P(GRAPH_AXIS)
    return jax.shard_map(device_step, mesh=mesh, in_specs=(row_spec, P(), P(), row_spec, row_spec, row_spec, row_spec, row_spec, row_spec), out_specs=(P(), P(), P()), check_vma=False)
```

```python
import functools

import jax
import jax.numpy as jnp
from jax import lax
from jax.experimental import pallas as pl
from jax.experimental.pallas import tpu as pltpu
from jax.sharding import PartitionSpec as P


GRAPH_AXIS = "graph"
CONTRACT_ROWS = (((0,), (0,)), ((), ()))
CONTRACT_COLS = (((1,), (1,)), ((), ()))
MESH = pl.DeviceIdType.MESH
F32 = jnp.float32
BF16 = jnp.bfloat16
LANES = 128
BLOCK = 256
CHUNK = 256
SLOT = 384

SMEM_SPEC = pl.BlockSpec(memory_space=pltpu.SMEM)
VMEM_SPEC = pl.BlockSpec(memory_space=pltpu.VMEM)


def rows_at(i, base=0, size=BLOCK):
    return pl.ds(base + i * size, size)


def loop(count, body):
    lax.fori_loop(0, count, lambda i, _: (body(i), 0)[1], 0)


def params(mib, **kw):
    return pltpu.CompilerParams(vmem_limit_bytes=mib * 2**20, **kw)


def zero_rows(refs):
    rows = refs[0].shape[0]

    def body(i):
        for ref in refs:
            ref[pl.ds(i * 64, 64), :] = jnp.zeros((64, LANES), F32)

    loop(rows // 64, body)


def sum_rows(out, refs):
    rows = refs[0].shape[0]

    def body(i):
        total = refs[0][pl.ds(i * 64, 64), :]
        for ref in refs[1:]:
            total = total + ref[pl.ds(i * 64, 64), :]
        out[pl.ds(i * 64, 64), :] = total

    loop(rows // 64, body)


def edge_pass(from_ref, to_ref, w_ref, cnt_ref, table, accs, width, unroll, back):
    n_acc = len(accs)
    shift = unroll.bit_length() - 1

    def row(r):
        blocks = lax.shift_right_logical(cnt_ref[r] + (unroll - 1), shift)

        def body(j):
            off = r * SLOT + (SLOT - unroll - j * unroll if back else j * unroll)
            frm, to, wgt = (ref.at[pl.ds(off, unroll)] for ref in (from_ref, to_ref, w_ref))
            for u in range(unroll):
                acc = accs[u % n_acc]
                val = table[pl.ds(pl.multiple_of(frm[u], width), width), :] * wgt[u]
                at = pl.ds(pl.multiple_of(to[u], width), width)
                acc[at, :] = acc[at, :] + val

        loop(blocks, body)

    loop(cnt_ref.shape[0], row)


def scatter_pass(ids_ref, table, accs, width, unroll):
    n_acc = len(accs)

    def body(j):
        off = j * unroll
        for g in range(unroll // n_acc):
            rows = [pl.multiple_of(ids_ref[off + g * n_acc + k], width) for k in range(n_acc)]
            vals = [table[pl.ds(pl.multiple_of((off + g * n_acc + k) * width, width), width), :] for k in range(n_acc)]
            old = [accs[k][pl.ds(rows[k], width), :] for k in range(n_acc)]
            for k in range(n_acc):
                accs[k][pl.ds(rows[k], width), :] = old[k] + vals[k]

    loop(ids_ref.shape[0] // unroll, body)


def gather_pass(ids_ref, table, out, width, unroll=16):
    def body(j):
        for u in range(unroll):
            i = j * unroll + u
            out[pl.ds(pl.multiple_of(i * width, width), width), :] = table[pl.ds(pl.multiple_of(ids_ref[i] * width, width), width), :]

    loop(ids_ref.shape[0] // unroll, body)


def spread(table, start, block):
    tiles = block.shape[1] // LANES
    for c in range(tiles):
        table[pl.ds(start * tiles + c, block.shape[0], tiles), :] = block[:, c * LANES:(c + 1) * LANES]


def unspread(table, start, rows, tiles):
    return jnp.concatenate([table[pl.ds(start * tiles + c, rows, tiles), :] for c in range(tiles)], axis=1)


def enter(me, num_dev):
    barrier = pltpu.get_barrier_semaphore()
    for step in range(1, num_dev):
        pl.semaphore_signal(barrier, inc=1, device_id=(lax.rem(me + step, num_dev),), device_id_type=MESH)
    pl.semaphore_wait(barrier, num_dev - 1)


def push(src, dst, send_sem, recv_sem, dev):
    copy = pltpu.make_async_remote_copy(src_ref=src, dst_ref=dst, send_sem=send_sem, recv_sem=recv_sem, device_id=(dev,), device_id_type=MESH)
    copy.start()
    return copy


def lists_kernel(num_dev, mask, code, wgt, count, code_prev, code_next, w_prev, w_next, part, slots, send_sem, recv_sem, lsend, lrecv):
    ones = jnp.sum(jnp.sum(mask[...].astype(F32), axis=1, keepdims=True), axis=0, keepdims=True)
    part[...] = jnp.broadcast_to(ones, part.shape)
    me = lax.axis_index(GRAPH_AXIS)
    succ, pred = lax.rem(me + 1, num_dev), lax.rem(me + num_dev - 1, num_dev)
    enter(me, num_dev)
    copies = []
    for step in range(1, num_dev):
        copies.append(push(part, slots.at[step - 1], send_sem.at[step - 1], recv_sem.at[step - 1], lax.rem(me + step, num_dev)))
    copies.append(push(code, code_prev, lsend.at[0], lrecv.at[0], succ))
    copies.append(push(code, code_next, lsend.at[1], lrecv.at[1], pred))
    copies.append(push(wgt, w_prev, lsend.at[2], lrecv.at[2], succ))
    copies.append(push(wgt, w_next, lsend.at[3], lrecv.at[3], pred))
    for copy in copies:
        copy.wait()
    total = part[...]
    for step in range(num_dev - 1):
        total = total + slots[step]
    count[...] = jnp.maximum(total, 1.0)


def halo_rows_kernel(ids, x, to_next, to_prev, table, picked):
    rows = x.shape[0]

    def put(i):
        block = x[rows_at(i), :].astype(F32)
        pad = jnp.zeros((BLOCK, 2 * LANES - block.shape[1]), F32)
        spread(table, i * BLOCK, jnp.concatenate([block, pad], axis=1))

    loop(rows // BLOCK, put)
    gather_pass(ids, table, picked, 2)
    half = to_next.shape[0]

    def take(i):
        to_next[rows_at(i), :] = unspread(picked, i * BLOCK, BLOCK, 2).astype(BF16)
        to_prev[rows_at(i), :] = unspread(picked, half + i * BLOCK, BLOCK, 2).astype(BF16)

    loop(half // BLOCK, take)


def one_own_kernel(s4, d4, w, cnt, x, w1, y, table, *accs):
    zero_rows(accs)

    def put(i):
        t = jnp.dot(x[rows_at(i), :], w1[...], preferred_element_type=F32)
        spread(table, i * BLOCK, t.astype(BF16).astype(F32))

    loop(x.shape[0] // BLOCK, put)
    edge_pass(s4, d4, w, cnt, table, accs, 4, 32, False)
    sum_rows(y, accs)


def one_halo_kernel(s4, d4, w, cnt, ids, y_own, x_prev, x_next, w1, w2t, hid_a, hid_b, t2, to_next, to_prev, table, picked, *accs):
    zero_rows(accs)
    half = x_prev.shape[0]

    def put(i):
        t = jnp.dot(x_prev[rows_at(i), :w1.shape[0]], w1[...], preferred_element_type=F32)
        spread(table, i * BLOCK, t.astype(BF16).astype(F32))
        t = jnp.dot(x_next[rows_at(i), :w1.shape[0]], w1[...], preferred_element_type=F32)
        spread(table, half + i * BLOCK, t.astype(BF16).astype(F32))

    loop(half // BLOCK, put)
    edge_pass(s4, d4, w, cnt, table, accs, 4, 16, True)
    sum_rows(accs[0], (y_own,) + accs)

    def act(i):
        h = jnp.maximum(unspread(accs[0], i * BLOCK, BLOCK, 4), 0.0).astype(BF16)
        cut = hid_a.shape[1]
        hid_a[rows_at(i), :] = h[:, :cut]
        hid_b[rows_at(i), :] = h[:, cut:]
        t = lax.dot_general(h, w2t[...], CONTRACT_COLS, preferred_element_type=F32)
        t2[rows_at(i), :] = t.astype(BF16).astype(F32)

    loop(t2.shape[0] // BLOCK, act)
    gather_pass(ids, t2, picked, 1)

    def take(i):
        to_next[rows_at(i), :] = picked[rows_at(i), :].astype(BF16)
        to_prev[rows_at(i), :] = picked[rows_at(i, half), :].astype(BF16)

    loop(half // BLOCK, take)


def narrow_own_kernel(frm, to, w, cnt, table, out, *accs):
    zero_rows(accs)
    edge_pass(frm, to, w, cnt, table, accs, 1, 32, False)
    sum_rows(out, accs)


def wide_own_kernel(frm, to, w, cnt, table, out, *accs):
    zero_rows(accs)
    edge_pass(frm, to, w, cnt, table, accs, 4, 32, False)
    sum_rows(out, accs)


def logits_kernel(classes, s, d, w, cnt, z_own, t_prev, t_next, labels, count, dz, back_prev, back_next, loss, table, *accs):
    zero_rows(accs)
    half = t_prev.shape[0]

    def put(i):
        table[rows_at(i), :] = t_prev[rows_at(i), :].astype(F32)
        table[rows_at(i, half), :] = t_next[rows_at(i), :].astype(F32)

    loop(half // BLOCK, put)
    edge_pass(s, d, w, cnt, table, accs, 1, 16, True)
    denom = count[0:1, :]
    loss[...] = jnp.zeros_like(loss)

    def soft(i):
        at = pl.ds(i * 64, 64)
        z = z_own[at, :]
        for acc in accs:
            z = z + acc[at, :]
        lane = lax.broadcasted_iota(jnp.int32, z.shape, 1)
        lab = labels[at, :]
        hot = lab == lane
        keep = lab >= 0
        zm = jnp.where(lane < classes, z, -jnp.inf)
        top = jnp.max(zm, axis=1, keepdims=True)
        ex = jnp.exp(zm - top)
        log_norm = jnp.log(jnp.sum(ex, axis=1, keepdims=True)) + top
        hot_f = jnp.where(hot, 1.0, 0.0)
        term = jnp.where(hot, log_norm - z, 0.0)
        part = term[0:8]
        for b in range(1, 8):
            part = part + term[b * 8:b * 8 + 8]
        loss[...] += part
        mask_f = jnp.where(keep, 1.0, 0.0)
        dz[at, :] = jnp.where(lane < classes, (jnp.exp(zm - log_norm) - hot_f) * (mask_f / denom), 0.0)

    loop(dz.shape[0] // 64, soft)
    zero_rows(accs)
    edge_pass(d, s, w, cnt, dz, accs, 1, 16, True)

    def fin(i):
        at = pl.ds(i * 64, 64)
        bt = pl.ds(half + i * 64, 64)
        a, b = accs[0][at, :], accs[0][bt, :]
        for acc in accs[1:]:
            a, b = a + acc[at, :], b + acc[bt, :]
        back_prev[at, :] = a
        back_next[at, :] = b

    loop(half // 64, fin)


def masked(grad, hid_a, hid_b):
    cut = hid_a.shape[1]
    lo = jnp.where(hid_a.astype(F32) > 0.0, grad[:, :cut], 0.0)
    hi = jnp.where(hid_b.astype(F32) > 0.0, grad[:, cut:], 0.0)
    return jnp.concatenate([lo, hi], axis=1)


def hidden_grad_kernel(ids, own, ret_next, ret_prev, hid_a, hid_b, w2t, dt2, dy, g2, *accs):
    n_loc, half = own.shape[0], ret_next.shape[0]
    zero_rows(accs)
    scatter_pass(ids.at[pl.ds(0, half)], ret_next, accs, 1, 8)
    scatter_pass(ids.at[pl.ds(half, half)], ret_prev, accs, 1, 8)
    g2[...] = jnp.zeros_like(g2)

    def fold(i):
        at = rows_at(i)
        total = own[at, :]
        for acc in accs:
            total = total + acc[at, :]
        dt = total.astype(BF16)
        dt2[at, :] = dt
        cut = hid_a.shape[1]
        g2[:cut, :] += lax.dot_general(hid_a[at, :], dt, CONTRACT_ROWS, preferred_element_type=F32)
        g2[cut:, :] += lax.dot_general(hid_b[at, :], dt, CONTRACT_ROWS, preferred_element_type=F32)
        dh = jnp.dot(dt, w2t[...], preferred_element_type=F32)
        spread(dy, i * BLOCK, masked(dh, hid_a[at, :], hid_b[at, :]))

    loop(n_loc // BLOCK, fold)


def peer_pass(ids, code_ref, w_ref, rows, far, table, accs):
    n_acc = len(accs)
    tally = rows * SLOT
    n_loc = ids.shape[0]
    shift = n_loc.bit_length() - 1

    def row(r):
        first = SLOT - 16 - (code_ref[tally + 2 * rows + r] if far else 0)
        edges = code_ref[tally + far * rows + r]

        def body(j):
            off = r * SLOT + first - j * 16
            codes, wgt = (ref.at[pl.ds(off, 16)] for ref in (code_ref, w_ref))
            for u in range(16):
                acc = accs[u % n_acc]
                code = codes[u]
                frm = lax.shift_right_logical(code, shift) * 4
                val = table[pl.ds(pl.multiple_of(frm, 4), 4), :] * wgt[u]
                at = pl.ds(pl.multiple_of(ids[code & (n_loc - 1)] * 4, 4), 4)
                acc[at, :] = acc[at, :] + val

        loop(lax.shift_right_logical(edges + 15, 4), body)

    loop(rows, row)


def table_grad_kernel(rows, ids, cn, wn, cp, wp, own, tn, han, hbn, tp, hap, hbp, w2t, x, g1, table, *accs):
    zero_rows(accs)
    g1[...] = jnp.zeros_like(g1)

    def fill(dt, hid_a, hid_b):
        def put(i):
            at = rows_at(i)
            dh = jnp.dot(dt[at, :], w2t[...], preferred_element_type=F32)
            spread(table, i * BLOCK, masked(dh, hid_a[at, :], hid_b[at, :]))

        loop(dt.shape[0] // BLOCK, put)

    fill(tn, han, hbn)
    peer_pass(ids, cn, wn, rows, 0, table, accs)
    fill(tp, hap, hbp)
    peer_pass(ids, cp, wp, rows, 1, table, accs)

    def fold(i):
        total = unspread(own, i * BLOCK, BLOCK, 4)
        for acc in accs:
            total = total + unspread(acc, i * BLOCK, BLOCK, 4)
        g1[:x.shape[1], :] += lax.dot_general(x[rows_at(i), :], total.astype(BF16), CONTRACT_ROWS, preferred_element_type=F32)

    loop(x.shape[0] // BLOCK, fold)


def reduce_kernel(num_dev, g1, g2, loss, count, o1, o2, lo, r1, r2, s1, s2, q1, q2, lslots, sem_s, sem_r, lsem_s, lsem_r):
    me = lax.axis_index(GRAPH_AXIS)
    core = lax.rem(me, 2)
    chip = me // 2
    mate = me + 1 - 2 * core
    h1, h2 = g1.shape[0] // 2, g2.shape[0] // 2
    e1, e2 = h1 // 4, h2 // 4
    enter(me, num_dev)
    other = 1 - core
    pair = [
        push(g1.at[pl.ds(pl.multiple_of(other * h1, h1), h1)], r1, sem_s.at[0], sem_r.at[0], mate),
        push(g2.at[pl.ds(pl.multiple_of(other * h2, h2), h2)], r2, sem_s.at[1], sem_r.at[1], mate),
    ]
    scalar = []
    for step in range(1, num_dev):
        scalar.append(push(loss, lslots.at[step - 1], lsem_s.at[step - 1], lsem_r.at[step - 1], lax.rem(me + step, num_dev)))
    for copy in pair:
        copy.wait()
    s1[...] = g1[pl.ds(pl.multiple_of(core * h1, h1), h1), :] + r1[...]
    s2[...] = g2[pl.ds(pl.multiple_of(core * h2, h2), h2), :] + r2[...]
    spreads = []
    for step in range(1, 4):
        far = lax.rem(chip + step, 4)
        dev = far * 2 + core
        k = 2 * step
        spreads.append(push(s1.at[pl.ds(pl.multiple_of(far * e1, e1), e1)], q1.at[step - 1], sem_s.at[k], sem_r.at[k], dev))
        spreads.append(push(s2.at[pl.ds(pl.multiple_of(far * e2, e2), e2)], q2.at[step - 1], sem_s.at[k + 1], sem_r.at[k + 1], dev))
    for copy in spreads:
        copy.wait()
    mine1 = pl.ds(pl.multiple_of(core * h1 + chip * e1, e1), e1)
    mine2 = pl.ds(pl.multiple_of(core * h2 + chip * e2, e2), e2)
    t1 = s1[pl.ds(pl.multiple_of(chip * e1, e1), e1), :]
    t2 = s2[pl.ds(pl.multiple_of(chip * e2, e2), e2), :]
    for step in range(3):
        t1 = t1 + q1[step]
        t2 = t2 + q2[step]
    o1[mine1, :] = t1
    o2[mine2, :] = t2
    gathers = []
    for step in range(1, 4):
        dev = lax.rem(chip + step, 4) * 2 + core
        k = 6 + 2 * step
        gathers.append((push(o1.at[mine1], o1.at[mine1], sem_s.at[k], sem_r.at[k], dev), push(o2.at[mine2], o2.at[mine2], sem_s.at[k + 1], sem_r.at[k + 1], dev)))
    tails = [push(o1.at[mine1], o1.at[mine1], sem_s.at[14], sem_r.at[14], mate), push(o2.at[mine2], o2.at[mine2], sem_s.at[15], sem_r.at[15], mate)]
    for step in range(1, 4):
        near = lax.rem(chip + 4 - step, 4)
        at1 = pl.ds(pl.multiple_of(core * h1 + near * e1, e1), e1)
        at2 = pl.ds(pl.multiple_of(core * h2 + near * e2, e2), e2)
        for copy in gathers[step - 1]:
            copy.wait()
        k = 14 + 2 * step
        tails.append(push(o1.at[at1], o1.at[at1], sem_s.at[k], sem_r.at[k], mate))
        tails.append(push(o2.at[at2], o2.at[at2], sem_s.at[k + 1], sem_r.at[k + 1], mate))
    for copy in scalar:
        copy.wait()
    total = loss[...]
    for step in range(num_dev - 1):
        total = total + lslots[step]
    total = jnp.sum(jnp.sum(total, axis=1, keepdims=True), axis=0, keepdims=True)
    lo[...] = total / count[...]
    for copy in tails:
        copy.wait()


def solution(mesh):
    num_dev = mesh.shape[GRAPH_AXIS]
    to_next = [(dev_id, (dev_id + 1) % num_dev) for dev_id in range(num_dev)]
    to_prev = [(dev_id, (dev_id - 1) % num_dev) for dev_id in range(num_dev)]

    def shift_next(a):
        return lax.ppermute(a, GRAPH_AXIS, to_next)

    def shift_prev(a):
        return lax.ppermute(a, GRAPH_AXIS, to_prev)

    def compact(edge_src, edge_dst, edge_w, n_loc, halo):
        rows = edge_src.shape[0] // CHUNK
        src, dst, w = (a.reshape(rows, CHUNK) for a in (edge_src, edge_dst, edge_w))
        live = w != 0.0
        own = live & (src < n_loc)
        far = live & (src >= n_loc + halo)
        near = live & (src >= n_loc) & (src < n_loc + halo)
        tri = (jnp.arange(CHUNK)[:, None] < jnp.arange(CHUNK)[None, :]).astype(BF16)
        sets = jnp.concatenate([own, near, far], axis=0).astype(BF16)
        rank = jnp.dot(sets, tri, preferred_element_type=F32).astype(jnp.int32)
        counts = jnp.sum(sets.astype(F32), axis=1).astype(jnp.int32)
        n_own, n_near, n_far = counts[:rows], counts[rows:2 * rows], counts[2 * rows:]
        skip = (n_near + 15) // 16 * 16
        place = jnp.where(far, SLOT - 1 - skip[:, None] - rank[2 * rows:], SLOT)
        place = jnp.where(near, SLOT - 1 - rank[rows:2 * rows], place)
        place = jnp.where(own, rank[:rows], place)
        hit = place[:, :, None] == jnp.arange(SLOT)[None, None, :]
        code = jnp.where(src < n_loc, src, src - n_loc) + dst * n_loc
        picks = (jnp.where(hit, code[:, :, None], 0), jnp.where(hit, w[:, :, None], 0.0))
        code, wc = lax.reduce(picks, (jnp.int32(0), jnp.float32(0.0)), lambda a, b: (a[0] + b[0], a[1] + b[1]), (1,))
        n_hal = jnp.where(n_far > 0, skip + n_far, n_near)
        return code, wc, n_own, n_hal, n_near, n_far, skip

    def device_step(node_feats, w_one, w_two, send_rows, edge_src, edge_dst, edge_w, labels, label_mask):
        n_loc, f_in = node_feats.shape
        halo = send_rows.shape[1]
        f_hid, classes = w_two.shape
        quad = 4 * n_loc
        sds = jax.ShapeDtypeStruct
        x = node_feats
        w1 = w_one.astype(BF16)
        w2t = jnp.pad(w_two.T.astype(BF16), ((0, LANES - classes), (0, 0)))
        ids = jnp.concatenate([send_rows[1], send_rows[0]])
        code, wc, n_own, n_hal, n_near, n_far, skip = compact(edge_src, edge_dst, edge_w, n_loc, halo)
        rows = n_own.shape[0]
        slots = code.size // LANES
        code, wc = code.reshape(-1), wc.reshape(-1)
        tally = jnp.concatenate([n_near, n_far, skip, jnp.zeros((8 * LANES - 3 * rows,), jnp.int32)])
        lists = jnp.concatenate([code, tally]).reshape(slots + 8, LANES)
        count, code_prev, code_next, w_prev, w_next = pl.pallas_call(
            functools.partial(lists_kernel, num_dev),
            out_shape=[sds((8, LANES), F32)] + [sds((slots + 8, LANES), jnp.int32)] * 2 + [sds((slots, LANES), F32)] * 2,
            in_specs=[VMEM_SPEC] * 3,
            out_specs=[VMEM_SPEC] * 5,
            scratch_shapes=[pltpu.VMEM((8, LANES), F32), pltpu.VMEM((num_dev - 1, 8, LANES), F32)] + [pltpu.SemaphoreType.DMA((n,)) for n in (num_dev - 1, num_dev - 1, 4, 4)],
            compiler_params=params(1, collective_id=0, has_side_effects=True),
            name="lists",
        )(label_mask.reshape(-1, LANES), lists, wc.reshape(slots, LANES))
        s, d = code % n_loc, code // n_loc
        s4, d4 = s * 4, d * 4
        count, x = lax.optimization_barrier((count, x))
        x_next, x_prev = pl.pallas_call(
            halo_rows_kernel,
            out_shape=[sds((halo, 256), BF16)] * 2,
            in_specs=[SMEM_SPEC, VMEM_SPEC],
            out_specs=[VMEM_SPEC] * 2,
            scratch_shapes=[pltpu.VMEM((2 * n_loc, LANES), F32), pltpu.VMEM((4 * halo, LANES), F32)],
            compiler_params=params(12),
            name="halo_rows",
        )(ids, x)
        xh_prev = shift_next(x_next)
        xh_next = shift_prev(x_prev)
        wide4 = [pltpu.VMEM((quad, LANES), F32)] * 4
        thin4 = [pltpu.VMEM((n_loc, LANES), F32)] * 4
        marks = jnp.where(label_mask == 1, labels, -1)
        s4, w2t, marks, ids = lax.optimization_barrier((s4, w2t, marks, ids))
        y_own = pl.pallas_call(
            one_own_kernel,
            out_shape=sds((quad, LANES), F32),
            in_specs=[SMEM_SPEC] * 4 + [VMEM_SPEC] * 2,
            out_specs=VMEM_SPEC,
            scratch_shapes=[pltpu.VMEM((quad, LANES), F32)] + wide4,
            compiler_params=params(28),
            cost_estimate=pl.CostEstimate(flops=200000000000, bytes_accessed=8000000, transcendentals=0),
            name="one_own",
        )(s4, d4, wc, n_own, x, w1)
        hid_a, hid_b, t2, t_next, t_prev = pl.pallas_call(
            one_halo_kernel,
            out_shape=[sds((n_loc, f_hid // 2), BF16)] * 2 + [sds((n_loc, LANES), F32), sds((halo, LANES), BF16), sds((halo, LANES), BF16)],
            in_specs=[SMEM_SPEC] * 5 + [VMEM_SPEC] * 5,
            out_specs=[VMEM_SPEC] * 5,
            scratch_shapes=[pltpu.VMEM((4 * 2 * halo, LANES), F32), pltpu.VMEM((2 * halo, LANES), F32)] + wide4,
            compiler_params=params(32),
            name="one_halo",
        )(s4, d4, wc, n_hal, ids, y_own, xh_prev, xh_next, w1, w2t)
        th_prev = shift_next(t_next)
        th_next = shift_prev(t_prev)
        ha_prev, ha_next = shift_next(hid_a), shift_prev(hid_a)
        narrow_own = functools.partial(
            pl.pallas_call,
            narrow_own_kernel,
            out_shape=sds((n_loc, LANES), F32),
            in_specs=[SMEM_SPEC] * 4 + [VMEM_SPEC],
            out_specs=VMEM_SPEC,
            scratch_shapes=thin4,
            compiler_params=params(10),
            cost_estimate=pl.CostEstimate(flops=200000000000, bytes_accessed=8000000, transcendentals=0),
        )
        z_own = narrow_own(name="two_own")(s, d, wc, n_own, t2)
        marks = jnp.broadcast_to(marks[:, None], (n_loc, LANES))
        dz, bz_prev, bz_next, loss = pl.pallas_call(
            functools.partial(logits_kernel, classes),
            out_shape=[sds((n_loc, LANES), F32), sds((halo, LANES), F32), sds((halo, LANES), F32), sds((8, LANES), F32)],
            in_specs=[SMEM_SPEC] * 4 + [VMEM_SPEC] * 5,
            out_specs=[VMEM_SPEC] * 4,
            scratch_shapes=[pltpu.VMEM((2 * halo, LANES), F32)] + thin4,
            compiler_params=params(12),
            name="logits",
        )(s, d, wc, n_hal, z_own, th_prev, th_next, marks, count)
        rz_next = shift_prev(bz_prev)
        rz_prev = shift_next(bz_next)
        late_b, _ = lax.optimization_barrier((hid_b, bz_prev))
        hb_prev, hb_next = shift_next(late_b), shift_prev(late_b)
        dt2_own = narrow_own(name="two_back_own")(d, s, wc, n_own, dz)
        dt2, dy, grad_two = pl.pallas_call(
            hidden_grad_kernel,
            out_shape=[sds((n_loc, LANES), BF16), sds((quad, LANES), F32), sds((f_hid, LANES), F32)],
            in_specs=[SMEM_SPEC] + [VMEM_SPEC] * 6,
            out_specs=[VMEM_SPEC] * 3,
            scratch_shapes=thin4,
            compiler_params=params(16),
            name="hidden_grad",
        )(ids, dt2_own, rz_next, rz_prev, hid_a, hid_b, w2t)
        dt_prev, dt_next = shift_next(dt2), shift_prev(dt2)
        dt1_own = pl.pallas_call(
            wide_own_kernel,
            out_shape=sds((quad, LANES), F32),
            in_specs=[SMEM_SPEC] * 4 + [VMEM_SPEC],
            out_specs=VMEM_SPEC,
            scratch_shapes=wide4,
            compiler_params=params(28),
            cost_estimate=pl.CostEstimate(flops=200000000000, bytes_accessed=8000000, transcendentals=0),
            name="one_back_own",
        )(d4, s4, wc, n_own, dy)
        grad_one = pl.pallas_call(
            functools.partial(table_grad_kernel, rows),
            out_shape=sds((256, f_hid), F32),
            in_specs=[SMEM_SPEC] * 5 + [VMEM_SPEC] * 9,
            out_specs=VMEM_SPEC,
            scratch_shapes=[pltpu.VMEM((quad, LANES), F32)] + wide4,
            compiler_params=params(36),
            name="table_grad",
        )(ids, code_next.reshape(-1), w_next.reshape(-1), code_prev.reshape(-1), w_prev.reshape(-1), dt1_own, dt_next, ha_next, hb_next, dt_prev, ha_prev, hb_prev, w2t, x)
        grad_one, grad_two, loss = pl.pallas_call(
            functools.partial(reduce_kernel, num_dev),
            out_shape=[sds((256, f_hid), F32), sds((f_hid, LANES), F32), sds((8, LANES), F32)],
            in_specs=[VMEM_SPEC] * 4,
            out_specs=[VMEM_SPEC] * 3,
            scratch_shapes=[
                pltpu.VMEM((128, f_hid), F32), pltpu.VMEM((f_hid // 2, LANES), F32),
                pltpu.VMEM((128, f_hid), F32), pltpu.VMEM((f_hid // 2, LANES), F32),
                pltpu.VMEM((3, 32, f_hid), F32), pltpu.VMEM((3, f_hid // 8, LANES), F32),
                pltpu.VMEM((num_dev - 1, 8, LANES), F32),
                pltpu.SemaphoreType.DMA((22,)), pltpu.SemaphoreType.DMA((22,)),
                pltpu.SemaphoreType.DMA((num_dev - 1,)), pltpu.SemaphoreType.DMA((num_dev - 1,)),
            ],
            compiler_params=params(8, collective_id=1, has_side_effects=True),
            name="reduce",
        )(grad_one, grad_two, loss, count)
        return loss[0, 0], grad_one[:f_in], grad_two[:, :classes]

    row_spec = P(GRAPH_AXIS)
    return jax.shard_map(device_step, mesh=mesh, in_specs=(row_spec, P(), P(), row_spec, row_spec, row_spec, row_spec, row_spec, row_spec), out_specs=(P(), P(), P()), check_vma=False)
```

```python
import functools

import jax
import jax.numpy as jnp
from jax import lax
from jax.experimental import pallas as pl
from jax.experimental.pallas import tpu as pltpu
from jax.sharding import PartitionSpec as P


GRAPH_AXIS = "graph"
CONTRACT_ROWS = (((0,), (0,)), ((), ()))
CONTRACT_COLS = (((1,), (1,)), ((), ()))
MESH = pl.DeviceIdType.MESH
F32 = jnp.float32
BF16 = jnp.bfloat16
LANES = 128
BLOCK = 256
CHUNK = 256
SLOT = 384

SMEM_SPEC = pl.BlockSpec(memory_space=pltpu.SMEM)
VMEM_SPEC = pl.BlockSpec(memory_space=pltpu.VMEM)


def rows_at(i, base=0, size=BLOCK):
    return pl.ds(base + i * size, size)


def loop(count, body):
    lax.fori_loop(0, count, lambda i, _: (body(i), 0)[1], 0)


def params(mib, **kw):
    return pltpu.CompilerParams(vmem_limit_bytes=mib * 2**20, **kw)


def zero_rows(refs):
    rows = refs[0].shape[0]

    def body(i):
        for ref in refs:
            ref[pl.ds(i * 64, 64), :] = jnp.zeros((64, LANES), F32)

    loop(rows // 64, body)


def sum_rows(out, refs):
    rows = refs[0].shape[0]

    def body(i):
        total = refs[0][pl.ds(i * 64, 64), :]
        for ref in refs[1:]:
            total = total + ref[pl.ds(i * 64, 64), :]
        out[pl.ds(i * 64, 64), :] = total

    loop(rows // 64, body)


def edge_pass(from_ref, to_ref, w_ref, cnt_ref, table, accs, width, unroll, back):
    n_acc = len(accs)
    shift = unroll.bit_length() - 1

    def row(r):
        blocks = lax.shift_right_logical(cnt_ref[r] + (unroll - 1), shift)

        def body(j):
            off = r * SLOT + (SLOT - unroll - j * unroll if back else j * unroll)
            frm, to = (ref.at[pl.ds(off, unroll)] for ref in (from_ref, to_ref))
            if back:
                wgt = w_ref.at[pl.ds(off, unroll)]
            else:
                wgt = [jnp.broadcast_to(w_ref[pl.ds(r * CHUNK + j * unroll + u, 1), :], (width, LANES)) for u in range(unroll)]
            for u in range(unroll):
                acc = accs[u % n_acc]
                val = table[pl.ds(pl.multiple_of(frm[u], width), width), :] * wgt[u]
                at = pl.ds(pl.multiple_of(to[u], width), width)
                acc[at, :] = acc[at, :] + val

        loop(blocks, body)

    loop(cnt_ref.shape[0], row)


def scatter_pass(ids_ref, table, accs, width, unroll):
    n_acc = len(accs)

    def body(j):
        off = j * unroll
        for g in range(unroll // n_acc):
            rows = [pl.multiple_of(ids_ref[off + g * n_acc + k], width) for k in range(n_acc)]
            vals = [table[pl.ds(pl.multiple_of((off + g * n_acc + k) * width, width), width), :] for k in range(n_acc)]
            old = [accs[k][pl.ds(rows[k], width), :] for k in range(n_acc)]
            for k in range(n_acc):
                accs[k][pl.ds(rows[k], width), :] = old[k] + vals[k]

    loop(ids_ref.shape[0] // unroll, body)


def gather_pass(ids_ref, table, out, width, unroll=16):
    def body(j):
        for u in range(unroll):
            i = j * unroll + u
            out[pl.ds(pl.multiple_of(i * width, width), width), :] = table[pl.ds(pl.multiple_of(ids_ref[i] * width, width), width), :]

    loop(ids_ref.shape[0] // unroll, body)


def spread(table, start, block):
    tiles = block.shape[1] // LANES
    for c in range(tiles):
        table[pl.ds(start * tiles + c, block.shape[0], tiles), :] = block[:, c * LANES:(c + 1) * LANES]


def unspread(table, start, rows, tiles):
    return jnp.concatenate([table[pl.ds(start * tiles + c, rows, tiles), :] for c in range(tiles)], axis=1)


def enter(me, num_dev):
    barrier = pltpu.get_barrier_semaphore()
    for step in range(1, num_dev):
        pl.semaphore_signal(barrier, inc=1, device_id=(lax.rem(me + step, num_dev),), device_id_type=MESH)
    pl.semaphore_wait(barrier, num_dev - 1)


def push(src, dst, send_sem, recv_sem, dev):
    copy = pltpu.make_async_remote_copy(src_ref=src, dst_ref=dst, send_sem=send_sem, recv_sem=recv_sem, device_id=(dev,), device_id_type=MESH)
    copy.start()
    return copy


def lists_kernel(num_dev, mask, code, wgt, count, code_prev, code_next, w_prev, w_next, part, slots, send_sem, recv_sem, lsend, lrecv):
    ones = jnp.sum(jnp.sum(mask[...].astype(F32), axis=1, keepdims=True), axis=0, keepdims=True)
    part[...] = jnp.broadcast_to(ones, part.shape)
    me = lax.axis_index(GRAPH_AXIS)
    succ, pred = lax.rem(me + 1, num_dev), lax.rem(me + num_dev - 1, num_dev)
    enter(me, num_dev)
    copies = []
    for step in range(1, num_dev):
        copies.append(push(part, slots.at[step - 1], send_sem.at[step - 1], recv_sem.at[step - 1], lax.rem(me + step, num_dev)))
    copies.append(push(code, code_prev, lsend.at[0], lrecv.at[0], succ))
    copies.append(push(code, code_next, lsend.at[1], lrecv.at[1], pred))
    copies.append(push(wgt, w_prev, lsend.at[2], lrecv.at[2], succ))
    copies.append(push(wgt, w_next, lsend.at[3], lrecv.at[3], pred))
    for copy in copies:
        copy.wait()
    total = part[...]
    for step in range(num_dev - 1):
        total = total + slots[step]
    count[...] = jnp.maximum(total, 1.0)


def halo_rows_kernel(ids, x, to_next, to_prev, table, picked):
    rows = x.shape[0]

    def put(i):
        block = x[rows_at(i), :].astype(F32)
        pad = jnp.zeros((BLOCK, 2 * LANES - block.shape[1]), F32)
        spread(table, i * BLOCK, jnp.concatenate([block, pad], axis=1))

    loop(rows // BLOCK, put)
    gather_pass(ids, table, picked, 2)
    half = to_next.shape[0]

    def take(i):
        to_next[rows_at(i), :] = unspread(picked, i * BLOCK, BLOCK, 2).astype(BF16)
        to_prev[rows_at(i), :] = unspread(picked, half + i * BLOCK, BLOCK, 2).astype(BF16)

    loop(half // BLOCK, take)


def one_own_kernel(s4, d4, cnt, x, w1, w, y, table, *accs):
    zero_rows(accs)

    def put(i):
        t = jnp.dot(x[rows_at(i), :], w1[...], preferred_element_type=F32)
        spread(table, i * BLOCK, t.astype(BF16).astype(F32))

    loop(x.shape[0] // BLOCK, put)
    edge_pass(s4, d4, w, cnt, table, accs, 4, 32, False)
    sum_rows(y, accs)


def one_halo_kernel(s4, d4, w, cnt, ids, y_own, x_prev, x_next, w1, w2t, hid_a, hid_b, t2, to_next, to_prev, table, picked, *accs):
    zero_rows(accs)
    half = x_prev.shape[0]

    def put(i):
        t = jnp.dot(x_prev[rows_at(i), :w1.shape[0]], w1[...], preferred_element_type=F32)
        spread(table, i * BLOCK, t.astype(BF16).astype(F32))
        t = jnp.dot(x_next[rows_at(i), :w1.shape[0]], w1[...], preferred_element_type=F32)
        spread(table, half + i * BLOCK, t.astype(BF16).astype(F32))

    loop(half // BLOCK, put)
    edge_pass(s4, d4, w, cnt, table, accs, 4, 16, True)
    sum_rows(accs[0], (y_own,) + accs)

    def act(i):
        h = jnp.maximum(unspread(accs[0], i * BLOCK, BLOCK, 4), 0.0).astype(BF16)
        cut = hid_a.shape[1]
        hid_a[rows_at(i), :] = h[:, :cut]
        hid_b[rows_at(i), :] = h[:, cut:]
        t = lax.dot_general(h, w2t[...], CONTRACT_COLS, preferred_element_type=F32)
        t2[rows_at(i), :] = t.astype(BF16).astype(F32)

    loop(t2.shape[0] // BLOCK, act)
    gather_pass(ids, t2, picked, 1)

    def take(i):
        to_next[rows_at(i), :] = picked[rows_at(i), :].astype(BF16)
        to_prev[rows_at(i), :] = picked[rows_at(i, half), :].astype(BF16)

    loop(half // BLOCK, take)


def narrow_own_kernel(frm, to, cnt, table, w, out, *accs):
    zero_rows(accs)
    edge_pass(frm, to, w, cnt, table, accs, 1, 32, False)
    sum_rows(out, accs)


def wide_own_kernel(frm, to, cnt, table, w, out, *accs):
    zero_rows(accs)
    edge_pass(frm, to, w, cnt, table, accs, 4, 32, False)
    sum_rows(out, accs)


def logits_kernel(classes, s, d, w, cnt, z_own, t_prev, t_next, labels, count, dz, back_prev, back_next, loss, table, *accs):
    zero_rows(accs)
    half = t_prev.shape[0]

    def put(i):
        table[rows_at(i), :] = t_prev[rows_at(i), :].astype(F32)
        table[rows_at(i, half), :] = t_next[rows_at(i), :].astype(F32)

    loop(half // BLOCK, put)
    edge_pass(s, d, w, cnt, table, accs, 1, 16, True)
    denom = count[0:1, :]
    loss[...] = jnp.zeros_like(loss)

    def soft(i):
        at = pl.ds(i * 64, 64)
        z = z_own[at, :]
        for acc in accs:
            z = z + acc[at, :]
        lane = lax.broadcasted_iota(jnp.int32, z.shape, 1)
        lab = labels[at, :]
        hot = lab == lane
        keep = lab >= 0
        zm = jnp.where(lane < classes, z, -jnp.inf)
        top = jnp.max(zm, axis=1, keepdims=True)
        ex = jnp.exp(zm - top)
        log_norm = jnp.log(jnp.sum(ex, axis=1, keepdims=True)) + top
        hot_f = jnp.where(hot, 1.0, 0.0)
        term = jnp.where(hot, log_norm - z, 0.0)
        part = term[0:8]
        for b in range(1, 8):
            part = part + term[b * 8:b * 8 + 8]
        loss[...] += part
        mask_f = jnp.where(keep, 1.0, 0.0)
        dz[at, :] = jnp.where(lane < classes, (jnp.exp(zm - log_norm) - hot_f) * (mask_f / denom), 0.0)

    loop(dz.shape[0] // 64, soft)
    zero_rows(accs)
    edge_pass(d, s, w, cnt, dz, accs, 1, 16, True)

    def fin(i):
        at = pl.ds(i * 64, 64)
        bt = pl.ds(half + i * 64, 64)
        a, b = accs[0][at, :], accs[0][bt, :]
        for acc in accs[1:]:
            a, b = a + acc[at, :], b + acc[bt, :]
        back_prev[at, :] = a
        back_next[at, :] = b

    loop(half // 64, fin)


def masked(grad, hid_a, hid_b):
    cut = hid_a.shape[1]
    lo = jnp.where(hid_a.astype(F32) > 0.0, grad[:, :cut], 0.0)
    hi = jnp.where(hid_b.astype(F32) > 0.0, grad[:, cut:], 0.0)
    return jnp.concatenate([lo, hi], axis=1)


def hidden_grad_kernel(ids, own, ret_next, ret_prev, hid_a, hid_b, w2t, dt2, dy, g2, *accs):
    n_loc, half = own.shape[0], ret_next.shape[0]
    zero_rows(accs)
    scatter_pass(ids.at[pl.ds(0, half)], ret_next, accs, 1, 8)
    scatter_pass(ids.at[pl.ds(half, half)], ret_prev, accs, 1, 8)
    g2[...] = jnp.zeros_like(g2)

    def fold(i):
        at = rows_at(i)
        total = own[at, :]
        for acc in accs:
            total = total + acc[at, :]
        dt = total.astype(BF16)
        dt2[at, :] = dt
        cut = hid_a.shape[1]
        g2[:cut, :] += lax.dot_general(hid_a[at, :], dt, CONTRACT_ROWS, preferred_element_type=F32)
        g2[cut:, :] += lax.dot_general(hid_b[at, :], dt, CONTRACT_ROWS, preferred_element_type=F32)
        dh = jnp.dot(dt, w2t[...], preferred_element_type=F32)
        spread(dy, i * BLOCK, masked(dh, hid_a[at, :], hid_b[at, :]))

    loop(n_loc // BLOCK, fold)


def peer_pass(ids, code_ref, w_ref, rows, far, table, accs):
    n_acc = len(accs)
    tally = rows * SLOT
    n_loc = ids.shape[0]
    shift = n_loc.bit_length() - 1

    def row(r):
        first = SLOT - 16 - (code_ref[tally + 2 * rows + r] if far else 0)
        edges = code_ref[tally + far * rows + r]

        def body(j):
            off = r * SLOT + first - j * 16
            codes, wgt = (ref.at[pl.ds(off, 16)] for ref in (code_ref, w_ref))
            for u in range(16):
                acc = accs[u % n_acc]
                code = codes[u]
                frm = lax.shift_right_logical(code, shift) * 4
                val = table[pl.ds(pl.multiple_of(frm, 4), 4), :] * wgt[u]
                at = pl.ds(pl.multiple_of(ids[code & (n_loc - 1)] * 4, 4), 4)
                acc[at, :] = acc[at, :] + val

        loop(lax.shift_right_logical(edges + 15, 4), body)

    loop(rows, row)


def table_grad_kernel(rows, ids, cn, wn, cp, wp, own, tn, han, hbn, tp, hap, hbp, w2t, x, g1, table, *accs):
    zero_rows(accs)
    g1[...] = jnp.zeros_like(g1)

    def fill(dt, hid_a, hid_b):
        def put(i):
            at = rows_at(i)
            dh = jnp.dot(dt[at, :], w2t[...], preferred_element_type=F32)
            spread(table, i * BLOCK, masked(dh, hid_a[at, :], hid_b[at, :]))

        loop(dt.shape[0] // BLOCK, put)

    fill(tn, han, hbn)
    peer_pass(ids, cn, wn, rows, 0, table, accs)
    fill(tp, hap, hbp)
    peer_pass(ids, cp, wp, rows, 1, table, accs)

    def fold(i):
        total = unspread(own, i * BLOCK, BLOCK, 4)
        for acc in accs:
            total = total + unspread(acc, i * BLOCK, BLOCK, 4)
        g1[:x.shape[1], :] += lax.dot_general(x[rows_at(i), :], total.astype(BF16), CONTRACT_ROWS, preferred_element_type=F32)

    loop(x.shape[0] // BLOCK, fold)


def reduce_kernel(num_dev, g1, g2, loss, count, o1, o2, lo, r1, r2, s1, s2, q1, q2, lslots, sem_s, sem_r, lsem_s, lsem_r):
    me = lax.axis_index(GRAPH_AXIS)
    core = lax.rem(me, 2)
    chip = me // 2
    mate = me + 1 - 2 * core
    h1, h2 = g1.shape[0] // 2, g2.shape[0] // 2
    e1, e2 = h1 // 4, h2 // 4
    enter(me, num_dev)
    other = 1 - core
    pair = [
        push(g1.at[pl.ds(pl.multiple_of(other * h1, h1), h1)], r1, sem_s.at[0], sem_r.at[0], mate),
        push(g2.at[pl.ds(pl.multiple_of(other * h2, h2), h2)], r2, sem_s.at[1], sem_r.at[1], mate),
    ]
    scalar = []
    for step in range(1, num_dev):
        scalar.append(push(loss, lslots.at[step - 1], lsem_s.at[step - 1], lsem_r.at[step - 1], lax.rem(me + step, num_dev)))
    for copy in pair:
        copy.wait()
    s1[...] = g1[pl.ds(pl.multiple_of(core * h1, h1), h1), :] + r1[...]
    s2[...] = g2[pl.ds(pl.multiple_of(core * h2, h2), h2), :] + r2[...]
    spreads = []
    for step in range(1, 4):
        far = lax.rem(chip + step, 4)
        dev = far * 2 + core
        k = 2 * step
        spreads.append(push(s1.at[pl.ds(pl.multiple_of(far * e1, e1), e1)], q1.at[step - 1], sem_s.at[k], sem_r.at[k], dev))
        spreads.append(push(s2.at[pl.ds(pl.multiple_of(far * e2, e2), e2)], q2.at[step - 1], sem_s.at[k + 1], sem_r.at[k + 1], dev))
    for copy in spreads:
        copy.wait()
    mine1 = pl.ds(pl.multiple_of(core * h1 + chip * e1, e1), e1)
    mine2 = pl.ds(pl.multiple_of(core * h2 + chip * e2, e2), e2)
    t1 = s1[pl.ds(pl.multiple_of(chip * e1, e1), e1), :]
    t2 = s2[pl.ds(pl.multiple_of(chip * e2, e2), e2), :]
    for step in range(3):
        t1 = t1 + q1[step]
        t2 = t2 + q2[step]
    o1[mine1, :] = t1
    o2[mine2, :] = t2
    gathers = []
    for step in range(1, 4):
        dev = lax.rem(chip + step, 4) * 2 + core
        k = 6 + 2 * step
        gathers.append((push(o1.at[mine1], o1.at[mine1], sem_s.at[k], sem_r.at[k], dev), push(o2.at[mine2], o2.at[mine2], sem_s.at[k + 1], sem_r.at[k + 1], dev)))
    tails = [push(o1.at[mine1], o1.at[mine1], sem_s.at[14], sem_r.at[14], mate), push(o2.at[mine2], o2.at[mine2], sem_s.at[15], sem_r.at[15], mate)]
    for step in range(1, 4):
        near = lax.rem(chip + 4 - step, 4)
        at1 = pl.ds(pl.multiple_of(core * h1 + near * e1, e1), e1)
        at2 = pl.ds(pl.multiple_of(core * h2 + near * e2, e2), e2)
        for copy in gathers[step - 1]:
            copy.wait()
        k = 14 + 2 * step
        tails.append(push(o1.at[at1], o1.at[at1], sem_s.at[k], sem_r.at[k], mate))
        tails.append(push(o2.at[at2], o2.at[at2], sem_s.at[k + 1], sem_r.at[k + 1], mate))
    for copy in scalar:
        copy.wait()
    total = loss[...]
    for step in range(num_dev - 1):
        total = total + lslots[step]
    total = jnp.sum(jnp.sum(total, axis=1, keepdims=True), axis=0, keepdims=True)
    lo[...] = total / count[...]
    for copy in tails:
        copy.wait()


def solution(mesh):
    num_dev = mesh.shape[GRAPH_AXIS]
    to_next = [(dev_id, (dev_id + 1) % num_dev) for dev_id in range(num_dev)]
    to_prev = [(dev_id, (dev_id - 1) % num_dev) for dev_id in range(num_dev)]

    def shift_next(a):
        return lax.ppermute(a, GRAPH_AXIS, to_next)

    def shift_prev(a):
        return lax.ppermute(a, GRAPH_AXIS, to_prev)

    def compact(edge_src, edge_dst, edge_w, n_loc, halo):
        rows = edge_src.shape[0] // CHUNK
        src, dst, w = (a.reshape(rows, CHUNK) for a in (edge_src, edge_dst, edge_w))
        live = w != 0.0
        own = live & (src < n_loc)
        far = live & (src >= n_loc + halo)
        near = live & (src >= n_loc) & (src < n_loc + halo)
        tri = (jnp.arange(CHUNK)[:, None] < jnp.arange(CHUNK)[None, :]).astype(BF16)
        sets = jnp.concatenate([own, near, far], axis=0).astype(BF16)
        rank = jnp.dot(sets, tri, preferred_element_type=F32).astype(jnp.int32)
        counts = jnp.sum(sets.astype(F32), axis=1).astype(jnp.int32)
        n_own, n_near, n_far = counts[:rows], counts[rows:2 * rows], counts[2 * rows:]
        skip = (n_near + 15) // 16 * 16
        place = jnp.where(far, SLOT - 1 - skip[:, None] - rank[2 * rows:], SLOT)
        place = jnp.where(near, SLOT - 1 - rank[rows:2 * rows], place)
        place = jnp.where(own, rank[:rows], place)
        hit = place[:, :, None] == jnp.arange(SLOT)[None, None, :]
        code = jnp.where(src < n_loc, src, src - n_loc) + dst * n_loc
        picks = (jnp.where(hit, code[:, :, None], 0), jnp.where(hit, w[:, :, None], 0.0))
        code, wc = lax.reduce(picks, (jnp.int32(0), jnp.float32(0.0)), lambda a, b: (a[0] + b[0], a[1] + b[1]), (1,))
        n_hal = jnp.where(n_far > 0, skip + n_far, n_near)
        return code, wc, n_own, n_hal, n_near, n_far, skip

    def device_step(node_feats, w_one, w_two, send_rows, edge_src, edge_dst, edge_w, labels, label_mask):
        n_loc, f_in = node_feats.shape
        halo = send_rows.shape[1]
        f_hid, classes = w_two.shape
        quad = 4 * n_loc
        sds = jax.ShapeDtypeStruct
        x = node_feats
        w1 = w_one.astype(BF16)
        w2t = jnp.pad(w_two.T.astype(BF16), ((0, LANES - classes), (0, 0)))
        ids = jnp.concatenate([send_rows[1], send_rows[0]])
        code, wc, n_own, n_hal, n_near, n_far, skip = compact(edge_src, edge_dst, edge_w, n_loc, halo)
        rows = n_own.shape[0]
        slots = code.size // LANES
        w_own = jnp.broadcast_to(wc[:, :CHUNK].reshape(-1, 1), (rows * CHUNK, LANES))
        code, wc = code.reshape(-1), wc.reshape(-1)
        tally = jnp.concatenate([n_near, n_far, skip, jnp.zeros((8 * LANES - 3 * rows,), jnp.int32)])
        lists = jnp.concatenate([code, tally]).reshape(slots + 8, LANES)
        count, code_prev, code_next, w_prev, w_next = pl.pallas_call(
            functools.partial(lists_kernel, num_dev),
            out_shape=[sds((8, LANES), F32)] + [sds((slots + 8, LANES), jnp.int32)] * 2 + [sds((slots, LANES), F32)] * 2,
            in_specs=[VMEM_SPEC] * 3,
            out_specs=[VMEM_SPEC] * 5,
            scratch_shapes=[pltpu.VMEM((8, LANES), F32), pltpu.VMEM((num_dev - 1, 8, LANES), F32)] + [pltpu.SemaphoreType.DMA((n,)) for n in (num_dev - 1, num_dev - 1, 4, 4)],
            compiler_params=params(1, collective_id=0, has_side_effects=True),
            name="lists",
        )(label_mask.reshape(-1, LANES), lists, wc.reshape(slots, LANES))
        s, d = code % n_loc, code // n_loc
        s4, d4 = s * 4, d * 4
        count, x = lax.optimization_barrier((count, x))
        x_next, x_prev = pl.pallas_call(
            halo_rows_kernel,
            out_shape=[sds((halo, 256), BF16)] * 2,
            in_specs=[SMEM_SPEC, VMEM_SPEC],
            out_specs=[VMEM_SPEC] * 2,
            scratch_shapes=[pltpu.VMEM((2 * n_loc, LANES), F32), pltpu.VMEM((4 * halo, LANES), F32)],
            compiler_params=params(12),
            name="halo_rows",
        )(ids, x)
        xh_prev = shift_next(x_next)
        xh_next = shift_prev(x_prev)
        wide4 = [pltpu.VMEM((quad, LANES), F32)] * 4
        thin4 = [pltpu.VMEM((n_loc, LANES), F32)] * 4
        marks = jnp.where(label_mask == 1, labels, -1)
        s4, w2t, marks, ids, w_own, wc = lax.optimization_barrier((s4, w2t, marks, ids, w_own, wc))
        y_own = pl.pallas_call(
            one_own_kernel,
            out_shape=sds((quad, LANES), F32),
            in_specs=[SMEM_SPEC] * 3 + [VMEM_SPEC] * 3,
            out_specs=VMEM_SPEC,
            scratch_shapes=[pltpu.VMEM((quad, LANES), F32)] + wide4,
            compiler_params=params(32),
            cost_estimate=pl.CostEstimate(flops=200000000000, bytes_accessed=8000000, transcendentals=0),
            name="one_own",
        )(s4, d4, n_own, x, w1, w_own)
        hid_a, hid_b, t2, t_next, t_prev = pl.pallas_call(
            one_halo_kernel,
            out_shape=[sds((n_loc, f_hid // 2), BF16)] * 2 + [sds((n_loc, LANES), F32), sds((halo, LANES), BF16), sds((halo, LANES), BF16)],
            in_specs=[SMEM_SPEC] * 5 + [VMEM_SPEC] * 5,
            out_specs=[VMEM_SPEC] * 5,
            scratch_shapes=[pltpu.VMEM((4 * 2 * halo, LANES), F32), pltpu.VMEM((2 * halo, LANES), F32)] + wide4,
            compiler_params=params(32),
            name="one_halo",
        )(s4, d4, wc, n_hal, ids, y_own, xh_prev, xh_next, w1, w2t)
        th_prev = shift_next(t_next)
        th_next = shift_prev(t_prev)
        ha_prev, ha_next = shift_next(hid_a), shift_prev(hid_a)
        narrow_own = functools.partial(
            pl.pallas_call,
            narrow_own_kernel,
            out_shape=sds((n_loc, LANES), F32),
            in_specs=[SMEM_SPEC] * 3 + [VMEM_SPEC] * 2,
            out_specs=VMEM_SPEC,
            scratch_shapes=thin4,
            compiler_params=params(14),
            cost_estimate=pl.CostEstimate(flops=200000000000, bytes_accessed=8000000, transcendentals=0),
        )
        z_own = narrow_own(name="two_own")(s, d, n_own, t2, w_own)
        marks = jnp.broadcast_to(marks[:, None], (n_loc, LANES))
        dz, bz_prev, bz_next, loss = pl.pallas_call(
            functools.partial(logits_kernel, classes),
            out_shape=[sds((n_loc, LANES), F32), sds((halo, LANES), F32), sds((halo, LANES), F32), sds((8, LANES), F32)],
            in_specs=[SMEM_SPEC] * 4 + [VMEM_SPEC] * 5,
            out_specs=[VMEM_SPEC] * 4,
            scratch_shapes=[pltpu.VMEM((2 * halo, LANES), F32)] + thin4,
            compiler_params=params(12),
            name="logits",
        )(s, d, wc, n_hal, z_own, th_prev, th_next, marks, count)
        rz_next = shift_prev(bz_prev)
        rz_prev = shift_next(bz_next)
        late_b, _ = lax.optimization_barrier((hid_b, bz_prev))
        hb_prev, hb_next = shift_next(late_b), shift_prev(late_b)
        dt2_own = narrow_own(name="two_back_own")(d, s, n_own, dz, w_own)
        dt2, dy, grad_two = pl.pallas_call(
            hidden_grad_kernel,
            out_shape=[sds((n_loc, LANES), BF16), sds((quad, LANES), F32), sds((f_hid, LANES), F32)],
            in_specs=[SMEM_SPEC] + [VMEM_SPEC] * 6,
            out_specs=[VMEM_SPEC] * 3,
            scratch_shapes=thin4,
            compiler_params=params(16),
            name="hidden_grad",
        )(ids, dt2_own, rz_next, rz_prev, hid_a, hid_b, w2t)
        dt_prev, dt_next = shift_next(dt2), shift_prev(dt2)
        dt1_own = pl.pallas_call(
            wide_own_kernel,
            out_shape=sds((quad, LANES), F32),
            in_specs=[SMEM_SPEC] * 3 + [VMEM_SPEC] * 2,
            out_specs=VMEM_SPEC,
            scratch_shapes=wide4,
            compiler_params=params(32),
            cost_estimate=pl.CostEstimate(flops=200000000000, bytes_accessed=8000000, transcendentals=0),
            name="one_back_own",
        )(d4, s4, n_own, dy, w_own)
        grad_one = pl.pallas_call(
            functools.partial(table_grad_kernel, rows),
            out_shape=sds((256, f_hid), F32),
            in_specs=[SMEM_SPEC] * 5 + [VMEM_SPEC] * 9,
            out_specs=VMEM_SPEC,
            scratch_shapes=[pltpu.VMEM((quad, LANES), F32)] + wide4,
            compiler_params=params(36),
            name="table_grad",
        )(ids, code_next.reshape(-1), w_next.reshape(-1), code_prev.reshape(-1), w_prev.reshape(-1), dt1_own, dt_next, ha_next, hb_next, dt_prev, ha_prev, hb_prev, w2t, x)
        grad_one, grad_two, loss = pl.pallas_call(
            functools.partial(reduce_kernel, num_dev),
            out_shape=[sds((256, f_hid), F32), sds((f_hid, LANES), F32), sds((8, LANES), F32)],
            in_specs=[VMEM_SPEC] * 4,
            out_specs=[VMEM_SPEC] * 3,
            scratch_shapes=[
                pltpu.VMEM((128, f_hid), F32), pltpu.VMEM((f_hid // 2, LANES), F32),
                pltpu.VMEM((128, f_hid), F32), pltpu.VMEM((f_hid // 2, LANES), F32),
                pltpu.VMEM((3, 32, f_hid), F32), pltpu.VMEM((3, f_hid // 8, LANES), F32),
                pltpu.VMEM((num_dev - 1, 8, LANES), F32),
                pltpu.SemaphoreType.DMA((22,)), pltpu.SemaphoreType.DMA((22,)),
                pltpu.SemaphoreType.DMA((num_dev - 1,)), pltpu.SemaphoreType.DMA((num_dev - 1,)),
            ],
            compiler_params=params(8, collective_id=1, has_side_effects=True),
            name="reduce",
        )(grad_one, grad_two, loss, count)
        return loss[0, 0], grad_one[:f_in], grad_two[:, :classes]

    row_spec = P(GRAPH_AXIS)
    return jax.shard_map(device_step, mesh=mesh, in_specs=(row_spec, P(), P(), row_spec, row_spec, row_spec, row_spec, row_spec, row_spec), out_specs=(P(), P(), P()), check_vma=False)
```

```python
import functools

import jax
import jax.numpy as jnp
from jax import lax
from jax.experimental import pallas as pl
from jax.experimental.pallas import tpu as pltpu
from jax.sharding import PartitionSpec as P


GRAPH_AXIS = "graph"
CONTRACT_ROWS = (((0,), (0,)), ((), ()))
CONTRACT_COLS = (((1,), (1,)), ((), ()))
MESH = pl.DeviceIdType.MESH
F32 = jnp.float32
BF16 = jnp.bfloat16
LANES = 128
BLOCK = 256
CHUNK = 256
SLOT = 384

SMEM_SPEC = pl.BlockSpec(memory_space=pltpu.SMEM)
VMEM_SPEC = pl.BlockSpec(memory_space=pltpu.VMEM)


def rows_at(i, base=0, size=BLOCK):
    return pl.ds(base + i * size, size)


def loop(count, body):
    lax.fori_loop(0, count, lambda i, _: (body(i), 0)[1], 0)


def params(mib, **kw):
    return pltpu.CompilerParams(vmem_limit_bytes=mib * 2**20, **kw)


def zero_rows(refs):
    rows = refs[0].shape[0]

    def body(i):
        for ref in refs:
            ref[pl.ds(i * 64, 64), :] = jnp.zeros((64, LANES), F32)

    loop(rows // 64, body)


def sum_rows(out, refs):
    rows = refs[0].shape[0]

    def body(i):
        total = refs[0][pl.ds(i * 64, 64), :]
        for ref in refs[1:]:
            total = total + ref[pl.ds(i * 64, 64), :]
        out[pl.ds(i * 64, 64), :] = total

    loop(rows // 64, body)


def edge_pass(from_ref, to_ref, w_ref, cnt_ref, table, accs, width, unroll, back):
    n_acc = len(accs)
    shift = unroll.bit_length() - 1

    def row(r):
        blocks = lax.shift_right_logical(cnt_ref[r] + (unroll - 1), shift)

        def body(j):
            off = r * SLOT + (SLOT - unroll - j * unroll if back else j * unroll)
            frm, to = (ref.at[pl.ds(off, unroll)] for ref in (from_ref, to_ref))
            if back:
                wgt = w_ref.at[pl.ds(off, unroll)]
            else:
                wgt = [jnp.broadcast_to(w_ref[pl.ds(r * CHUNK + j * unroll + u, 1), :], (width, LANES)) for u in range(unroll)]
            for u in range(unroll):
                acc = accs[u % n_acc]
                val = table[pl.ds(pl.multiple_of(frm[u], width), width), :] * wgt[u]
                at = pl.ds(pl.multiple_of(to[u], width), width)
                acc[at, :] = acc[at, :] + val

        loop(blocks, body)

    loop(cnt_ref.shape[0], row)


def scatter_pass(ids_ref, table, accs, width, unroll):
    n_acc = len(accs)

    def body(j):
        off = j * unroll
        for g in range(unroll // n_acc):
            rows = [pl.multiple_of(ids_ref[off + g * n_acc + k], width) for k in range(n_acc)]
            vals = [table[pl.ds(pl.multiple_of((off + g * n_acc + k) * width, width), width), :] for k in range(n_acc)]
            old = [accs[k][pl.ds(rows[k], width), :] for k in range(n_acc)]
            for k in range(n_acc):
                accs[k][pl.ds(rows[k], width), :] = old[k] + vals[k]

    loop(ids_ref.shape[0] // unroll, body)


def gather_pass(ids_ref, table, out, width, unroll=16):
    def body(j):
        for u in range(unroll):
            i = j * unroll + u
            out[pl.ds(pl.multiple_of(i * width, width), width), :] = table[pl.ds(pl.multiple_of(ids_ref[i] * width, width), width), :]

    loop(ids_ref.shape[0] // unroll, body)


def spread(table, start, block):
    tiles = block.shape[1] // LANES
    for c in range(tiles):
        table[pl.ds(start * tiles + c, block.shape[0], tiles), :] = block[:, c * LANES:(c + 1) * LANES]


def unspread(table, start, rows, tiles):
    return jnp.concatenate([table[pl.ds(start * tiles + c, rows, tiles), :] for c in range(tiles)], axis=1)


def enter(me, num_dev):
    barrier = pltpu.get_barrier_semaphore()
    for step in range(1, num_dev):
        pl.semaphore_signal(barrier, inc=1, device_id=(lax.rem(me + step, num_dev),), device_id_type=MESH)
    pl.semaphore_wait(barrier, num_dev - 1)


def push(src, dst, send_sem, recv_sem, dev):
    copy = pltpu.make_async_remote_copy(src_ref=src, dst_ref=dst, send_sem=send_sem, recv_sem=recv_sem, device_id=(dev,), device_id_type=MESH)
    copy.start()
    return copy


def lists_kernel(num_dev, mask, code, wgt, x, w1, count, code_prev, code_next, w_prev, w_next, table, part, slots, send_sem, recv_sem, lsend, lrecv):
    ones = jnp.sum(jnp.sum(mask[...].astype(F32), axis=1, keepdims=True), axis=0, keepdims=True)
    part[...] = jnp.broadcast_to(ones, part.shape)
    me = lax.axis_index(GRAPH_AXIS)
    succ, pred = lax.rem(me + 1, num_dev), lax.rem(me + num_dev - 1, num_dev)
    enter(me, num_dev)
    copies = []
    for step in range(1, num_dev):
        copies.append(push(part, slots.at[step - 1], send_sem.at[step - 1], recv_sem.at[step - 1], lax.rem(me + step, num_dev)))
    copies.append(push(code, code_prev, lsend.at[0], lrecv.at[0], succ))
    copies.append(push(code, code_next, lsend.at[1], lrecv.at[1], pred))
    copies.append(push(wgt, w_prev, lsend.at[2], lrecv.at[2], succ))
    copies.append(push(wgt, w_next, lsend.at[3], lrecv.at[3], pred))

    def put(i):
        t = jnp.dot(x[rows_at(i), :], w1[...], preferred_element_type=F32)
        spread(table, i * BLOCK, t.astype(BF16).astype(F32))

    loop(x.shape[0] // BLOCK, put)
    for copy in copies:
        copy.wait()
    total = part[...]
    for step in range(num_dev - 1):
        total = total + slots[step]
    count[...] = jnp.maximum(total, 1.0)


def halo_rows_kernel(ids, x, to_next, to_prev, table, picked):
    rows = x.shape[0]

    def put(i):
        block = x[rows_at(i), :].astype(F32)
        pad = jnp.zeros((BLOCK, 2 * LANES - block.shape[1]), F32)
        spread(table, i * BLOCK, jnp.concatenate([block, pad], axis=1))

    loop(rows // BLOCK, put)
    gather_pass(ids, table, picked, 2)
    half = to_next.shape[0]

    def take(i):
        to_prev[rows_at(i), :] = unspread(picked, i * BLOCK, BLOCK, 2).astype(BF16)
        to_next[rows_at(i), :] = unspread(picked, half + i * BLOCK, BLOCK, 2).astype(BF16)

    loop(half // BLOCK, take)


def one_halo_kernel(s4, d4, w, cnt, ids, y_own, x_prev, x_next, w1, w2t, hid_a, hid_b, t2, to_next, to_prev, table, picked, *accs):
    zero_rows(accs)
    half = x_prev.shape[0]

    def put(i):
        t = jnp.dot(x_prev[rows_at(i), :w1.shape[0]], w1[...], preferred_element_type=F32)
        spread(table, i * BLOCK, t.astype(BF16).astype(F32))
        t = jnp.dot(x_next[rows_at(i), :w1.shape[0]], w1[...], preferred_element_type=F32)
        spread(table, half + i * BLOCK, t.astype(BF16).astype(F32))

    loop(half // BLOCK, put)
    edge_pass(s4, d4, w, cnt, table, accs, 4, 16, True)
    sum_rows(accs[0], (y_own,) + accs)

    def act(i):
        h = jnp.maximum(unspread(accs[0], i * BLOCK, BLOCK, 4), 0.0).astype(BF16)
        cut = hid_a.shape[1]
        hid_a[rows_at(i), :] = h[:, :cut]
        hid_b[rows_at(i), :] = h[:, cut:]
        t = lax.dot_general(h, w2t[...], CONTRACT_COLS, preferred_element_type=F32)
        t2[rows_at(i), :] = t.astype(BF16).astype(F32)

    loop(t2.shape[0] // BLOCK, act)
    gather_pass(ids, t2, picked, 1)

    def take(i):
        to_prev[rows_at(i), :] = picked[rows_at(i), :].astype(BF16)
        to_next[rows_at(i), :] = picked[rows_at(i, half), :].astype(BF16)

    loop(half // BLOCK, take)


def narrow_own_kernel(frm, to, cnt, table, w, out, *accs):
    zero_rows(accs)
    edge_pass(frm, to, w, cnt, table, accs, 1, 32, False)
    sum_rows(out, accs)


def wide_own_kernel(frm, to, cnt, table, w, out, *accs):
    zero_rows(accs)
    edge_pass(frm, to, w, cnt, table, accs, 4, 32, False)
    sum_rows(out, accs)


def logits_kernel(classes, s, d, w, cnt, z_own, t_prev, t_next, labels, count, dz, back_prev, back_next, loss, table, *accs):
    zero_rows(accs)
    half = t_prev.shape[0]

    def put(i):
        table[rows_at(i), :] = t_prev[rows_at(i), :].astype(F32)
        table[rows_at(i, half), :] = t_next[rows_at(i), :].astype(F32)

    loop(half // BLOCK, put)
    edge_pass(s, d, w, cnt, table, accs, 1, 16, True)
    denom = count[0:1, :]
    loss[...] = jnp.zeros_like(loss)

    def soft(i):
        at = pl.ds(i * 64, 64)
        z = z_own[at, :]
        for acc in accs:
            z = z + acc[at, :]
        lane = lax.broadcasted_iota(jnp.int32, z.shape, 1)
        lab = labels[at, :]
        hot = lab == lane
        keep = lab >= 0
        zm = jnp.where(lane < classes, z, -jnp.inf)
        top = jnp.max(zm, axis=1, keepdims=True)
        ex = jnp.exp(zm - top)
        log_norm = jnp.log(jnp.sum(ex, axis=1, keepdims=True)) + top
        hot_f = jnp.where(hot, 1.0, 0.0)
        term = jnp.where(hot, log_norm - z, 0.0)
        part = term[0:8]
        for b in range(1, 8):
            part = part + term[b * 8:b * 8 + 8]
        loss[...] += part
        mask_f = jnp.where(keep, 1.0, 0.0)
        dz[at, :] = jnp.where(lane < classes, (jnp.exp(zm - log_norm) - hot_f) * (mask_f / denom), 0.0)

    loop(dz.shape[0] // 64, soft)
    zero_rows(accs)
    edge_pass(d, s, w, cnt, dz, accs, 1, 16, True)

    def fin(i):
        at = pl.ds(i * 64, 64)
        bt = pl.ds(half + i * 64, 64)
        a, b = accs[0][at, :], accs[0][bt, :]
        for acc in accs[1:]:
            a, b = a + acc[at, :], b + acc[bt, :]
        back_prev[at, :] = a
        back_next[at, :] = b

    loop(half // 64, fin)


def masked(grad, hid_a, hid_b):
    cut = hid_a.shape[1]
    lo = jnp.where(hid_a.astype(F32) > 0.0, grad[:, :cut], 0.0)
    hi = jnp.where(hid_b.astype(F32) > 0.0, grad[:, cut:], 0.0)
    return jnp.concatenate([lo, hi], axis=1)


def hidden_grad_kernel(ids, own, ret_next, ret_prev, hid_a, hid_b, w2t, dt2, dy, g2, *accs):
    n_loc, half = own.shape[0], ret_next.shape[0]
    zero_rows(accs)
    scatter_pass(ids.at[pl.ds(half, half)], ret_next, accs, 1, 8)
    scatter_pass(ids.at[pl.ds(0, half)], ret_prev, accs, 1, 8)
    g2[...] = jnp.zeros_like(g2)

    def fold(i):
        at = rows_at(i)
        total = own[at, :]
        for acc in accs:
            total = total + acc[at, :]
        dt = total.astype(BF16)
        dt2[at, :] = dt
        cut = hid_a.shape[1]
        g2[:cut, :] += lax.dot_general(hid_a[at, :], dt, CONTRACT_ROWS, preferred_element_type=F32)
        g2[cut:, :] += lax.dot_general(hid_b[at, :], dt, CONTRACT_ROWS, preferred_element_type=F32)
        dh = jnp.dot(dt, w2t[...], preferred_element_type=F32)
        spread(dy, i * BLOCK, masked(dh, hid_a[at, :], hid_b[at, :]))

    loop(n_loc // BLOCK, fold)


def peer_pass(ids, code_ref, w_ref, rows, far, table, accs):
    n_acc = len(accs)
    tally = rows * SLOT
    n_loc = ids.shape[0]
    shift = n_loc.bit_length() - 1
    half = n_loc // 2
    owners = ids.at[pl.ds(0 if far else half, half)]

    def row(r):
        first = SLOT - 16 - (code_ref[tally + 2 * rows + r] if far else 0)
        edges = code_ref[tally + far * rows + r]

        def body(j):
            off = r * SLOT + first - j * 16
            codes, wgt = (ref.at[pl.ds(off, 16)] for ref in (code_ref, w_ref))
            for u in range(16):
                acc = accs[u % n_acc]
                code = codes[u]
                frm = lax.shift_right_logical(code, shift) * 4
                val = table[pl.ds(pl.multiple_of(frm, 4), 4), :] * wgt[u]
                at = pl.ds(pl.multiple_of(owners[code & (half - 1)] * 4, 4), 4)
                acc[at, :] = acc[at, :] + val

        loop(lax.shift_right_logical(edges + 15, 4), body)

    loop(rows, row)


def table_grad_kernel(rows, ids, cn, wn, cp, wp, own, tn, han, hbn, tp, hap, hbp, w2t, x, g1, table, *accs):
    zero_rows(accs)
    g1[...] = jnp.zeros_like(g1)

    def fill(dt, hid_a, hid_b):
        def put(i):
            at = rows_at(i)
            dh = jnp.dot(dt[at, :], w2t[...], preferred_element_type=F32)
            spread(table, i * BLOCK, masked(dh, hid_a[at, :], hid_b[at, :]))

        loop(dt.shape[0] // BLOCK, put)

    fill(tn, han, hbn)
    peer_pass(ids, cn, wn, rows, 0, table, accs)
    fill(tp, hap, hbp)
    peer_pass(ids, cp, wp, rows, 1, table, accs)

    def fold(i):
        total = unspread(own, i * BLOCK, BLOCK, 4)
        for acc in accs:
            total = total + unspread(acc, i * BLOCK, BLOCK, 4)
        g1[...] += lax.dot_general(x[rows_at(i), :], total.astype(BF16), CONTRACT_ROWS, preferred_element_type=F32)

    loop(x.shape[0] // BLOCK, fold)


def reduce_kernel(num_dev, g1, g2, loss, count, o1, o2, lo, pack, total, other_half, sums, parts, lslots, sem_s, sem_r, lsem_s, lsem_r):
    rows, tiles = g1.shape[0], g1.shape[1] // LANES
    base = rows * tiles
    for c in range(tiles):
        pack[c * rows:(c + 1) * rows, :] = g1[:, c * LANES:(c + 1) * LANES]
    end = base + g2.shape[0]
    pack[base:end, :] = g2[...]
    pack[end:, :] = jnp.zeros((pack.shape[0] - end, LANES), F32)
    me = lax.axis_index(GRAPH_AXIS)
    core = lax.rem(me, 2)
    chip = me // 2
    mate = me + 1 - 2 * core
    half = pack.shape[0] // 2
    part = half // 4
    enter(me, num_dev)

    def piece(owner):
        return pl.ds(pl.multiple_of(core * half + owner * part, 8), part)

    pair = push(pack.at[pl.ds(pl.multiple_of((1 - core) * half, 8), half)], other_half, sem_s.at[0], sem_r.at[0], mate)
    scalar = []
    for step in range(1, num_dev):
        scalar.append(push(loss, lslots.at[step - 1], lsem_s.at[step - 1], lsem_r.at[step - 1], lax.rem(me + step, num_dev)))
    pair.wait()
    sums[...] = pack[pl.ds(pl.multiple_of(core * half, 8), half), :] + other_half[...]
    spreads = []
    for step in range(1, 4):
        far = lax.rem(chip + step, 4)
        at = pl.ds(pl.multiple_of(far * part, 8), part)
        spreads.append(push(sums.at[at], parts.at[step - 1], sem_s.at[step], sem_r.at[step], far * 2 + core))
    for copy in spreads:
        copy.wait()
    mine = sums[pl.ds(pl.multiple_of(chip * part, 8), part), :]
    for step in range(3):
        mine = mine + parts[step]
    total[piece(chip), :] = mine
    gathers = []
    for step in range(1, 4):
        dev = lax.rem(chip + step, 4) * 2 + core
        gathers.append(push(total.at[piece(chip)], total.at[piece(chip)], sem_s.at[3 + step], sem_r.at[3 + step], dev))
    tails = [push(total.at[piece(chip)], total.at[piece(chip)], sem_s.at[7], sem_r.at[7], mate)]
    for step in range(1, 4):
        near = lax.rem(chip + 4 - step, 4)
        gathers[step - 1].wait()
        tails.append(push(total.at[piece(near)], total.at[piece(near)], sem_s.at[7 + step], sem_r.at[7 + step], mate))
    for copy in scalar:
        copy.wait()
    lsum = loss[...]
    for step in range(num_dev - 1):
        lsum = lsum + lslots[step]
    lsum = jnp.sum(jnp.sum(lsum, axis=1, keepdims=True), axis=0, keepdims=True)
    lo[...] = lsum / count[...]
    for copy in tails:
        copy.wait()
    for c in range(tiles):
        o1[:, c * LANES:(c + 1) * LANES] = total[c * rows:(c + 1) * rows, :]
    o2[...] = total[base:end, :]


def solution(mesh):
    num_dev = mesh.shape[GRAPH_AXIS]
    to_next = [(dev_id, (dev_id + 1) % num_dev) for dev_id in range(num_dev)]
    to_prev = [(dev_id, (dev_id - 1) % num_dev) for dev_id in range(num_dev)]

    def shift_next(a):
        return lax.ppermute(a, GRAPH_AXIS, to_next)

    def shift_prev(a):
        return lax.ppermute(a, GRAPH_AXIS, to_prev)

    def compact(edge_src, edge_dst, edge_w, n_loc, halo):
        rows = edge_src.shape[0] // CHUNK
        src, dst, w = (a.reshape(rows, CHUNK) for a in (edge_src, edge_dst, edge_w))
        live = w != 0.0
        own = live & (src < n_loc)
        far = live & (src >= n_loc + halo)
        near = live & (src >= n_loc) & (src < n_loc + halo)
        tri = (jnp.arange(CHUNK)[:, None] < jnp.arange(CHUNK)[None, :]).astype(BF16)
        sets = jnp.concatenate([own, near, far], axis=0).astype(BF16)
        rank = jnp.dot(sets, tri, preferred_element_type=F32).astype(jnp.int32)
        counts = jnp.sum(sets.astype(F32), axis=1).astype(jnp.int32)
        n_own, n_near, n_far = counts[:rows], counts[rows:2 * rows], counts[2 * rows:]
        skip = (n_near + 15) // 16 * 16
        place = jnp.where(far, SLOT - 1 - skip[:, None] - rank[2 * rows:], SLOT)
        place = jnp.where(near, SLOT - 1 - rank[rows:2 * rows], place)
        place = jnp.where(own, rank[:rows], place)
        hit = place[:, :, None] == jnp.arange(SLOT)[None, None, :]
        code = jnp.where(src < n_loc, src, src - n_loc) + dst * n_loc
        picks = (jnp.where(hit, code[:, :, None], 0), jnp.where(hit, w[:, :, None], 0.0))
        code, wc = lax.reduce(picks, (jnp.int32(0), jnp.float32(0.0)), lambda a, b: (a[0] + b[0], a[1] + b[1]), (1,))
        n_hal = jnp.where(n_far > 0, skip + n_far, n_near)
        return code, wc, n_own, n_hal, n_near, n_far, skip

    def device_step(node_feats, w_one, w_two, send_rows, edge_src, edge_dst, edge_w, labels, label_mask):
        n_loc, f_in = node_feats.shape
        halo = send_rows.shape[1]
        f_hid, classes = w_two.shape
        quad = 4 * n_loc
        sds = jax.ShapeDtypeStruct
        x = node_feats
        w1 = w_one.astype(BF16)
        w2t = jnp.pad(w_two.T.astype(BF16), ((0, LANES - classes), (0, 0)))
        ids = send_rows.reshape(-1)
        code, wc, n_own, n_hal, n_near, n_far, skip = compact(edge_src, edge_dst, edge_w, n_loc, halo)
        rows = n_own.shape[0]
        slots = code.size // LANES
        w_own = jnp.broadcast_to(wc[:, :CHUNK].reshape(-1, 1), (rows * CHUNK, LANES))
        code, wc = code.reshape(-1), wc.reshape(-1)
        tally = jnp.concatenate([n_near, n_far, skip, jnp.zeros((8 * LANES - 3 * rows,), jnp.int32)])
        lists = jnp.concatenate([code, tally]).reshape(slots + 8, LANES)
        count, code_prev, code_next, w_prev, w_next, t1 = pl.pallas_call(
            functools.partial(lists_kernel, num_dev),
            out_shape=[sds((8, LANES), F32)] + [sds((slots + 8, LANES), jnp.int32)] * 2 + [sds((slots, LANES), F32)] * 2 + [sds((quad, LANES), F32)],
            in_specs=[VMEM_SPEC] * 5,
            out_specs=[VMEM_SPEC] * 6,
            scratch_shapes=[pltpu.VMEM((8, LANES), F32), pltpu.VMEM((num_dev - 1, 8, LANES), F32)] + [pltpu.SemaphoreType.DMA((n,)) for n in (num_dev - 1, num_dev - 1, 4, 4)],
            compiler_params=params(8, collective_id=0, has_side_effects=True),
            name="lists",
        )(label_mask.reshape(-1, LANES), lists, wc.reshape(slots, LANES), x, w1)
        s, d = code % n_loc, code // n_loc
        s4, d4 = s * 4, d * 4
        count, x = lax.optimization_barrier((count, x))
        x_next, x_prev = pl.pallas_call(
            halo_rows_kernel,
            out_shape=[sds((halo, 256), BF16)] * 2,
            in_specs=[SMEM_SPEC, VMEM_SPEC],
            out_specs=[VMEM_SPEC] * 2,
            scratch_shapes=[pltpu.VMEM((2 * n_loc, LANES), F32), pltpu.VMEM((4 * halo, LANES), F32)],
            compiler_params=params(12),
            name="halo_rows",
        )(ids, x)
        xh_prev = shift_next(x_next)
        xh_next = shift_prev(x_prev)
        wide4 = [pltpu.VMEM((quad, LANES), F32)] * 4
        thin4 = [pltpu.VMEM((n_loc, LANES), F32)] * 4
        marks = jnp.where(label_mask == 1, labels, -1)
        s4, w2t, marks, ids, w_own, wc = lax.optimization_barrier((s4, w2t, marks, ids, w_own, wc))
        wide_own = functools.partial(
            pl.pallas_call,
            wide_own_kernel,
            out_shape=sds((quad, LANES), F32),
            in_specs=[SMEM_SPEC] * 3 + [VMEM_SPEC] * 2,
            out_specs=VMEM_SPEC,
            scratch_shapes=wide4,
            compiler_params=params(28),
            cost_estimate=pl.CostEstimate(flops=200000000000, bytes_accessed=8000000, transcendentals=0),
        )
        y_own = wide_own(name="one_own")(s4, d4, n_own, t1, w_own)
        hid_a, hid_b, t2, t_next, t_prev = pl.pallas_call(
            one_halo_kernel,
            out_shape=[sds((n_loc, f_hid // 2), BF16)] * 2 + [sds((n_loc, LANES), F32), sds((halo, LANES), BF16), sds((halo, LANES), BF16)],
            in_specs=[SMEM_SPEC] * 5 + [VMEM_SPEC] * 5,
            out_specs=[VMEM_SPEC] * 5,
            scratch_shapes=[pltpu.VMEM((4 * 2 * halo, LANES), F32), pltpu.VMEM((2 * halo, LANES), F32)] + wide4,
            compiler_params=params(32),
            name="one_halo",
        )(s4, d4, wc, n_hal, ids, y_own, xh_prev, xh_next, w1, w2t)
        th_prev = shift_next(t_next)
        th_next = shift_prev(t_prev)
        ha_prev, ha_next = shift_next(hid_a), shift_prev(hid_a)
        narrow_own = functools.partial(
            pl.pallas_call,
            narrow_own_kernel,
            out_shape=sds((n_loc, LANES), F32),
            in_specs=[SMEM_SPEC] * 3 + [VMEM_SPEC] * 2,
            out_specs=VMEM_SPEC,
            scratch_shapes=thin4,
            compiler_params=params(14),
            cost_estimate=pl.CostEstimate(flops=200000000000, bytes_accessed=8000000, transcendentals=0),
        )
        z_own = narrow_own(name="two_own")(s, d, n_own, t2, w_own)
        marks = jnp.broadcast_to(marks[:, None], (n_loc, LANES))
        dz, bz_prev, bz_next, loss = pl.pallas_call(
            functools.partial(logits_kernel, classes),
            out_shape=[sds((n_loc, LANES), F32), sds((halo, LANES), F32), sds((halo, LANES), F32), sds((8, LANES), F32)],
            in_specs=[SMEM_SPEC] * 4 + [VMEM_SPEC] * 5,
            out_specs=[VMEM_SPEC] * 4,
            scratch_shapes=[pltpu.VMEM((2 * halo, LANES), F32)] + thin4,
            compiler_params=params(12),
            name="logits",
        )(s, d, wc, n_hal, z_own, th_prev, th_next, marks, count)
        rz_next = shift_prev(bz_prev)
        rz_prev = shift_next(bz_next)
        late_b, _ = lax.optimization_barrier((hid_b, bz_prev))
        hb_prev, hb_next = shift_next(late_b), shift_prev(late_b)
        dt2_own = narrow_own(name="two_back_own")(d, s, n_own, dz, w_own)
        dt2, dy, grad_two = pl.pallas_call(
            hidden_grad_kernel,
            out_shape=[sds((n_loc, LANES), BF16), sds((quad, LANES), F32), sds((f_hid, LANES), F32)],
            in_specs=[SMEM_SPEC] + [VMEM_SPEC] * 6,
            out_specs=[VMEM_SPEC] * 3,
            scratch_shapes=thin4,
            compiler_params=params(16),
            name="hidden_grad",
        )(ids, dt2_own, rz_next, rz_prev, hid_a, hid_b, w2t)
        dt_prev, dt_next = shift_next(dt2), shift_prev(dt2)
        dt1_own = wide_own(name="one_back_own")(d4, s4, n_own, dy, w_own)
        grad_one = pl.pallas_call(
            functools.partial(table_grad_kernel, rows),
            out_shape=sds((f_in, f_hid), F32),
            in_specs=[SMEM_SPEC] * 5 + [VMEM_SPEC] * 9,
            out_specs=VMEM_SPEC,
            scratch_shapes=[pltpu.VMEM((quad, LANES), F32)] + wide4,
            compiler_params=params(36),
            name="table_grad",
        )(ids, code_next.reshape(-1), w_next.reshape(-1), code_prev.reshape(-1), w_prev.reshape(-1), dt1_own, dt_next, ha_next, hb_next, dt_prev, ha_prev, hb_prev, w2t, x)
        pack_rows = f_in * f_hid // LANES + f_hid
        pack_rows += -pack_rows % 64
        grad_one, grad_two, loss = pl.pallas_call(
            functools.partial(reduce_kernel, num_dev),
            out_shape=[sds((f_in, f_hid), F32), sds((f_hid, LANES), F32), sds((8, LANES), F32)],
            in_specs=[VMEM_SPEC] * 4,
            out_specs=[VMEM_SPEC] * 3,
            scratch_shapes=[
                pltpu.VMEM((pack_rows, LANES), F32), pltpu.VMEM((pack_rows, LANES), F32),
                pltpu.VMEM((pack_rows // 2, LANES), F32), pltpu.VMEM((pack_rows // 2, LANES), F32),
                pltpu.VMEM((3, pack_rows // 8, LANES), F32), pltpu.VMEM((num_dev - 1, 8, LANES), F32),
            ] + [pltpu.SemaphoreType.DMA((n,)) for n in (11, 11, num_dev - 1, num_dev - 1)],
            compiler_params=params(8, collective_id=1, has_side_effects=True),
            name="reduce",
        )(grad_one, grad_two, loss, count)
        return loss[0, 0], grad_one, grad_two[:, :classes]

    row_spec = P(GRAPH_AXIS)
    return jax.shard_map(device_step, mesh=mesh, in_specs=(row_spec, P(), P(), row_spec, row_spec, row_spec, row_spec, row_spec, row_spec), out_specs=(P(), P(), P()), check_vma=False)
```

```python
import functools

import jax
import jax.numpy as jnp
from jax import lax
from jax.experimental import pallas as pl
from jax.experimental.pallas import tpu as pltpu
from jax.sharding import PartitionSpec as P


GRAPH_AXIS = "graph"
CONTRACT_ROWS = (((0,), (0,)), ((), ()))
CONTRACT_COLS = (((1,), (1,)), ((), ()))
MESH = pl.DeviceIdType.MESH
F32 = jnp.float32
BF16 = jnp.bfloat16
LANES = 128
BLOCK = 256
CHUNK = 256
SLOT = 384

SMEM_SPEC = pl.BlockSpec(memory_space=pltpu.SMEM)
VMEM_SPEC = pl.BlockSpec(memory_space=pltpu.VMEM)


def rows_at(i, base=0, size=BLOCK):
    return pl.ds(base + i * size, size)


def loop(count, body):
    lax.fori_loop(0, count, lambda i, _: (body(i), 0)[1], 0)


def params(mib, **kw):
    return pltpu.CompilerParams(vmem_limit_bytes=mib * 2**20, **kw)


def zero_rows(refs):
    rows = refs[0].shape[0]

    def body(i):
        for ref in refs:
            ref[pl.ds(i * 64, 64), :] = jnp.zeros((64, LANES), F32)

    loop(rows // 64, body)


def sum_rows(out, refs):
    rows = refs[0].shape[0]

    def body(i):
        total = refs[0][pl.ds(i * 64, 64), :]
        for ref in refs[1:]:
            total = total + ref[pl.ds(i * 64, 64), :]
        out[pl.ds(i * 64, 64), :] = total

    loop(rows // 64, body)


def edge_pass(from_ref, to_ref, w_ref, cnt_ref, table, accs, width, unroll, back):
    n_acc = len(accs)
    shift = unroll.bit_length() - 1

    def row(r):
        blocks = lax.shift_right_logical(cnt_ref[r] + (unroll - 1), shift)

        def body(j):
            off = r * SLOT + (SLOT - unroll - j * unroll if back else j * unroll)
            frm, to = (ref.at[pl.ds(off, unroll)] for ref in (from_ref, to_ref))
            if back:
                wgt = w_ref.at[pl.ds(off, unroll)]
            else:
                wgt = [jnp.broadcast_to(w_ref[pl.ds(r * CHUNK + j * unroll + u, 1), :], (width, LANES)) for u in range(unroll)]
            for u in range(unroll):
                acc = accs[u % n_acc]
                val = table[pl.ds(pl.multiple_of(frm[u], width), width), :] * wgt[u]
                at = pl.ds(pl.multiple_of(to[u], width), width)
                acc[at, :] = acc[at, :] + val

        loop(blocks, body)

    loop(cnt_ref.shape[0], row)


def scatter_pass(ids_ref, table, accs, width, unroll):
    n_acc = len(accs)

    def body(j):
        off = j * unroll
        for g in range(unroll // n_acc):
            rows = [pl.multiple_of(ids_ref[off + g * n_acc + k], width) for k in range(n_acc)]
            vals = [table[pl.ds(pl.multiple_of((off + g * n_acc + k) * width, width), width), :] for k in range(n_acc)]
            old = [accs[k][pl.ds(rows[k], width), :] for k in range(n_acc)]
            for k in range(n_acc):
                accs[k][pl.ds(rows[k], width), :] = old[k] + vals[k]

    loop(ids_ref.shape[0] // unroll, body)


def gather_pass(ids_ref, table, out, width, unroll=16):
    def body(j):
        for u in range(unroll):
            i = j * unroll + u
            out[pl.ds(pl.multiple_of(i * width, width), width), :] = table[pl.ds(pl.multiple_of(ids_ref[i] * width, width), width), :]

    loop(ids_ref.shape[0] // unroll, body)


def spread(table, start, block):
    tiles = block.shape[1] // LANES
    for c in range(tiles):
        table[pl.ds(start * tiles + c, block.shape[0], tiles), :] = block[:, c * LANES:(c + 1) * LANES]


def unspread(table, start, rows, tiles):
    return jnp.concatenate([table[pl.ds(start * tiles + c, rows, tiles), :] for c in range(tiles)], axis=1)


def enter(me, num_dev):
    barrier = pltpu.get_barrier_semaphore()
    for step in range(1, num_dev):
        pl.semaphore_signal(barrier, inc=1, device_id=(lax.rem(me + step, num_dev),), device_id_type=MESH)
    pl.semaphore_wait(barrier, num_dev - 1)


def push(src, dst, send_sem, recv_sem, dev):
    copy = pltpu.make_async_remote_copy(src_ref=src, dst_ref=dst, send_sem=send_sem, recv_sem=recv_sem, device_id=(dev,), device_id_type=MESH)
    copy.start()
    return copy


def lists_kernel(num_dev, mask, code, wgt, count, code_prev, code_next, w_prev, w_next, part, slots, send_sem, recv_sem, lsend, lrecv):
    ones = jnp.sum(jnp.sum(mask[...].astype(F32), axis=1, keepdims=True), axis=0, keepdims=True)
    part[...] = jnp.broadcast_to(ones, part.shape)
    me = lax.axis_index(GRAPH_AXIS)
    succ, pred = lax.rem(me + 1, num_dev), lax.rem(me + num_dev - 1, num_dev)
    enter(me, num_dev)
    copies = []
    for step in range(1, num_dev):
        copies.append(push(part, slots.at[step - 1], send_sem.at[step - 1], recv_sem.at[step - 1], lax.rem(me + step, num_dev)))
    copies.append(push(code, code_prev, lsend.at[0], lrecv.at[0], succ))
    copies.append(push(code, code_next, lsend.at[1], lrecv.at[1], pred))
    copies.append(push(wgt, w_prev, lsend.at[2], lrecv.at[2], succ))
    copies.append(push(wgt, w_next, lsend.at[3], lrecv.at[3], pred))
    for copy in copies:
        copy.wait()
    total = part[...]
    for step in range(num_dev - 1):
        total = total + slots[step]
    count[...] = jnp.maximum(total, 1.0)


def halo_rows_kernel(ids, x, to_next, to_prev, table, picked):
    rows = x.shape[0]

    def put(i):
        block = x[rows_at(i), :].astype(F32)
        pad = jnp.zeros((BLOCK, 2 * LANES - block.shape[1]), F32)
        spread(table, i * BLOCK, jnp.concatenate([block, pad], axis=1))

    loop(rows // BLOCK, put)
    gather_pass(ids, table, picked, 2)
    half = to_next.shape[0]

    def take(i):
        to_prev[rows_at(i), :] = unspread(picked, i * BLOCK, BLOCK, 2).astype(BF16)
        to_next[rows_at(i), :] = unspread(picked, half + i * BLOCK, BLOCK, 2).astype(BF16)

    loop(half // BLOCK, take)


def one_own_kernel(s4, d4, cnt, x, w1, w, y, table, *accs):
    zero_rows(accs)

    def put(i):
        t = jnp.dot(x[rows_at(i), :], w1[...], preferred_element_type=F32)
        spread(table, i * BLOCK, t.astype(BF16).astype(F32))

    loop(x.shape[0] // BLOCK, put)
    edge_pass(s4, d4, w, cnt, table, accs, 4, 32, False)
    sum_rows(y, accs)


def one_halo_kernel(s4, d4, w, cnt, ids, y_own, x_prev, x_next, w1, w2t, hid_a, hid_b, t2, to_next, to_prev, table, picked, *accs):
    zero_rows(accs)
    half = x_prev.shape[0]

    def put(i):
        t = jnp.dot(x_prev[rows_at(i), :w1.shape[0]], w1[...], preferred_element_type=F32)
        spread(table, i * BLOCK, t.astype(BF16).astype(F32))
        t = jnp.dot(x_next[rows_at(i), :w1.shape[0]], w1[...], preferred_element_type=F32)
        spread(table, half + i * BLOCK, t.astype(BF16).astype(F32))

    loop(half // BLOCK, put)
    edge_pass(s4, d4, w, cnt, table, accs, 4, 16, True)
    sum_rows(accs[0], (y_own,) + accs)

    def act(i):
        h = jnp.maximum(unspread(accs[0], i * BLOCK, BLOCK, 4), 0.0).astype(BF16)
        cut = hid_a.shape[1]
        hid_a[rows_at(i), :] = h[:, :cut]
        hid_b[rows_at(i), :] = h[:, cut:]
        t = lax.dot_general(h, w2t[...], CONTRACT_COLS, preferred_element_type=F32)
        t2[rows_at(i), :] = t.astype(BF16).astype(F32)

    loop(t2.shape[0] // BLOCK, act)
    gather_pass(ids, t2, picked, 1)

    def take(i):
        to_prev[rows_at(i), :] = picked[rows_at(i), :].astype(BF16)
        to_next[rows_at(i), :] = picked[rows_at(i, half), :].astype(BF16)

    loop(half // BLOCK, take)


def narrow_own_kernel(frm, to, cnt, table, w, out, *accs):
    zero_rows(accs)
    edge_pass(frm, to, w, cnt, table, accs, 1, 32, False)
    sum_rows(out, accs)


def wide_own_kernel(frm, to, cnt, table, w, out, *accs):
    zero_rows(accs)
    edge_pass(frm, to, w, cnt, table, accs, 4, 32, False)
    sum_rows(out, accs)


def logits_kernel(classes, s, d, w, cnt, z_own, t_prev, t_next, labels, count, dz, back_prev, back_next, loss, table, *accs):
    zero_rows(accs)
    half = t_prev.shape[0]

    def put(i):
        table[rows_at(i), :] = t_prev[rows_at(i), :].astype(F32)
        table[rows_at(i, half), :] = t_next[rows_at(i), :].astype(F32)

    loop(half // BLOCK, put)
    edge_pass(s, d, w, cnt, table, accs, 1, 16, True)
    denom = count[0:1, :]
    loss[...] = jnp.zeros_like(loss)

    def soft(i):
        at = pl.ds(i * 64, 64)
        z = z_own[at, :]
        for acc in accs:
            z = z + acc[at, :]
        lane = lax.broadcasted_iota(jnp.int32, z.shape, 1)
        lab = labels[at, :]
        hot = lab == lane
        keep = lab >= 0
        zm = jnp.where(lane < classes, z, -jnp.inf)
        top = jnp.max(zm, axis=1, keepdims=True)
        ex = jnp.exp(zm - top)
        log_norm = jnp.log(jnp.sum(ex, axis=1, keepdims=True)) + top
        hot_f = jnp.where(hot, 1.0, 0.0)
        term = jnp.where(hot, log_norm - z, 0.0)
        part = term[0:8]
        for b in range(1, 8):
            part = part + term[b * 8:b * 8 + 8]
        loss[...] += part
        mask_f = jnp.where(keep, 1.0, 0.0)
        dz[at, :] = jnp.where(lane < classes, (jnp.exp(zm - log_norm) - hot_f) * (mask_f / denom), 0.0)

    loop(dz.shape[0] // 64, soft)
    zero_rows(accs)
    edge_pass(d, s, w, cnt, dz, accs, 1, 16, True)

    def fin(i):
        at = pl.ds(i * 64, 64)
        bt = pl.ds(half + i * 64, 64)
        a, b = accs[0][at, :], accs[0][bt, :]
        for acc in accs[1:]:
            a, b = a + acc[at, :], b + acc[bt, :]
        back_prev[at, :] = a
        back_next[at, :] = b

    loop(half // 64, fin)


def masked(grad, hid_a, hid_b):
    cut = hid_a.shape[1]
    lo = jnp.where(hid_a.astype(F32) > 0.0, grad[:, :cut], 0.0)
    hi = jnp.where(hid_b.astype(F32) > 0.0, grad[:, cut:], 0.0)
    return jnp.concatenate([lo, hi], axis=1)


def hidden_grad_kernel(ids, own, ret_next, ret_prev, hid_a, hid_b, w2t, dt2, dy, g2, *accs):
    n_loc, half = own.shape[0], ret_next.shape[0]
    zero_rows(accs)
    scatter_pass(ids.at[pl.ds(half, half)], ret_next, accs, 1, 8)
    scatter_pass(ids.at[pl.ds(0, half)], ret_prev, accs, 1, 8)
    g2[...] = jnp.zeros_like(g2)

    def fold(i):
        at = rows_at(i)
        total = own[at, :]
        for acc in accs:
            total = total + acc[at, :]
        dt = total.astype(BF16)
        dt2[at, :] = dt
        cut = hid_a.shape[1]
        g2[:cut, :] += lax.dot_general(hid_a[at, :], dt, CONTRACT_ROWS, preferred_element_type=F32)
        g2[cut:, :] += lax.dot_general(hid_b[at, :], dt, CONTRACT_ROWS, preferred_element_type=F32)
        dh = jnp.dot(dt, w2t[...], preferred_element_type=F32)
        spread(dy, i * BLOCK, masked(dh, hid_a[at, :], hid_b[at, :]))

    loop(n_loc // BLOCK, fold)


def peer_pass(ids, code_ref, w_ref, rows, far, table, accs):
    n_acc = len(accs)
    tally = rows * SLOT
    n_loc = ids.shape[0]
    shift = n_loc.bit_length() - 1
    half = n_loc // 2
    owners = ids.at[pl.ds(0 if far else half, half)]

    def row(r):
        first = SLOT - 16 - (code_ref[tally + 2 * rows + r] if far else 0)
        edges = code_ref[tally + far * rows + r]

        def body(j):
            off = r * SLOT + first - j * 16
            codes, wgt = (ref.at[pl.ds(off, 16)] for ref in (code_ref, w_ref))
            for u in range(16):
                acc = accs[u % n_acc]
                code = codes[u]
                frm = lax.shift_right_logical(code, shift) * 4
                val = table[pl.ds(pl.multiple_of(frm, 4), 4), :] * wgt[u]
                at = pl.ds(pl.multiple_of(owners[code & (half - 1)] * 4, 4), 4)
                acc[at, :] = acc[at, :] + val

        loop(lax.shift_right_logical(edges + 15, 4), body)

    loop(rows, row)


def table_grad_kernel(rows, ids, cn, wn, cp, wp, own, tn, han, hbn, tp, hap, hbp, w2t, x, g1, table, *accs):
    zero_rows(accs)
    g1[...] = jnp.zeros_like(g1)

    def fill(dt, hid_a, hid_b):
        def put(i):
            at = rows_at(i)
            dh = jnp.dot(dt[at, :], w2t[...], preferred_element_type=F32)
            spread(table, i * BLOCK, masked(dh, hid_a[at, :], hid_b[at, :]))

        loop(dt.shape[0] // BLOCK, put)

    fill(tn, han, hbn)
    peer_pass(ids, cn, wn, rows, 0, table, accs)
    fill(tp, hap, hbp)
    peer_pass(ids, cp, wp, rows, 1, table, accs)

    def fold(i):
        total = unspread(own, i * BLOCK, BLOCK, 4)
        for acc in accs:
            total = total + unspread(acc, i * BLOCK, BLOCK, 4)
        g1[...] += lax.dot_general(x[rows_at(i), :], total.astype(BF16), CONTRACT_ROWS, preferred_element_type=F32)

    loop(x.shape[0] // BLOCK, fold)


def reduce_kernel(num_dev, g1, g2, loss, count, o1, o2, lo, pack, total, other_half, sums, parts, lslots, sem_s, sem_r, lsem_s, lsem_r):
    rows, tiles = g1.shape[0], g1.shape[1] // LANES
    base = rows * tiles
    for c in range(tiles):
        pack[c * rows:(c + 1) * rows, :] = g1[:, c * LANES:(c + 1) * LANES]
    end = base + g2.shape[0]
    pack[base:end, :] = g2[...]
    pack[end:, :] = jnp.zeros((pack.shape[0] - end, LANES), F32)
    me = lax.axis_index(GRAPH_AXIS)
    core = lax.rem(me, 2)
    chip = me // 2
    mate = me + 1 - 2 * core
    half = pack.shape[0] // 2
    part = half // 4
    enter(me, num_dev)

    def piece(owner):
        return pl.ds(pl.multiple_of(core * half + owner * part, 8), part)

    pair = push(pack.at[pl.ds(pl.multiple_of((1 - core) * half, 8), half)], other_half, sem_s.at[0], sem_r.at[0], mate)
    scalar = []
    for step in range(1, num_dev):
        scalar.append(push(loss, lslots.at[step - 1], lsem_s.at[step - 1], lsem_r.at[step - 1], lax.rem(me + step, num_dev)))
    pair.wait()
    sums[...] = pack[pl.ds(pl.multiple_of(core * half, 8), half), :] + other_half[...]
    spreads = []
    for step in range(1, 4):
        far = lax.rem(chip + step, 4)
        at = pl.ds(pl.multiple_of(far * part, 8), part)
        spreads.append(push(sums.at[at], parts.at[step - 1], sem_s.at[step], sem_r.at[step], far * 2 + core))
    for copy in spreads:
        copy.wait()
    mine = sums[pl.ds(pl.multiple_of(chip * part, 8), part), :]
    for step in range(3):
        mine = mine + parts[step]
    total[piece(chip), :] = mine
    gathers = []
    for step in range(1, 4):
        dev = lax.rem(chip + step, 4) * 2 + core
        gathers.append(push(total.at[piece(chip)], total.at[piece(chip)], sem_s.at[3 + step], sem_r.at[3 + step], dev))
    tails = [push(total.at[piece(chip)], total.at[piece(chip)], sem_s.at[7], sem_r.at[7], mate)]
    for step in range(1, 4):
        near = lax.rem(chip + 4 - step, 4)
        gathers[step - 1].wait()
        tails.append(push(total.at[piece(near)], total.at[piece(near)], sem_s.at[7 + step], sem_r.at[7 + step], mate))
    for copy in scalar:
        copy.wait()
    lsum = loss[...]
    for step in range(num_dev - 1):
        lsum = lsum + lslots[step]
    lsum = jnp.sum(jnp.sum(lsum, axis=1, keepdims=True), axis=0, keepdims=True)
    lo[...] = lsum / count[...]
    for copy in tails:
        copy.wait()
    for c in range(tiles):
        o1[:, c * LANES:(c + 1) * LANES] = total[c * rows:(c + 1) * rows, :]
    o2[...] = total[base:end, :]


def solution(mesh):
    num_dev = mesh.shape[GRAPH_AXIS]
    to_next = [(dev_id, (dev_id + 1) % num_dev) for dev_id in range(num_dev)]
    to_prev = [(dev_id, (dev_id - 1) % num_dev) for dev_id in range(num_dev)]

    def shift_next(a):
        return lax.ppermute(a, GRAPH_AXIS, to_next)

    def shift_prev(a):
        return lax.ppermute(a, GRAPH_AXIS, to_prev)

    def compact(edge_src, edge_dst, edge_w, n_loc, halo):
        rows = edge_src.shape[0] // CHUNK
        src, dst, w = (a.reshape(rows, CHUNK) for a in (edge_src, edge_dst, edge_w))
        live = w != 0.0
        own = live & (src < n_loc)
        far = live & (src >= n_loc + halo)
        near = live & (src >= n_loc) & (src < n_loc + halo)
        tri = (jnp.arange(CHUNK)[:, None] < jnp.arange(CHUNK)[None, :]).astype(BF16)
        sets = jnp.concatenate([own, near, far], axis=0).astype(BF16)
        rank = jnp.dot(sets, tri, preferred_element_type=F32).astype(jnp.int32)
        counts = jnp.sum(sets.astype(F32), axis=1).astype(jnp.int32)
        n_own, n_near, n_far = counts[:rows], counts[rows:2 * rows], counts[2 * rows:]
        skip = (n_near + 15) // 16 * 16
        place = jnp.where(far, SLOT - 1 - skip[:, None] - rank[2 * rows:], SLOT)
        place = jnp.where(near, SLOT - 1 - rank[rows:2 * rows], place)
        place = jnp.where(own, rank[:rows], place)
        hit = place[:, :, None] == jnp.arange(SLOT)[None, None, :]
        code = jnp.where(src < n_loc, src, src - n_loc) + dst * n_loc
        picks = (jnp.where(hit, code[:, :, None], 0), jnp.where(hit, w[:, :, None], 0.0))
        code, wc = lax.reduce(picks, (jnp.int32(0), jnp.float32(0.0)), lambda a, b: (a[0] + b[0], a[1] + b[1]), (1,))
        n_hal = jnp.where(n_far > 0, skip + n_far, n_near)
        return code, wc, n_own, n_hal, n_near, n_far, skip

    def device_step(node_feats, w_one, w_two, send_rows, edge_src, edge_dst, edge_w, labels, label_mask):
        n_loc, f_in = node_feats.shape
        halo = send_rows.shape[1]
        f_hid, classes = w_two.shape
        quad = 4 * n_loc
        sds = jax.ShapeDtypeStruct
        x = node_feats
        w1 = w_one.astype(BF16)
        w2t = jnp.pad(w_two.T.astype(BF16), ((0, LANES - classes), (0, 0)))
        ids = send_rows.reshape(-1)
        code, wc, n_own, n_hal, n_near, n_far, skip = compact(edge_src, edge_dst, edge_w, n_loc, halo)
        rows = n_own.shape[0]
        slots = code.size // LANES
        w_own = jnp.broadcast_to(wc[:, :CHUNK].reshape(-1, 1), (rows * CHUNK, LANES))
        code, wc = code.reshape(-1), wc.reshape(-1)
        tally = jnp.concatenate([n_near, n_far, skip, jnp.zeros((8 * LANES - 3 * rows,), jnp.int32)])
        lists = jnp.concatenate([code, tally]).reshape(slots + 8, LANES)
        count, code_prev, code_next, w_prev, w_next = pl.pallas_call(
            functools.partial(lists_kernel, num_dev),
            out_shape=[sds((8, LANES), F32)] + [sds((slots + 8, LANES), jnp.int32)] * 2 + [sds((slots, LANES), F32)] * 2,
            in_specs=[VMEM_SPEC] * 3,
            out_specs=[VMEM_SPEC] * 5,
            scratch_shapes=[pltpu.VMEM((8, LANES), F32), pltpu.VMEM((num_dev - 1, 8, LANES), F32)] + [pltpu.SemaphoreType.DMA((n,)) for n in (num_dev - 1, num_dev - 1, 4, 4)],
            compiler_params=params(1, collective_id=0, has_side_effects=True),
            name="lists",
        )(label_mask.reshape(-1, LANES), lists, wc.reshape(slots, LANES))
        s, d = code % n_loc, code // n_loc
        s4, d4 = s * 4, d * 4
        count, x = lax.optimization_barrier((count, x))
        x_next, x_prev = pl.pallas_call(
            halo_rows_kernel,
            out_shape=[sds((halo, 256), BF16)] * 2,
            in_specs=[SMEM_SPEC, VMEM_SPEC],
            out_specs=[VMEM_SPEC] * 2,
            scratch_shapes=[pltpu.VMEM((2 * n_loc, LANES), F32), pltpu.VMEM((4 * halo, LANES), F32)],
            compiler_params=params(12),
            name="halo_rows",
        )(ids, x)
        xh_prev = shift_next(x_next)
        xh_next = shift_prev(x_prev)
        wide4 = [pltpu.VMEM((quad, LANES), F32)] * 4
        thin4 = [pltpu.VMEM((n_loc, LANES), F32)] * 4
        marks = jnp.where(label_mask == 1, labels, -1)
        s4, w2t, marks, ids, w_own, wc = lax.optimization_barrier((s4, w2t, marks, ids, w_own, wc))
        y_own = pl.pallas_call(
            one_own_kernel,
            out_shape=sds((quad, LANES), F32),
            in_specs=[SMEM_SPEC] * 3 + [VMEM_SPEC] * 3,
            out_specs=VMEM_SPEC,
            scratch_shapes=[pltpu.VMEM((quad, LANES), F32)] + wide4,
            compiler_params=params(32),
            cost_estimate=pl.CostEstimate(flops=200000000000, bytes_accessed=8000000, transcendentals=0),
            name="one_own",
        )(s4, d4, n_own, x, w1, w_own)
        hid_a, hid_b, t2, t_next, t_prev = pl.pallas_call(
            one_halo_kernel,
            out_shape=[sds((n_loc, f_hid // 2), BF16)] * 2 + [sds((n_loc, LANES), F32), sds((halo, LANES), BF16), sds((halo, LANES), BF16)],
            in_specs=[SMEM_SPEC] * 5 + [VMEM_SPEC] * 5,
            out_specs=[VMEM_SPEC] * 5,
            scratch_shapes=[pltpu.VMEM((4 * 2 * halo, LANES), F32), pltpu.VMEM((2 * halo, LANES), F32)] + wide4,
            compiler_params=params(32),
            name="one_halo",
        )(s4, d4, wc, n_hal, ids, y_own, xh_prev, xh_next, w1, w2t)
        th_prev = shift_next(t_next)
        th_next = shift_prev(t_prev)
        ha_prev, ha_next = shift_next(hid_a), shift_prev(hid_a)
        narrow_own = functools.partial(
            pl.pallas_call,
            narrow_own_kernel,
            out_shape=sds((n_loc, LANES), F32),
            in_specs=[SMEM_SPEC] * 3 + [VMEM_SPEC] * 2,
            out_specs=VMEM_SPEC,
            scratch_shapes=thin4,
            compiler_params=params(14),
            cost_estimate=pl.CostEstimate(flops=200000000000, bytes_accessed=8000000, transcendentals=0),
        )
        z_own = narrow_own(name="two_own")(s, d, n_own, t2, w_own)
        marks = jnp.broadcast_to(marks[:, None], (n_loc, LANES))
        dz, bz_prev, bz_next, loss = pl.pallas_call(
            functools.partial(logits_kernel, classes),
            out_shape=[sds((n_loc, LANES), F32), sds((halo, LANES), F32), sds((halo, LANES), F32), sds((8, LANES), F32)],
            in_specs=[SMEM_SPEC] * 4 + [VMEM_SPEC] * 5,
            out_specs=[VMEM_SPEC] * 4,
            scratch_shapes=[pltpu.VMEM((2 * halo, LANES), F32)] + thin4,
            compiler_params=params(12),
            name="logits",
        )(s, d, wc, n_hal, z_own, th_prev, th_next, marks, count)
        rz_next = shift_prev(bz_prev)
        rz_prev = shift_next(bz_next)
        late_b, _ = lax.optimization_barrier((hid_b, bz_prev))
        hb_prev, hb_next = shift_next(late_b), shift_prev(late_b)
        dt2_own = narrow_own(name="two_back_own")(d, s, n_own, dz, w_own)
        dt2, dy, grad_two = pl.pallas_call(
            hidden_grad_kernel,
            out_shape=[sds((n_loc, LANES), BF16), sds((quad, LANES), F32), sds((f_hid, LANES), F32)],
            in_specs=[SMEM_SPEC] + [VMEM_SPEC] * 6,
            out_specs=[VMEM_SPEC] * 3,
            scratch_shapes=thin4,
            compiler_params=params(16),
            name="hidden_grad",
        )(ids, dt2_own, rz_next, rz_prev, hid_a, hid_b, w2t)
        dt_prev, dt_next = shift_next(dt2), shift_prev(dt2)
        dt1_own = pl.pallas_call(
            wide_own_kernel,
            out_shape=sds((quad, LANES), F32),
            in_specs=[SMEM_SPEC] * 3 + [VMEM_SPEC] * 2,
            out_specs=VMEM_SPEC,
            scratch_shapes=wide4,
            compiler_params=params(32),
            cost_estimate=pl.CostEstimate(flops=200000000000, bytes_accessed=8000000, transcendentals=0),
            name="one_back_own",
        )(d4, s4, n_own, dy, w_own)
        grad_one = pl.pallas_call(
            functools.partial(table_grad_kernel, rows),
            out_shape=sds((f_in, f_hid), F32),
            in_specs=[SMEM_SPEC] * 5 + [VMEM_SPEC] * 9,
            out_specs=VMEM_SPEC,
            scratch_shapes=[pltpu.VMEM((quad, LANES), F32)] + wide4,
            compiler_params=params(36),
            name="table_grad",
        )(ids, code_next.reshape(-1), w_next.reshape(-1), code_prev.reshape(-1), w_prev.reshape(-1), dt1_own, dt_next, ha_next, hb_next, dt_prev, ha_prev, hb_prev, w2t, x)
        pack_rows = f_in * f_hid // LANES + f_hid
        pack_rows += -pack_rows % 64
        grad_one, grad_two, loss = pl.pallas_call(
            functools.partial(reduce_kernel, num_dev),
            out_shape=[sds((f_in, f_hid), F32), sds((f_hid, LANES), F32), sds((8, LANES), F32)],
            in_specs=[VMEM_SPEC] * 4,
            out_specs=[VMEM_SPEC] * 3,
            scratch_shapes=[
                pltpu.VMEM((pack_rows, LANES), F32), pltpu.VMEM((pack_rows, LANES), F32),
                pltpu.VMEM((pack_rows // 2, LANES), F32), pltpu.VMEM((pack_rows // 2, LANES), F32),
                pltpu.VMEM((3, pack_rows // 8, LANES), F32), pltpu.VMEM((num_dev - 1, 8, LANES), F32),
            ] + [pltpu.SemaphoreType.DMA((n,)) for n in (11, 11, num_dev - 1, num_dev - 1)],
            compiler_params=params(8, collective_id=1, has_side_effects=True),
            name="reduce",
        )(grad_one, grad_two, loss, count)
        return loss[0, 0], grad_one, grad_two[:, :classes]

    row_spec = P(GRAPH_AXIS)
    return jax.shard_map(device_step, mesh=mesh, in_specs=(row_spec, P(), P(), row_spec, row_spec, row_spec, row_spec, row_spec, row_spec), out_specs=(P(), P(), P()), check_vma=False)
```

```python
import functools

import jax
import jax.numpy as jnp
from jax import lax
from jax.experimental import pallas as pl
from jax.experimental.pallas import tpu as pltpu
from jax.sharding import PartitionSpec as P


GRAPH_AXIS = "graph"
CONTRACT_ROWS = (((0,), (0,)), ((), ()))
CONTRACT_COLS = (((1,), (1,)), ((), ()))
MESH = pl.DeviceIdType.MESH
F32 = jnp.float32
BF16 = jnp.bfloat16
LANES = 128
BLOCK = 256
CHUNK = 256
SLOT = 384

SMEM_SPEC = pl.BlockSpec(memory_space=pltpu.SMEM)
VMEM_SPEC = pl.BlockSpec(memory_space=pltpu.VMEM)


def rows_at(i, base=0, size=BLOCK):
    return pl.ds(base + i * size, size)


def loop(count, body):
    lax.fori_loop(0, count, lambda i, _: (body(i), 0)[1], 0)


def params(mib, **kw):
    return pltpu.CompilerParams(vmem_limit_bytes=mib * 2**20, **kw)


def zero_rows(refs):
    rows = refs[0].shape[0]

    def body(i):
        for ref in refs:
            ref[pl.ds(i * 64, 64), :] = jnp.zeros((64, LANES), F32)

    loop(rows // 64, body)


def sum_rows(out, refs):
    rows = refs[0].shape[0]

    def body(i):
        total = refs[0][pl.ds(i * 64, 64), :]
        for ref in refs[1:]:
            total = total + ref[pl.ds(i * 64, 64), :]
        out[pl.ds(i * 64, 64), :] = total

    loop(rows // 64, body)


def edge_pass(from_ref, to_ref, w_ref, cnt_ref, table, accs, width, unroll, back):
    n_acc = len(accs)
    shift = unroll.bit_length() - 1

    def row(r):
        blocks = lax.shift_right_logical(cnt_ref[r] + (unroll - 1), shift)

        def body(j):
            off = r * SLOT + (SLOT - unroll - j * unroll if back else j * unroll)
            frm, to = (ref.at[pl.ds(off, unroll)] for ref in (from_ref, to_ref))
            if back:
                wgt = w_ref.at[pl.ds(off, unroll)]
            else:
                wgt = [jnp.broadcast_to(w_ref[pl.ds(r * CHUNK + j * unroll + u, 1), :], (width, LANES)) for u in range(unroll)]
            for u in range(unroll):
                acc = accs[u % n_acc]
                val = table[pl.ds(pl.multiple_of(frm[u], width), width), :] * wgt[u]
                at = pl.ds(pl.multiple_of(to[u], width), width)
                acc[at, :] = acc[at, :] + val

        loop(blocks, body)

    loop(cnt_ref.shape[0], row)


def scatter_pass(ids_ref, table, accs, width, unroll):
    n_acc = len(accs)

    def body(j):
        off = j * unroll
        for g in range(unroll // n_acc):
            rows = [pl.multiple_of(ids_ref[off + g * n_acc + k], width) for k in range(n_acc)]
            vals = [table[pl.ds(pl.multiple_of((off + g * n_acc + k) * width, width), width), :] for k in range(n_acc)]
            old = [accs[k][pl.ds(rows[k], width), :] for k in range(n_acc)]
            for k in range(n_acc):
                accs[k][pl.ds(rows[k], width), :] = old[k] + vals[k]

    loop(ids_ref.shape[0] // unroll, body)


def gather_pass(ids_ref, table, out, width, unroll=16):
    def body(j):
        for u in range(unroll):
            i = j * unroll + u
            out[pl.ds(pl.multiple_of(i * width, width), width), :] = table[pl.ds(pl.multiple_of(ids_ref[i] * width, width), width), :]

    loop(ids_ref.shape[0] // unroll, body)


def spread(table, start, block):
    tiles = block.shape[1] // LANES
    for c in range(tiles):
        table[pl.ds(start * tiles + c, block.shape[0], tiles), :] = block[:, c * LANES:(c + 1) * LANES]


def unspread(table, start, rows, tiles):
    return jnp.concatenate([table[pl.ds(start * tiles + c, rows, tiles), :] for c in range(tiles)], axis=1)


def enter(me, num_dev):
    barrier = pltpu.get_barrier_semaphore()
    for step in range(1, num_dev):
        pl.semaphore_signal(barrier, inc=1, device_id=(lax.rem(me + step, num_dev),), device_id_type=MESH)
    pl.semaphore_wait(barrier, num_dev - 1)


def push(src, dst, send_sem, recv_sem, dev):
    copy = pltpu.make_async_remote_copy(src_ref=src, dst_ref=dst, send_sem=send_sem, recv_sem=recv_sem, device_id=(dev,), device_id_type=MESH)
    copy.start()
    return copy


def lists_kernel(num_dev, mask, code, wgt, count, code_prev, code_next, w_prev, w_next, part, slots, send_sem, recv_sem, lsend, lrecv):
    ones = jnp.sum(jnp.sum(mask[...].astype(F32), axis=1, keepdims=True), axis=0, keepdims=True)
    part[...] = jnp.broadcast_to(ones, part.shape)
    me = lax.axis_index(GRAPH_AXIS)
    succ, pred = lax.rem(me + 1, num_dev), lax.rem(me + num_dev - 1, num_dev)
    enter(me, num_dev)
    copies = []
    for step in range(1, num_dev):
        copies.append(push(part, slots.at[step - 1], send_sem.at[step - 1], recv_sem.at[step - 1], lax.rem(me + step, num_dev)))
    copies.append(push(code, code_prev, lsend.at[0], lrecv.at[0], succ))
    copies.append(push(code, code_next, lsend.at[1], lrecv.at[1], pred))
    copies.append(push(wgt, w_prev, lsend.at[2], lrecv.at[2], succ))
    copies.append(push(wgt, w_next, lsend.at[3], lrecv.at[3], pred))
    for copy in copies:
        copy.wait()
    total = part[...]
    for step in range(num_dev - 1):
        total = total + slots[step]
    count[...] = jnp.maximum(total, 1.0)


def halo_rows_kernel(ids, x, to_next, to_prev, table, picked):
    rows = x.shape[0]

    def put(i):
        block = x[rows_at(i), :].astype(F32)
        pad = jnp.zeros((BLOCK, 2 * LANES - block.shape[1]), F32)
        spread(table, i * BLOCK, jnp.concatenate([block, pad], axis=1))

    loop(rows // BLOCK, put)
    gather_pass(ids, table, picked, 2)
    half = to_next.shape[0]

    def take(i):
        to_prev[rows_at(i), :] = unspread(picked, i * BLOCK, BLOCK, 2).astype(BF16)
        to_next[rows_at(i), :] = unspread(picked, half + i * BLOCK, BLOCK, 2).astype(BF16)

    loop(half // BLOCK, take)


def one_own_kernel(s4, d4, cnt, x, w1, w, y, table, *accs):
    zero_rows(accs)

    def put(i):
        t = jnp.dot(x[rows_at(i), :], w1[...], preferred_element_type=F32)
        spread(table, i * BLOCK, t.astype(BF16).astype(F32))

    loop(x.shape[0] // BLOCK, put)
    edge_pass(s4, d4, w, cnt, table, accs, 4, 32, False)
    sum_rows(y, accs)


def one_halo_kernel(s4, d4, w, cnt, ids, y_own, x_prev, x_next, w1, w2t, hid_a, hid_b, t2, to_next, to_prev, table, picked, *accs):
    zero_rows(accs)
    half = x_prev.shape[0]

    def put(i):
        t = jnp.dot(x_prev[rows_at(i), :w1.shape[0]], w1[...], preferred_element_type=F32)
        spread(table, i * BLOCK, t.astype(BF16).astype(F32))
        t = jnp.dot(x_next[rows_at(i), :w1.shape[0]], w1[...], preferred_element_type=F32)
        spread(table, half + i * BLOCK, t.astype(BF16).astype(F32))

    loop(half // BLOCK, put)
    edge_pass(s4, d4, w, cnt, table, accs, 4, 16, True)
    sum_rows(accs[0], (y_own,) + accs)

    def act(i):
        h = jnp.maximum(unspread(accs[0], i * BLOCK, BLOCK, 4), 0.0).astype(BF16)
        cut = hid_a.shape[1]
        hid_a[rows_at(i), :] = h[:, :cut]
        hid_b[rows_at(i), :] = h[:, cut:]
        t = lax.dot_general(h, w2t[...], CONTRACT_COLS, preferred_element_type=F32)
        t2[rows_at(i), :] = t.astype(BF16).astype(F32)

    loop(t2.shape[0] // BLOCK, act)
    gather_pass(ids, t2, picked, 1)

    def take(i):
        to_prev[rows_at(i), :] = picked[rows_at(i), :].astype(BF16)
        to_next[rows_at(i), :] = picked[rows_at(i, half), :].astype(BF16)

    loop(half // BLOCK, take)


def narrow_own_kernel(frm, to, cnt, table, w, out, *accs):
    zero_rows(accs)
    edge_pass(frm, to, w, cnt, table, accs, 1, 32, False)
    sum_rows(out, accs)


def wide_own_kernel(frm, to, cnt, table, w, out, *accs):
    zero_rows(accs)
    edge_pass(frm, to, w, cnt, table, accs, 4, 32, False)
    sum_rows(out, accs)


def logits_kernel(classes, s, d, w, cnt, z_own, t_prev, t_next, labels, count, dz, back_prev, back_next, loss, table, *accs):
    zero_rows(accs)
    half = t_prev.shape[0]

    def put(i):
        table[rows_at(i), :] = t_prev[rows_at(i), :].astype(F32)
        table[rows_at(i, half), :] = t_next[rows_at(i), :].astype(F32)

    loop(half // BLOCK, put)
    edge_pass(s, d, w, cnt, table, accs, 1, 16, True)
    denom = count[0:1, :]
    loss[...] = jnp.zeros_like(loss)

    def soft(i):
        at = pl.ds(i * 64, 64)
        z = z_own[at, :]
        for acc in accs:
            z = z + acc[at, :]
        lane = lax.broadcasted_iota(jnp.int32, z.shape, 1)
        lab = labels[at, :]
        hot = lab == lane
        keep = lab >= 0
        zm = jnp.where(lane < classes, z, -jnp.inf)
        top = jnp.max(zm, axis=1, keepdims=True)
        ex = jnp.exp(zm - top)
        log_norm = jnp.log(jnp.sum(ex, axis=1, keepdims=True)) + top
        hot_f = jnp.where(hot, 1.0, 0.0)
        term = jnp.where(hot, log_norm - z, 0.0)
        part = term[0:8]
        for b in range(1, 8):
            part = part + term[b * 8:b * 8 + 8]
        loss[...] += part
        mask_f = jnp.where(keep, 1.0, 0.0)
        dz[at, :] = jnp.where(lane < classes, (jnp.exp(zm - log_norm) - hot_f) * (mask_f / denom), 0.0)

    loop(dz.shape[0] // 64, soft)
    zero_rows(accs)
    edge_pass(d, s, w, cnt, dz, accs, 1, 16, True)

    def fin(i):
        at = pl.ds(i * 64, 64)
        bt = pl.ds(half + i * 64, 64)
        a, b = accs[0][at, :], accs[0][bt, :]
        for acc in accs[1:]:
            a, b = a + acc[at, :], b + acc[bt, :]
        back_prev[at, :] = a
        back_next[at, :] = b

    loop(half // 64, fin)


def masked(grad, hid_a, hid_b):
    cut = hid_a.shape[1]
    lo = jnp.where(hid_a.astype(F32) > 0.0, grad[:, :cut], 0.0)
    hi = jnp.where(hid_b.astype(F32) > 0.0, grad[:, cut:], 0.0)
    return jnp.concatenate([lo, hi], axis=1)


def hidden_grad_kernel(ids, own, ret_next, ret_prev, hid_a, hid_b, w2t, dt2, dy, g2, *accs):
    n_loc, half = own.shape[0], ret_next.shape[0]
    zero_rows(accs)
    scatter_pass(ids.at[pl.ds(half, half)], ret_next, accs, 1, 16)
    scatter_pass(ids.at[pl.ds(0, half)], ret_prev, accs, 1, 16)
    g2[...] = jnp.zeros_like(g2)

    def fold(i):
        at = rows_at(i)
        total = own[at, :]
        for acc in accs:
            total = total + acc[at, :]
        dt = total.astype(BF16)
        dt2[at, :] = dt
        cut = hid_a.shape[1]
        g2[:cut, :] += lax.dot_general(hid_a[at, :], dt, CONTRACT_ROWS, preferred_element_type=F32)
        g2[cut:, :] += lax.dot_general(hid_b[at, :], dt, CONTRACT_ROWS, preferred_element_type=F32)
        dh = jnp.dot(dt, w2t[...], preferred_element_type=F32)
        spread(dy, i * BLOCK, masked(dh, hid_a[at, :], hid_b[at, :]))

    loop(n_loc // BLOCK, fold)


def peer_pass(ids, code_ref, w_ref, rows, far, table, accs):
    n_acc = len(accs)
    tally = rows * SLOT
    n_loc = ids.shape[0]
    shift = n_loc.bit_length() - 1
    half = n_loc // 2
    owners = ids.at[pl.ds(0 if far else half, half)]

    def row(r):
        first = SLOT - 16 - (code_ref[tally + 2 * rows + r] if far else 0)
        edges = code_ref[tally + far * rows + r]

        def body(j):
            off = r * SLOT + first - j * 16
            codes, wgt = (ref.at[pl.ds(off, 16)] for ref in (code_ref, w_ref))
            for u in range(16):
                acc = accs[u % n_acc]
                code = codes[u]
                frm = lax.shift_right_logical(code, shift)
                val = table[pl.ds(pl.multiple_of(frm, 4), 4), :] * wgt[u]
                at = pl.ds(pl.multiple_of(owners[code & (half - 1)] * 4, 4), 4)
                acc[at, :] = acc[at, :] + val

        loop(lax.shift_right_logical(edges + 15, 4), body)

    loop(rows, row)


def table_grad_kernel(rows, ids, cn, wn, cp, wp, own, tn, han, hbn, tp, hap, hbp, w2t, x, g1, table, *accs):
    zero_rows(accs)
    g1[...] = jnp.zeros_like(g1)

    def fill(dt, hid_a, hid_b):
        def put(i):
            at = rows_at(i)
            dh = jnp.dot(dt[at, :], w2t[...], preferred_element_type=F32)
            spread(table, i * BLOCK, masked(dh, hid_a[at, :], hid_b[at, :]))

        loop(dt.shape[0] // BLOCK, put)

    fill(tn, han, hbn)
    peer_pass(ids, cn, wn, rows, 0, table, accs)
    fill(tp, hap, hbp)
    peer_pass(ids, cp, wp, rows, 1, table, accs)

    def fold(i):
        total = unspread(own, i * BLOCK, BLOCK, 4)
        for acc in accs:
            total = total + unspread(acc, i * BLOCK, BLOCK, 4)
        g1[...] += lax.dot_general(x[rows_at(i), :], total.astype(BF16), CONTRACT_ROWS, preferred_element_type=F32)

    loop(x.shape[0] // BLOCK, fold)


def reduce_kernel(num_dev, g1, g2, loss, count, o1, o2, lo, pack, total, other_half, sums, parts, lslots, sem_s, sem_r, lsem_s, lsem_r):
    rows, tiles = g1.shape[0], g1.shape[1] // LANES
    base = rows * tiles
    for c in range(tiles):
        pack[c * rows:(c + 1) * rows, :] = g1[:, c * LANES:(c + 1) * LANES]
    end = base + g2.shape[0]
    pack[base:end, :] = g2[...]
    pack[end:, :] = jnp.zeros((pack.shape[0] - end, LANES), F32)
    me = lax.axis_index(GRAPH_AXIS)
    core = lax.rem(me, 2)
    chip = me // 2
    mate = me + 1 - 2 * core
    half = pack.shape[0] // 2
    part = half // 4
    enter(me, num_dev)

    def piece(owner):
        return pl.ds(pl.multiple_of(core * half + owner * part, 8), part)

    pair = push(pack.at[pl.ds(pl.multiple_of((1 - core) * half, 8), half)], other_half, sem_s.at[0], sem_r.at[0], mate)
    scalar = []
    for step in range(1, num_dev):
        scalar.append(push(loss, lslots.at[step - 1], lsem_s.at[step - 1], lsem_r.at[step - 1], lax.rem(me + step, num_dev)))
    pair.wait()
    sums[...] = pack[pl.ds(pl.multiple_of(core * half, 8), half), :] + other_half[...]
    spreads = []
    for step in range(1, 4):
        far = lax.rem(chip + step, 4)
        at = pl.ds(pl.multiple_of(far * part, 8), part)
        spreads.append(push(sums.at[at], parts.at[step - 1], sem_s.at[step], sem_r.at[step], far * 2 + core))
    for copy in spreads:
        copy.wait()
    mine = sums[pl.ds(pl.multiple_of(chip * part, 8), part), :]
    for step in range(3):
        mine = mine + parts[step]
    total[piece(chip), :] = mine
    gathers = []
    for step in range(1, 4):
        dev = lax.rem(chip + step, 4) * 2 + core
        gathers.append(push(total.at[piece(chip)], total.at[piece(chip)], sem_s.at[3 + step], sem_r.at[3 + step], dev))
    tails = [push(total.at[piece(chip)], total.at[piece(chip)], sem_s.at[7], sem_r.at[7], mate)]
    for step in range(1, 4):
        near = lax.rem(chip + 4 - step, 4)
        gathers[step - 1].wait()
        tails.append(push(total.at[piece(near)], total.at[piece(near)], sem_s.at[7 + step], sem_r.at[7 + step], mate))
    for copy in scalar:
        copy.wait()
    lsum = loss[...]
    for step in range(num_dev - 1):
        lsum = lsum + lslots[step]
    lsum = jnp.sum(jnp.sum(lsum, axis=1, keepdims=True), axis=0, keepdims=True)
    lo[...] = lsum / count[...]
    for copy in tails:
        copy.wait()
    for c in range(tiles):
        o1[:, c * LANES:(c + 1) * LANES] = total[c * rows:(c + 1) * rows, :]
    o2[...] = total[base:end, :]


def solution(mesh):
    num_dev = mesh.shape[GRAPH_AXIS]
    to_next = [(dev_id, (dev_id + 1) % num_dev) for dev_id in range(num_dev)]
    to_prev = [(dev_id, (dev_id - 1) % num_dev) for dev_id in range(num_dev)]

    def shift_next(a):
        return lax.ppermute(a, GRAPH_AXIS, to_next)

    def shift_prev(a):
        return lax.ppermute(a, GRAPH_AXIS, to_prev)

    def compact(edge_src, edge_dst, edge_w, n_loc, halo):
        rows = edge_src.shape[0] // CHUNK
        views = [a.reshape(2, rows, LANES) for a in (edge_src, edge_dst, edge_w)]
        src, dst, w = (jnp.concatenate([v[0], v[1]], axis=1) for v in views)
        live = w != 0.0
        own = live & (src < n_loc)
        far = live & (src >= n_loc + halo)
        near = live & (src >= n_loc) & (src < n_loc + halo)
        tri = (jnp.arange(CHUNK)[:, None] < jnp.arange(CHUNK)[None, :]).astype(BF16)
        sets = jnp.concatenate([own, near, far], axis=0).astype(BF16)
        rank = jnp.dot(sets, tri, preferred_element_type=F32).astype(jnp.int32)
        counts = jnp.sum(sets.astype(F32), axis=1).astype(jnp.int32)
        n_own, n_near, n_far = counts[:rows], counts[rows:2 * rows], counts[2 * rows:]
        skip = (n_near + 15) // 16 * 16
        place = jnp.where(far, SLOT - 1 - skip[:, None] - rank[2 * rows:], SLOT)
        place = jnp.where(near, SLOT - 1 - rank[rows:2 * rows], place)
        place = jnp.where(own, rank[:rows], place)
        hit = place[:, :, None] == jnp.arange(SLOT)[None, None, :]
        code = jnp.where(src < n_loc, src, src - n_loc) + dst * (4 * n_loc)
        picks = (jnp.where(hit, code[:, :, None], 0), jnp.where(hit, w[:, :, None], 0.0))
        code, wc = lax.reduce(picks, (jnp.int32(0), jnp.float32(0.0)), lambda a, b: (a[0] + b[0], a[1] + b[1]), (1,))
        n_hal = jnp.where(n_far > 0, skip + n_far, n_near)
        return code, wc, n_own, n_hal, n_near, n_far, skip

    def device_step(node_feats, w_one, w_two, send_rows, edge_src, edge_dst, edge_w, labels, label_mask):
        n_loc, f_in = node_feats.shape
        halo = send_rows.shape[1]
        f_hid, classes = w_two.shape
        quad = 4 * n_loc
        sds = jax.ShapeDtypeStruct
        x = node_feats
        w1 = w_one.astype(BF16)
        w2t = jnp.pad(w_two.T.astype(BF16), ((0, LANES - classes), (0, 0)))
        ids = send_rows.reshape(-1)
        code, wc, n_own, n_hal, n_near, n_far, skip = compact(edge_src, edge_dst, edge_w, n_loc, halo)
        rows = n_own.shape[0]
        slots = code.size // LANES
        w_own = jnp.broadcast_to(wc[:, :CHUNK].reshape(-1, 1), (rows * CHUNK, LANES))
        code, wc = code.reshape(-1), wc.reshape(-1)
        tally = jnp.concatenate([n_near, n_far, skip, jnp.zeros((8 * LANES - 3 * rows,), jnp.int32)])
        lists = jnp.concatenate([code, tally]).reshape(slots + 8, LANES)
        count, code_prev, code_next, w_prev, w_next = pl.pallas_call(
            functools.partial(lists_kernel, num_dev),
            out_shape=[sds((8, LANES), F32)] + [sds((slots + 8, LANES), jnp.int32)] * 2 + [sds((slots, LANES), F32)] * 2,
            in_specs=[VMEM_SPEC] * 3,
            out_specs=[VMEM_SPEC] * 5,
            scratch_shapes=[pltpu.VMEM((8, LANES), F32), pltpu.VMEM((num_dev - 1, 8, LANES), F32)] + [pltpu.SemaphoreType.DMA((n,)) for n in (num_dev - 1, num_dev - 1, 4, 4)],
            compiler_params=params(1, collective_id=0, has_side_effects=True),
            name="lists",
        )(label_mask.reshape(-1, LANES), lists, wc.reshape(slots, LANES))
        s, d4 = code % n_loc, code // n_loc
        s4, d = s * 4, d4 // 4
        count, x = lax.optimization_barrier((count, x))
        x_next, x_prev = pl.pallas_call(
            halo_rows_kernel,
            out_shape=[sds((halo, 256), BF16)] * 2,
            in_specs=[SMEM_SPEC, VMEM_SPEC],
            out_specs=[VMEM_SPEC] * 2,
            scratch_shapes=[pltpu.VMEM((2 * n_loc, LANES), F32), pltpu.VMEM((4 * halo, LANES), F32)],
            compiler_params=params(12),
            name="halo_rows",
        )(ids, x)
        xh_prev = shift_next(x_next)
        xh_next = shift_prev(x_prev)
        wide4 = [pltpu.VMEM((quad, LANES), F32)] * 4
        thin4 = [pltpu.VMEM((n_loc, LANES), F32)] * 4
        marks = jnp.where(label_mask == 1, labels, -1)
        s4, w2t, marks, ids, w_own, wc = lax.optimization_barrier((s4, w2t, marks, ids, w_own, wc))
        y_own = pl.pallas_call(
            one_own_kernel,
            out_shape=sds((quad, LANES), F32),
            in_specs=[SMEM_SPEC] * 3 + [VMEM_SPEC] * 3,
            out_specs=VMEM_SPEC,
            scratch_shapes=[pltpu.VMEM((quad, LANES), F32)] + wide4,
            compiler_params=params(32),
            cost_estimate=pl.CostEstimate(flops=200000000000, bytes_accessed=8000000, transcendentals=0),
            name="one_own",
        )(s4, d4, n_own, x, w1, w_own)
        hid_a, hid_b, t2, t_next, t_prev = pl.pallas_call(
            one_halo_kernel,
            out_shape=[sds((n_loc, f_hid // 2), BF16)] * 2 + [sds((n_loc, LANES), F32), sds((halo, LANES), BF16), sds((halo, LANES), BF16)],
            in_specs=[SMEM_SPEC] * 5 + [VMEM_SPEC] * 5,
            out_specs=[VMEM_SPEC] * 5,
            scratch_shapes=[pltpu.VMEM((4 * 2 * halo, LANES), F32), pltpu.VMEM((2 * halo, LANES), F32)] + wide4,
            compiler_params=params(32),
            name="one_halo",
        )(s4, d4, wc, n_hal, ids, y_own, xh_prev, xh_next, w1, w2t)
        th_prev = shift_next(t_next)
        th_next = shift_prev(t_prev)
        ha_prev, ha_next = shift_next(hid_a), shift_prev(hid_a)
        narrow_own = functools.partial(
            pl.pallas_call,
            narrow_own_kernel,
            out_shape=sds((n_loc, LANES), F32),
            in_specs=[SMEM_SPEC] * 3 + [VMEM_SPEC] * 2,
            out_specs=VMEM_SPEC,
            scratch_shapes=thin4,
            compiler_params=params(14),
            cost_estimate=pl.CostEstimate(flops=200000000000, bytes_accessed=8000000, transcendentals=0),
        )
        z_own = narrow_own(name="two_own")(s, d, n_own, t2, w_own)
        marks = jnp.broadcast_to(marks[:, None], (n_loc, LANES))
        dz, bz_prev, bz_next, loss = pl.pallas_call(
            functools.partial(logits_kernel, classes),
            out_shape=[sds((n_loc, LANES), F32), sds((halo, LANES), F32), sds((halo, LANES), F32), sds((8, LANES), F32)],
            in_specs=[SMEM_SPEC] * 4 + [VMEM_SPEC] * 5,
            out_specs=[VMEM_SPEC] * 4,
            scratch_shapes=[pltpu.VMEM((2 * halo, LANES), F32)] + thin4,
            compiler_params=params(12),
            name="logits",
        )(s, d, wc, n_hal, z_own, th_prev, th_next, marks, count)
        rz_next = shift_prev(bz_prev)
        rz_prev = shift_next(bz_next)
        late_b, _ = lax.optimization_barrier((hid_b, bz_prev))
        hb_prev, hb_next = shift_next(late_b), shift_prev(late_b)
        dt2_own = narrow_own(name="two_back_own")(d, s, n_own, dz, w_own)
        dt2, dy, grad_two = pl.pallas_call(
            hidden_grad_kernel,
            out_shape=[sds((n_loc, LANES), BF16), sds((quad, LANES), F32), sds((f_hid, LANES), F32)],
            in_specs=[SMEM_SPEC] + [VMEM_SPEC] * 6,
            out_specs=[VMEM_SPEC] * 3,
            scratch_shapes=thin4,
            compiler_params=params(16),
            name="hidden_grad",
        )(ids, dt2_own, rz_next, rz_prev, hid_a, hid_b, w2t)
        dt_prev, dt_next = shift_next(dt2), shift_prev(dt2)
        dt1_own = pl.pallas_call(
            wide_own_kernel,
            out_shape=sds((quad, LANES), F32),
            in_specs=[SMEM_SPEC] * 3 + [VMEM_SPEC] * 2,
            out_specs=VMEM_SPEC,
            scratch_shapes=wide4,
            compiler_params=params(32),
            cost_estimate=pl.CostEstimate(flops=200000000000, bytes_accessed=8000000, transcendentals=0),
            name="one_back_own",
        )(d4, s4, n_own, dy, w_own)
        grad_one = pl.pallas_call(
            functools.partial(table_grad_kernel, rows),
            out_shape=sds((f_in, f_hid), F32),
            in_specs=[SMEM_SPEC] * 5 + [VMEM_SPEC] * 9,
            out_specs=VMEM_SPEC,
            scratch_shapes=[pltpu.VMEM((quad, LANES), F32)] + wide4,
            compiler_params=params(36),
            name="table_grad",
        )(ids, code_next.reshape(-1), w_next.reshape(-1), code_prev.reshape(-1), w_prev.reshape(-1), dt1_own, dt_next, ha_next, hb_next, dt_prev, ha_prev, hb_prev, w2t, x)
        pack_rows = f_in * f_hid // LANES + f_hid
        pack_rows += -pack_rows % 64
        grad_one, grad_two, loss = pl.pallas_call(
            functools.partial(reduce_kernel, num_dev),
            out_shape=[sds((f_in, f_hid), F32), sds((f_hid, LANES), F32), sds((8, LANES), F32)],
            in_specs=[VMEM_SPEC] * 4,
            out_specs=[VMEM_SPEC] * 3,
            scratch_shapes=[
                pltpu.VMEM((pack_rows, LANES), F32), pltpu.VMEM((pack_rows, LANES), F32),
                pltpu.VMEM((pack_rows // 2, LANES), F32), pltpu.VMEM((pack_rows // 2, LANES), F32),
                pltpu.VMEM((3, pack_rows // 8, LANES), F32), pltpu.VMEM((num_dev - 1, 8, LANES), F32),
            ] + [pltpu.SemaphoreType.DMA((n,)) for n in (11, 11, num_dev - 1, num_dev - 1)],
            compiler_params=params(8, collective_id=1, has_side_effects=True),
            name="reduce",
        )(grad_one, grad_two, loss, count)
        return loss[0, 0], grad_one, grad_two[:, :classes]

    row_spec = P(GRAPH_AXIS)
    return jax.shard_map(device_step, mesh=mesh, in_specs=(row_spec, P(), P(), row_spec, row_spec, row_spec, row_spec, row_spec, row_spec), out_specs=(P(), P(), P()), check_vma=False)
```

```python
import functools

import jax
import jax.numpy as jnp
from jax import lax
from jax.experimental import pallas as pl
from jax.experimental.pallas import tpu as pltpu
from jax.sharding import PartitionSpec as P


GRAPH_AXIS = "graph"
CONTRACT_ROWS = (((0,), (0,)), ((), ()))
CONTRACT_COLS = (((1,), (1,)), ((), ()))
MESH = pl.DeviceIdType.MESH
F32 = jnp.float32
BF16 = jnp.bfloat16
LANES = 128
BLOCK = 256
CHUNK = 256
SLOT = 384

SMEM_SPEC = pl.BlockSpec(memory_space=pltpu.SMEM)
VMEM_SPEC = pl.BlockSpec(memory_space=pltpu.VMEM)


def rows_at(i, base=0, size=BLOCK):
    return pl.ds(base + i * size, size)


def loop(count, body):
    lax.fori_loop(0, count, lambda i, _: (body(i), 0)[1], 0)


def params(mib, **kw):
    return pltpu.CompilerParams(vmem_limit_bytes=mib * 2**20, **kw)


def zero_rows(refs):
    rows = refs[0].shape[0]

    def body(i):
        for ref in refs:
            ref[pl.ds(i * 64, 64), :] = jnp.zeros((64, LANES), F32)

    loop(rows // 64, body)


def start_rows(first, refs):
    def body(i):
        at = pl.ds(i * 64, 64)
        refs[0][at, :] = first[at, :]
        for ref in refs[1:]:
            ref[at, :] = jnp.zeros((64, LANES), F32)

    loop(refs[0].shape[0] // 64, body)


def sum_rows(out, refs):
    rows = refs[0].shape[0]

    def body(i):
        total = refs[0][pl.ds(i * 64, 64), :]
        for ref in refs[1:]:
            total = total + ref[pl.ds(i * 64, 64), :]
        out[pl.ds(i * 64, 64), :] = total

    loop(rows // 64, body)


def edge_pass(from_ref, to_ref, w_ref, cnt_ref, table, accs, width, unroll, back):
    n_acc = len(accs)
    shift = unroll.bit_length() - 1

    def row(r):
        blocks = lax.shift_right_logical(cnt_ref[r] + (unroll - 1), shift)

        def body(j):
            off = r * SLOT + (SLOT - unroll - j * unroll if back else j * unroll)
            frm, to = (ref.at[pl.ds(off, unroll)] for ref in (from_ref, to_ref))
            if back:
                wgt = w_ref.at[pl.ds(off, unroll)]
            else:
                wgt = [jnp.broadcast_to(w_ref[pl.ds(r * CHUNK + j * unroll + u, 1), :], (width, LANES)) for u in range(unroll)]
            for u in range(unroll):
                acc = accs[u % n_acc]
                val = table[pl.ds(pl.multiple_of(frm[u], width), width), :] * wgt[u]
                at = pl.ds(pl.multiple_of(to[u], width), width)
                acc[at, :] = acc[at, :] + val

        loop(blocks, body)

    loop(cnt_ref.shape[0], row)


def scatter_pass(ids_ref, table, accs, width, unroll):
    n_acc = len(accs)

    def body(j):
        off = j * unroll
        for g in range(unroll // n_acc):
            rows = [pl.multiple_of(ids_ref[off + g * n_acc + k], width) for k in range(n_acc)]
            vals = [table[pl.ds(pl.multiple_of((off + g * n_acc + k) * width, width), width), :] for k in range(n_acc)]
            old = [accs[k][pl.ds(rows[k], width), :] for k in range(n_acc)]
            for k in range(n_acc):
                accs[k][pl.ds(rows[k], width), :] = old[k] + vals[k]

    loop(ids_ref.shape[0] // unroll, body)


def gather_pass(ids_ref, table, out, width, unroll=16):
    def body(j):
        for u in range(unroll):
            i = j * unroll + u
            out[pl.ds(pl.multiple_of(i * width, width), width), :] = table[pl.ds(pl.multiple_of(ids_ref[i] * width, width), width), :]

    loop(ids_ref.shape[0] // unroll, body)


def spread(table, start, block):
    tiles = block.shape[1] // LANES
    for c in range(tiles):
        table[pl.ds(start * tiles + c, block.shape[0], tiles), :] = block[:, c * LANES:(c + 1) * LANES]


def unspread(table, start, rows, tiles):
    return jnp.concatenate([table[pl.ds(start * tiles + c, rows, tiles), :] for c in range(tiles)], axis=1)


def enter(me, num_dev):
    barrier = pltpu.get_barrier_semaphore()
    for step in range(1, num_dev):
        pl.semaphore_signal(barrier, inc=1, device_id=(lax.rem(me + step, num_dev),), device_id_type=MESH)
    pl.semaphore_wait(barrier, num_dev - 1)


def push(src, dst, send_sem, recv_sem, dev):
    copy = pltpu.make_async_remote_copy(src_ref=src, dst_ref=dst, send_sem=send_sem, recv_sem=recv_sem, device_id=(dev,), device_id_type=MESH)
    copy.start()
    return copy


def lists_kernel(num_dev, mask, code, wgt, count, code_prev, code_next, w_prev, w_next, part, slots, send_sem, recv_sem, lsend, lrecv):
    ones = jnp.sum(jnp.sum(mask[...].astype(F32), axis=1, keepdims=True), axis=0, keepdims=True)
    part[...] = jnp.broadcast_to(ones, part.shape)
    me = lax.axis_index(GRAPH_AXIS)
    succ, pred = lax.rem(me + 1, num_dev), lax.rem(me + num_dev - 1, num_dev)
    enter(me, num_dev)
    copies = []
    for step in range(1, num_dev):
        copies.append(push(part, slots.at[step - 1], send_sem.at[step - 1], recv_sem.at[step - 1], lax.rem(me + step, num_dev)))
    copies.append(push(code, code_prev, lsend.at[0], lrecv.at[0], succ))
    copies.append(push(code, code_next, lsend.at[1], lrecv.at[1], pred))
    copies.append(push(wgt, w_prev, lsend.at[2], lrecv.at[2], succ))
    copies.append(push(wgt, w_next, lsend.at[3], lrecv.at[3], pred))
    for copy in copies:
        copy.wait()
    total = part[...]
    for step in range(num_dev - 1):
        total = total + slots[step]
    count[...] = jnp.maximum(total, 1.0)


def halo_rows_kernel(ids, x, to_next, to_prev, table, picked):
    rows = x.shape[0]

    def put(i):
        block = x[rows_at(i), :].astype(F32)
        pad = jnp.zeros((BLOCK, 2 * LANES - block.shape[1]), F32)
        spread(table, i * BLOCK, jnp.concatenate([block, pad], axis=1))

    loop(rows // BLOCK, put)
    gather_pass(ids, table, picked, 2)
    half = to_next.shape[0]

    def take(i):
        to_prev[rows_at(i), :] = unspread(picked, i * BLOCK, BLOCK, 2).astype(BF16)
        to_next[rows_at(i), :] = unspread(picked, half + i * BLOCK, BLOCK, 2).astype(BF16)

    loop(half // BLOCK, take)


def one_own_kernel(s4, d4, cnt, x, w1, w, y, table, *accs):
    zero_rows(accs)

    def put(i):
        t = jnp.dot(x[rows_at(i), :], w1[...], preferred_element_type=F32)
        spread(table, i * BLOCK, t.astype(BF16).astype(F32))

    loop(x.shape[0] // BLOCK, put)
    edge_pass(s4, d4, w, cnt, table, accs, 4, 32, False)
    sum_rows(y, accs)


def one_halo_kernel(s4, d4, w, cnt, ids, y_own, x_prev, x_next, w1, w2t, hid_a, hid_b, t2, to_next, to_prev, table, picked, *accs):
    start_rows(y_own, accs)
    half = x_prev.shape[0]

    def put(i):
        t = jnp.dot(x_prev[rows_at(i), :w1.shape[0]], w1[...], preferred_element_type=F32)
        spread(table, i * BLOCK, t.astype(BF16).astype(F32))
        t = jnp.dot(x_next[rows_at(i), :w1.shape[0]], w1[...], preferred_element_type=F32)
        spread(table, half + i * BLOCK, t.astype(BF16).astype(F32))

    loop(half // BLOCK, put)
    edge_pass(s4, d4, w, cnt, table, accs, 4, 16, True)
    sum_rows(accs[0], accs)

    def act(i):
        h = jnp.maximum(unspread(accs[0], i * BLOCK, BLOCK, 4), 0.0).astype(BF16)
        cut = hid_a.shape[1]
        hid_a[rows_at(i), :] = h[:, :cut]
        hid_b[rows_at(i), :] = h[:, cut:]
        t = lax.dot_general(h, w2t[...], CONTRACT_COLS, preferred_element_type=F32)
        t2[rows_at(i), :] = t.astype(BF16).astype(F32)

    loop(t2.shape[0] // BLOCK, act)
    gather_pass(ids, t2, picked, 1)

    def take(i):
        to_prev[rows_at(i), :] = picked[rows_at(i), :].astype(BF16)
        to_next[rows_at(i), :] = picked[rows_at(i, half), :].astype(BF16)

    loop(half // BLOCK, take)


def narrow_own_kernel(frm, to, cnt, table, w, out, *accs):
    zero_rows(accs)
    edge_pass(frm, to, w, cnt, table, accs, 1, 32, False)
    sum_rows(out, accs)


def wide_own_kernel(frm, to, cnt, table, w, out, *accs):
    zero_rows(accs)
    edge_pass(frm, to, w, cnt, table, accs, 4, 32, False)
    sum_rows(out, accs)


def logits_kernel(classes, s, d, w, cnt, z_own, t_prev, t_next, labels, count, dz, back_prev, back_next, loss, table, *accs):
    zero_rows(accs)
    half = t_prev.shape[0]

    def put(i):
        table[rows_at(i), :] = t_prev[rows_at(i), :].astype(F32)
        table[rows_at(i, half), :] = t_next[rows_at(i), :].astype(F32)

    loop(half // BLOCK, put)
    edge_pass(s, d, w, cnt, table, accs, 1, 16, True)
    denom = count[0:1, :]
    loss[...] = jnp.zeros_like(loss)

    def soft(i):
        at = pl.ds(i * 64, 64)
        z = z_own[at, :]
        for acc in accs:
            z = z + acc[at, :]
        lane = lax.broadcasted_iota(jnp.int32, z.shape, 1)
        lab = labels[at, :]
        hot = lab == lane
        keep = lab >= 0
        zm = jnp.where(lane < classes, z, -jnp.inf)
        top = jnp.max(zm, axis=1, keepdims=True)
        ex = jnp.exp(zm - top)
        log_norm = jnp.log(jnp.sum(ex, axis=1, keepdims=True)) + top
        hot_f = jnp.where(hot, 1.0, 0.0)
        term = jnp.where(hot, log_norm - z, 0.0)
        part = term[0:8]
        for b in range(1, 8):
            part = part + term[b * 8:b * 8 + 8]
        loss[...] += part
        mask_f = jnp.where(keep, 1.0, 0.0)
        dz[at, :] = jnp.where(lane < classes, (jnp.exp(zm - log_norm) - hot_f) * (mask_f / denom), 0.0)

    loop(dz.shape[0] // 64, soft)
    zero_rows(accs)
    edge_pass(d, s, w, cnt, dz, accs, 1, 16, True)

    def fin(i):
        at = pl.ds(i * 64, 64)
        bt = pl.ds(half + i * 64, 64)
        a, b = accs[0][at, :], accs[0][bt, :]
        for acc in accs[1:]:
            a, b = a + acc[at, :], b + acc[bt, :]
        back_prev[at, :] = a
        back_next[at, :] = b

    loop(half // 64, fin)


def masked(grad, hid_a, hid_b):
    cut = hid_a.shape[1]
    lo = jnp.where(hid_a.astype(F32) > 0.0, grad[:, :cut], 0.0)
    hi = jnp.where(hid_b.astype(F32) > 0.0, grad[:, cut:], 0.0)
    return jnp.concatenate([lo, hi], axis=1)


def hidden_grad_kernel(ids, own, ret_next, ret_prev, hid_a, hid_b, w2t, dt2, dy, g2, *accs):
    n_loc, half = own.shape[0], ret_next.shape[0]
    zero_rows(accs)
    scatter_pass(ids.at[pl.ds(half, half)], ret_next, accs, 1, 16)
    scatter_pass(ids.at[pl.ds(0, half)], ret_prev, accs, 1, 16)
    g2[...] = jnp.zeros_like(g2)

    def fold(i):
        at = rows_at(i)
        total = own[at, :]
        for acc in accs:
            total = total + acc[at, :]
        dt = total.astype(BF16)
        dt2[at, :] = dt
        cut = hid_a.shape[1]
        g2[:cut, :] += lax.dot_general(hid_a[at, :], dt, CONTRACT_ROWS, preferred_element_type=F32)
        g2[cut:, :] += lax.dot_general(hid_b[at, :], dt, CONTRACT_ROWS, preferred_element_type=F32)
        dh = jnp.dot(dt, w2t[...], preferred_element_type=F32)
        spread(dy, i * BLOCK, masked(dh, hid_a[at, :], hid_b[at, :]))

    loop(n_loc // BLOCK, fold)


def peer_pass(ids, code_ref, w_ref, rows, far, table, accs):
    n_acc = len(accs)
    tally = rows * SLOT
    n_loc = ids.shape[0]
    shift = n_loc.bit_length() - 1
    half = n_loc // 2
    owners = ids.at[pl.ds(0 if far else half, half)]

    def row(r):
        first = SLOT - 16 - (code_ref[tally + 2 * rows + r] if far else 0)
        edges = code_ref[tally + far * rows + r]

        def body(j):
            off = r * SLOT + first - j * 16
            codes, wgt = (ref.at[pl.ds(off, 16)] for ref in (code_ref, w_ref))
            for u in range(16):
                acc = accs[u % n_acc]
                code = codes[u]
                frm = lax.shift_right_logical(code, shift)
                val = table[pl.ds(pl.multiple_of(frm, 4), 4), :] * wgt[u]
                at = pl.ds(pl.multiple_of(owners[code & (half - 1)] * 4, 4), 4)
                acc[at, :] = acc[at, :] + val

        loop(lax.shift_right_logical(edges + 15, 4), body)

    loop(rows, row)


def table_grad_kernel(rows, ids, cn, wn, cp, wp, own, tn, han, hbn, tp, hap, hbp, w2t, x, g1, table, *accs):
    start_rows(own, accs)
    g1[...] = jnp.zeros_like(g1)

    def fill(dt, hid_a, hid_b):
        def put(i):
            at = rows_at(i)
            dh = jnp.dot(dt[at, :], w2t[...], preferred_element_type=F32)
            spread(table, i * BLOCK, masked(dh, hid_a[at, :], hid_b[at, :]))

        loop(dt.shape[0] // BLOCK, put)

    fill(tn, han, hbn)
    peer_pass(ids, cn, wn, rows, 0, table, accs)
    fill(tp, hap, hbp)
    peer_pass(ids, cp, wp, rows, 1, table, accs)

    def fold(i):
        total = unspread(accs[0], i * BLOCK, BLOCK, 4)
        for acc in accs[1:]:
            total = total + unspread(acc, i * BLOCK, BLOCK, 4)
        g1[...] += lax.dot_general(x[rows_at(i), :], total.astype(BF16), CONTRACT_ROWS, preferred_element_type=F32)

    loop(x.shape[0] // BLOCK, fold)


def reduce_kernel(num_dev, g1, g2, loss, count, o1, o2, lo, pack, total, other_half, sums, parts, lslots, sem_s, sem_r, lsem_s, lsem_r):
    rows, tiles = g1.shape[0], g1.shape[1] // LANES
    base = rows * tiles
    for c in range(tiles):
        pack[c * rows:(c + 1) * rows, :] = g1[:, c * LANES:(c + 1) * LANES]
    end = base + g2.shape[0]
    pack[base:end, :] = g2[...]
    pack[end:, :] = jnp.zeros((pack.shape[0] - end, LANES), F32)
    me = lax.axis_index(GRAPH_AXIS)
    core = lax.rem(me, 2)
    chip = me // 2
    mate = me + 1 - 2 * core
    half = pack.shape[0] // 2
    part = half // 4
    enter(me, num_dev)

    def piece(owner):
        return pl.ds(pl.multiple_of(core * half + owner * part, 8), part)

    pair = push(pack.at[pl.ds(pl.multiple_of((1 - core) * half, 8), half)], other_half, sem_s.at[0], sem_r.at[0], mate)
    scalar = []
    for step in range(1, num_dev):
        scalar.append(push(loss, lslots.at[step - 1], lsem_s.at[step - 1], lsem_r.at[step - 1], lax.rem(me + step, num_dev)))
    pair.wait()
    sums[...] = pack[pl.ds(pl.multiple_of(core * half, 8), half), :] + other_half[...]
    spreads = []
    for step in range(1, 4):
        far = lax.rem(chip + step, 4)
        at = pl.ds(pl.multiple_of(far * part, 8), part)
        spreads.append(push(sums.at[at], parts.at[step - 1], sem_s.at[step], sem_r.at[step], far * 2 + core))
    for copy in spreads:
        copy.wait()
    mine = sums[pl.ds(pl.multiple_of(chip * part, 8), part), :]
    for step in range(3):
        mine = mine + parts[step]
    total[piece(chip), :] = mine
    gathers = []
    for step in range(1, 4):
        dev = lax.rem(chip + step, 4) * 2 + core
        gathers.append(push(total.at[piece(chip)], total.at[piece(chip)], sem_s.at[3 + step], sem_r.at[3 + step], dev))
    tails = [push(total.at[piece(chip)], total.at[piece(chip)], sem_s.at[7], sem_r.at[7], mate)]
    for step in range(1, 4):
        near = lax.rem(chip + 4 - step, 4)
        gathers[step - 1].wait()
        tails.append(push(total.at[piece(near)], total.at[piece(near)], sem_s.at[7 + step], sem_r.at[7 + step], mate))
    for copy in scalar:
        copy.wait()
    lsum = loss[...]
    for step in range(num_dev - 1):
        lsum = lsum + lslots[step]
    lsum = jnp.sum(jnp.sum(lsum, axis=1, keepdims=True), axis=0, keepdims=True)
    lo[...] = lsum / count[...]
    for copy in tails:
        copy.wait()
    for c in range(tiles):
        o1[:, c * LANES:(c + 1) * LANES] = total[c * rows:(c + 1) * rows, :]
    o2[...] = total[base:end, :]


def solution(mesh):
    num_dev = mesh.shape[GRAPH_AXIS]
    to_next = [(dev_id, (dev_id + 1) % num_dev) for dev_id in range(num_dev)]
    to_prev = [(dev_id, (dev_id - 1) % num_dev) for dev_id in range(num_dev)]

    def shift_next(a):
        return lax.ppermute(a, GRAPH_AXIS, to_next)

    def shift_prev(a):
        return lax.ppermute(a, GRAPH_AXIS, to_prev)

    def compact(edge_src, edge_dst, edge_w, n_loc, halo):
        rows = edge_src.shape[0] // CHUNK
        views = [a.reshape(2, rows, LANES) for a in (edge_src, edge_dst, edge_w)]
        src, dst, w = (jnp.concatenate([v[0], v[1]], axis=1) for v in views)
        live = w != 0.0
        own = live & (src < n_loc)
        far = live & (src >= n_loc + halo)
        near = live & (src >= n_loc) & (src < n_loc + halo)
        tri = (jnp.arange(CHUNK)[:, None] < jnp.arange(CHUNK)[None, :]).astype(BF16)
        sets = jnp.concatenate([own, near, far], axis=0).astype(BF16)
        rank = jnp.dot(sets, tri, preferred_element_type=F32).astype(jnp.int32)
        counts = jnp.sum(sets.astype(F32), axis=1).astype(jnp.int32)
        n_own, n_near, n_far = counts[:rows], counts[rows:2 * rows], counts[2 * rows:]
        skip = (n_near + 15) // 16 * 16
        place = jnp.where(far, SLOT - 1 - skip[:, None] - rank[2 * rows:], SLOT)
        place = jnp.where(near, SLOT - 1 - rank[rows:2 * rows], place)
        place = jnp.where(own, rank[:rows], place)
        hit = place[:, :, None] == jnp.arange(SLOT)[None, None, :]
        code = jnp.where(src < n_loc, src, src - n_loc) + dst * (4 * n_loc)
        picks = (jnp.where(hit, code[:, :, None], 0), jnp.where(hit, w[:, :, None], 0.0))
        code, wc = lax.reduce(picks, (jnp.int32(0), jnp.float32(0.0)), lambda a, b: (a[0] + b[0], a[1] + b[1]), (1,))
        n_hal = jnp.where(n_far > 0, skip + n_far, n_near)
        return code, wc, n_own, n_hal, n_near, n_far, skip

    def device_step(node_feats, w_one, w_two, send_rows, edge_src, edge_dst, edge_w, labels, label_mask):
        n_loc, f_in = node_feats.shape
        halo = send_rows.shape[1]
        f_hid, classes = w_two.shape
        quad = 4 * n_loc
        sds = jax.ShapeDtypeStruct
        x = node_feats
        w1 = w_one.astype(BF16)
        w2t = jnp.pad(w_two.T.astype(BF16), ((0, LANES - classes), (0, 0)))
        ids = send_rows.reshape(-1)
        code, wc, n_own, n_hal, n_near, n_far, skip = compact(edge_src, edge_dst, edge_w, n_loc, halo)
        rows = n_own.shape[0]
        slots = code.size // LANES
        w_own = jnp.broadcast_to(wc[:, :CHUNK].reshape(-1, 1), (rows * CHUNK, LANES))
        code, wc = code.reshape(-1), wc.reshape(-1)
        tally = jnp.concatenate([n_near, n_far, skip, jnp.zeros((8 * LANES - 3 * rows,), jnp.int32)])
        lists = jnp.concatenate([code, tally]).reshape(slots + 8, LANES)
        count, code_prev, code_next, w_prev, w_next = pl.pallas_call(
            functools.partial(lists_kernel, num_dev),
            out_shape=[sds((8, LANES), F32)] + [sds((slots + 8, LANES), jnp.int32)] * 2 + [sds((slots, LANES), F32)] * 2,
            in_specs=[VMEM_SPEC] * 3,
            out_specs=[VMEM_SPEC] * 5,
            scratch_shapes=[pltpu.VMEM((8, LANES), F32), pltpu.VMEM((num_dev - 1, 8, LANES), F32)] + [pltpu.SemaphoreType.DMA((n,)) for n in (num_dev - 1, num_dev - 1, 4, 4)],
            compiler_params=params(1, collective_id=0, has_side_effects=True),
            name="lists",
        )(label_mask.reshape(-1, LANES), lists, wc.reshape(slots, LANES))
        s, d4 = code % n_loc, code // n_loc
        s4, d = s * 4, d4 // 4
        count, x = lax.optimization_barrier((count, x))
        x_next, x_prev = pl.pallas_call(
            halo_rows_kernel,
            out_shape=[sds((halo, 256), BF16)] * 2,
            in_specs=[SMEM_SPEC, VMEM_SPEC],
            out_specs=[VMEM_SPEC] * 2,
            scratch_shapes=[pltpu.VMEM((2 * n_loc, LANES), F32), pltpu.VMEM((4 * halo, LANES), F32)],
            compiler_params=params(12),
            name="halo_rows",
        )(ids, x)
        xh_prev = shift_next(x_next)
        xh_next = shift_prev(x_prev)
        wide4 = [pltpu.VMEM((quad, LANES), F32)] * 4
        thin4 = [pltpu.VMEM((n_loc, LANES), F32)] * 4
        marks = jnp.where(label_mask == 1, labels, -1)
        s4, w2t, marks, ids, w_own, wc = lax.optimization_barrier((s4, w2t, marks, ids, w_own, wc))
        y_own = pl.pallas_call(
            one_own_kernel,
            out_shape=sds((quad, LANES), F32),
            in_specs=[SMEM_SPEC] * 3 + [VMEM_SPEC] * 3,
            out_specs=VMEM_SPEC,
            scratch_shapes=[pltpu.VMEM((quad, LANES), F32)] + wide4,
            compiler_params=params(32),
            cost_estimate=pl.CostEstimate(flops=200000000000, bytes_accessed=8000000, transcendentals=0),
            name="one_own",
        )(s4, d4, n_own, x, w1, w_own)
        hid_a, hid_b, t2, t_next, t_prev = pl.pallas_call(
            one_halo_kernel,
            out_shape=[sds((n_loc, f_hid // 2), BF16)] * 2 + [sds((n_loc, LANES), F32), sds((halo, LANES), BF16), sds((halo, LANES), BF16)],
            in_specs=[SMEM_SPEC] * 5 + [VMEM_SPEC] * 5,
            out_specs=[VMEM_SPEC] * 5,
            scratch_shapes=[pltpu.VMEM((4 * 2 * halo, LANES), F32), pltpu.VMEM((2 * halo, LANES), F32)] + wide4,
            compiler_params=params(32),
            name="one_halo",
        )(s4, d4, wc, n_hal, ids, y_own, xh_prev, xh_next, w1, w2t)
        th_prev = shift_next(t_next)
        th_next = shift_prev(t_prev)
        ha_prev, ha_next = shift_next(hid_a), shift_prev(hid_a)
        narrow_own = functools.partial(
            pl.pallas_call,
            narrow_own_kernel,
            out_shape=sds((n_loc, LANES), F32),
            in_specs=[SMEM_SPEC] * 3 + [VMEM_SPEC] * 2,
            out_specs=VMEM_SPEC,
            scratch_shapes=thin4,
            compiler_params=params(14),
            cost_estimate=pl.CostEstimate(flops=200000000000, bytes_accessed=8000000, transcendentals=0),
        )
        z_own = narrow_own(name="two_own")(s, d, n_own, t2, w_own)
        marks = jnp.broadcast_to(marks[:, None], (n_loc, LANES))
        dz, bz_prev, bz_next, loss = pl.pallas_call(
            functools.partial(logits_kernel, classes),
            out_shape=[sds((n_loc, LANES), F32), sds((halo, LANES), F32), sds((halo, LANES), F32), sds((8, LANES), F32)],
            in_specs=[SMEM_SPEC] * 4 + [VMEM_SPEC] * 5,
            out_specs=[VMEM_SPEC] * 4,
            scratch_shapes=[pltpu.VMEM((2 * halo, LANES), F32)] + thin4,
            compiler_params=params(12),
            name="logits",
        )(s, d, wc, n_hal, z_own, th_prev, th_next, marks, count)
        rz_next = shift_prev(bz_prev)
        rz_prev = shift_next(bz_next)
        late_b, _ = lax.optimization_barrier((hid_b, bz_prev))
        hb_prev, hb_next = shift_next(late_b), shift_prev(late_b)
        dt2_own = narrow_own(name="two_back_own")(d, s, n_own, dz, w_own)
        dt2, dy, grad_two = pl.pallas_call(
            hidden_grad_kernel,
            out_shape=[sds((n_loc, LANES), BF16), sds((quad, LANES), F32), sds((f_hid, LANES), F32)],
            in_specs=[SMEM_SPEC] + [VMEM_SPEC] * 6,
            out_specs=[VMEM_SPEC] * 3,
            scratch_shapes=thin4,
            compiler_params=params(16),
            name="hidden_grad",
        )(ids, dt2_own, rz_next, rz_prev, hid_a, hid_b, w2t)
        dt_prev, dt_next = shift_next(dt2), shift_prev(dt2)
        dt1_own = pl.pallas_call(
            wide_own_kernel,
            out_shape=sds((quad, LANES), F32),
            in_specs=[SMEM_SPEC] * 3 + [VMEM_SPEC] * 2,
            out_specs=VMEM_SPEC,
            scratch_shapes=wide4,
            compiler_params=params(32),
            cost_estimate=pl.CostEstimate(flops=200000000000, bytes_accessed=8000000, transcendentals=0),
            name="one_back_own",
        )(d4, s4, n_own, dy, w_own)
        grad_one = pl.pallas_call(
            functools.partial(table_grad_kernel, rows),
            out_shape=sds((f_in, f_hid), F32),
            in_specs=[SMEM_SPEC] * 5 + [VMEM_SPEC] * 9,
            out_specs=VMEM_SPEC,
            scratch_shapes=[pltpu.VMEM((quad, LANES), F32)] + wide4,
            compiler_params=params(36),
            name="table_grad",
        )(ids, code_next.reshape(-1), w_next.reshape(-1), code_prev.reshape(-1), w_prev.reshape(-1), dt1_own, dt_next, ha_next, hb_next, dt_prev, ha_prev, hb_prev, w2t, x)
        pack_rows = f_in * f_hid // LANES + f_hid
        pack_rows += -pack_rows % 64
        grad_one, grad_two, loss = pl.pallas_call(
            functools.partial(reduce_kernel, num_dev),
            out_shape=[sds((f_in, f_hid), F32), sds((f_hid, LANES), F32), sds((8, LANES), F32)],
            in_specs=[VMEM_SPEC] * 4,
            out_specs=[VMEM_SPEC] * 3,
            scratch_shapes=[
                pltpu.VMEM((pack_rows, LANES), F32), pltpu.VMEM((pack_rows, LANES), F32),
                pltpu.VMEM((pack_rows // 2, LANES), F32), pltpu.VMEM((pack_rows // 2, LANES), F32),
                pltpu.VMEM((3, pack_rows // 8, LANES), F32), pltpu.VMEM((num_dev - 1, 8, LANES), F32),
            ] + [pltpu.SemaphoreType.DMA((n,)) for n in (11, 11, num_dev - 1, num_dev - 1)],
            compiler_params=params(8, collective_id=1, has_side_effects=True),
            name="reduce",
        )(grad_one, grad_two, loss, count)
        return loss[0, 0], grad_one, grad_two[:, :classes]

    row_spec = P(GRAPH_AXIS)
    return jax.shard_map(device_step, mesh=mesh, in_specs=(row_spec, P(), P(), row_spec, row_spec, row_spec, row_spec, row_spec, row_spec), out_specs=(P(), P(), P()), check_vma=False)
```
